32 devices in a mesh: freq: 8 (over z, y), rows: 4 (over x, core).
Axes of the slice: x: 2, y: 2, z: 4, core: 2. Of those that a mesh axis runs over, the one named last changes fastest.
Arguments:
- wavefield: bfloat16 [10240, 32, 1024], P('freq', 'rows'), may hold values from -6 to 6
- u_factors: bfloat16 [2, 16, 4, 256, 512], P(None, 'freq', 'rows'), may hold values from -0.25 to 0.25
- v_factors: bfloat16 [2, 16, 4, 512, 256], P(None, 'freq', 'rows'), may hold values from -0.375 to 0.375
- tile_ranks: int32 [16, 4, 40], P('freq', 'rows'), may hold values from 1 to 64, as said below
- tile_offsets: int32 [16, 4, 40], P('freq', 'rows'), may hold values from 0 to 511, as said below
Outputs:
- convolved: bfloat16 [1024, 32, 1024], P(('rows', 'freq'))
The draws below stay inside these ranges and needn't reach their ends.
Inputs may be any that keep to these rules, and one draw needn't show every extreme that they name: tile_ranks[k, i, j] is the rank of tile (i, j) of frequency k; the ranks of one tile row sum to at most 512, exactly 512 on some row of every draw, and every tile row has a tile of rank 64. tile_offsets[k, i, j] is the sum of tile_ranks[k, i, j2] over j2 < j.
All inputs are finite; a program needn't handle non-finite values.
Results may differ from the reference program's by a relative error of at most 0.0072.
Values may be sent and summed in bfloat16 or wider, within the bound.
No kernel may reach another device: no remote copies, remote signals or barrier semaphores. Data moves between devices by JAX's collectives and lax.ppermute only.
A program may use at most 128 MiB of HBM per device.

```python
import math
import jax
import jax.numpy as jnp
from jax import lax

RECEIVERS = 10240
SAMPLES = 1024
TILE = 256
RANK_MAX = 64
SLOTS = 512
SOURCES = 32
FREQS = 16
TILE_ROWS = 4
TILE_COLS = 40


def rank_tables(key):
    base_key = jax.random.fold_in(key, 4242)
    key_weight, key_target, key_chosen, key_peak = jax.random.split(base_key, 4)
    weight = jax.random.randint(key_weight, (FREQS, TILE_ROWS, TILE_COLS), 1, 65)
    weight = weight * weight // 64 + 1
    target = SLOTS // 2 + jax.random.randint(key_target, (FREQS, TILE_ROWS), 0, SLOTS - SLOTS // 2 + 1)
    chosen = jax.random.randint(key_chosen, (), 0, FREQS * TILE_ROWS)
    row_number = jnp.arange(FREQS * TILE_ROWS, dtype=jnp.int32).reshape(FREQS, TILE_ROWS)
    target = jnp.where(row_number == chosen, SLOTS, target)
    peak_tile = jax.random.randint(key_peak, (FREQS, TILE_ROWS, 1), 0, TILE_COLS)
    is_peak = jnp.arange(TILE_COLS, dtype=jnp.int32)[None, None, :] == peak_tile
    spare_slots = target - (TILE_COLS - 1) - RANK_MAX
    others = jnp.where(is_peak, 0, weight)
    weight_sum = jnp.sum(others, axis=2)
    base_rank = jnp.minimum(1 + others * spare_slots[:, :, None] // weight_sum[:, :, None], RANK_MAX)
    rank_table = jnp.where(is_peak, RANK_MAX, base_rank)
    deficit = target - jnp.sum(rank_table, axis=2)
    headroom = jnp.where(is_peak, 0, RANK_MAX - rank_table)
    before = jnp.cumsum(headroom, axis=2) - headroom
    rank_table = rank_table + jnp.clip(deficit[:, :, None] - before, 0, headroom)
    starts = jnp.cumsum(rank_table, axis=2) - rank_table
    return (rank_table.astype(jnp.int32), starts.astype(jnp.int32))


def draw_tile_ranks(key, part):
    return rank_tables(key)[0]


def draw_tile_offsets(key, part):
    return rank_tables(key)[1]


def level_of(rng, shape, cuts, least, top_value):
    def one(dim, parts):
        steps = jax.random.uniform(jax.random.fold_in(jax.random.fold_in(rng, 6), dim), (parts,), jnp.float32, least / len(cuts), top_value / len(cuts))
        return jnp.repeat(jnp.exp(steps), shape[dim] // parts).reshape((-1,) + (1,) * (len(shape) - dim - 1))

    gain = one(*cuts[0])
    for cut in cuts[1:]:
        gain = gain * one(*cut)
    return gain


def gaussian(stream_key, shape, spread, most, shards=(), kind=jnp.bfloat16):
    entries = jax.random.normal(stream_key, shape, jnp.float32) * spread
    if len(shards) > 0:
        entries = level_of(stream_key, shape, shards, -0.22, 0.18) * entries
    return jnp.clip(entries, min=-most, max=most).astype(kind)


def setup_inputs(seed: int = 0) -> dict:
    seeds = jax.random.split(jax.random.key(seed), 6)
    return {
        "wavefield": gaussian(seeds[0], (RECEIVERS, SOURCES, SAMPLES), 1.0, 6.0, ((0, 8), (1, 4))),
        "u_factors": gaussian(seeds[1], (2, FREQS, TILE_ROWS, TILE, SLOTS), SLOTS ** -0.5, 0.25, ((1, 8), (2, 4))),
        "v_factors": gaussian(seeds[2], (2, FREQS, TILE_ROWS, SLOTS, TILE), TILE ** -0.5, 0.375, ((1, 8), (2, 4))),
        "tile_ranks": draw_tile_ranks(jax.random.fold_in(seeds[5], 71), 0),
        "tile_offsets": draw_tile_offsets(jax.random.fold_in(seeds[5], 71), 0),
    }


def spectral_tables(freq_count, sample_count):
    freq_bins = jnp.arange(freq_count, dtype=jnp.int32) + 1
    sample_index = jnp.arange(sample_count, dtype=jnp.int32)
    phase_int = freq_bins[:, None] * sample_index[None, :] % sample_count
    angles = phase_int.astype(jnp.float32) * (2.0 * math.pi / sample_count)
    cosine = jnp.cos(angles)
    minus_sine = -jnp.sin(angles)
    stacked = jnp.stack([cosine, minus_sine], axis=1)
    forward = (stacked / math.sqrt(sample_count)).astype(jnp.bfloat16)
    inverse = (stacked / math.sqrt(freq_count)).astype(jnp.bfloat16)
    return (forward, inverse)

def tile_windows(v_row, u_row, starts, rank_max):
    columns = starts.shape[0]
    slot_index = (starts[:, None] + jnp.arange(rank_max, dtype=jnp.int32)[None, :]).reshape(-1)
    v_padded = jnp.pad(v_row, ((0, 0), (0, rank_max), (0, 0)))
    u_padded = jnp.pad(u_row, ((0, 0), (0, 0), (0, rank_max)))
    v_win = jnp.take(v_padded, slot_index, axis=1).reshape(2, columns, rank_max, v_row.shape[2])
    u_win = jnp.take(u_padded, slot_index, axis=2).reshape(2, u_row.shape[1], columns, rank_max)
    return (v_win, u_win)

def tile_row_product(u_row, v_row, counts, starts, spectra):
    v_win, u_win = tile_windows(v_row, u_row, starts, RANK_MAX)
    quadrants = jnp.einsum('ajmr,jbrs->abjms', v_win.astype(jnp.float32), spectra.astype(jnp.float32))
    real_part = quadrants[0, 0] - quadrants[1, 1]
    imag_part = quadrants[0, 1] + quadrants[1, 0]
    rank_mask = jnp.arange(RANK_MAX, dtype=jnp.int32)[None, :] < counts[:, None]
    coeffs = jnp.where(rank_mask[None, :, :, None], jnp.stack([real_part, imag_part]), 0.0).astype(jnp.bfloat16)
    products = jnp.einsum('arjm,cjms->acrs', u_win.astype(jnp.float32), coeffs.astype(jnp.float32))
    return jnp.stack([products[0, 0] - products[1, 1], products[0, 1] + products[1, 0]]).astype(jnp.bfloat16)

def reference(wavefield, u_factors, v_factors, tile_ranks, tile_offsets):
    receivers, sources, samples = wavefield.shape
    freqs = u_factors.shape[1]
    tile_rows = u_factors.shape[2]
    tile_size = u_factors.shape[3]
    columns = receivers // tile_size
    forward, inverse = spectral_tables(freqs, samples)
    blocks = wavefield.reshape(columns, tile_size, sources, samples)

    def transform(block):
        return jnp.einsum('kct,rst->kcrs', forward.astype(jnp.float32), block.astype(jnp.float32)).astype(jnp.bfloat16)
    spectrum = jnp.moveaxis(lax.map(transform, blocks), 1, 0)

    def one_band(items):
        spectra, u_band, v_band, counts, starts = items
        rows_out = [tile_row_product(u_band[:, tile_row], v_band[:, tile_row], counts[tile_row], starts[tile_row], spectra) for tile_row in range(tile_rows)]
        return jnp.stack(rows_out, axis=1)
    bands = lax.map(one_band, (spectrum, jnp.moveaxis(u_factors, 1, 0), jnp.moveaxis(v_factors, 1, 0), tile_ranks, tile_offsets))
    flat_bands = bands.reshape(freqs, 2, tile_rows * tile_size * sources)
    series = jnp.einsum('kcq,kct->qt', flat_bands.astype(jnp.float32), inverse.astype(jnp.float32))
    return series.reshape(tile_rows * tile_size, sources, samples).astype(jnp.bfloat16)
```

```python
import functools
import math

import jax
import jax.numpy as jnp
from jax import lax
from jax.experimental import pallas as pl
from jax.experimental.pallas import tpu as pltpu
from jax.sharding import PartitionSpec as P

RANK_MAX = 64
LANES = 128
SUBLANES = 8
NT = (((1,), (1,)), ((), ()))


def spectral_tables(freq_count, sample_count):
    freq_bins = jnp.arange(freq_count, dtype=jnp.int32) + 1
    sample_index = jnp.arange(sample_count, dtype=jnp.int32)
    phase_int = freq_bins[:, None] * sample_index[None, :] % sample_count
    angles = phase_int.astype(jnp.float32) * (2.0 * math.pi / sample_count)
    cosine = jnp.cos(angles)
    minus_sine = -jnp.sin(angles)
    stacked = jnp.stack([cosine, minus_sine], axis=1)
    forward = (stacked / math.sqrt(sample_count)).astype(jnp.bfloat16)
    inverse = (stacked / math.sqrt(freq_count)).astype(jnp.bfloat16)
    return (forward, inverse)


def tile_windows(v_row, u_row, starts, rank_max):
    columns = starts.shape[0]
    slot_index = (starts[:, None] + jnp.arange(rank_max, dtype=jnp.int32)[None, :]).reshape(-1)
    v_padded = jnp.pad(v_row, ((0, 0), (0, rank_max), (0, 0)))
    u_padded = jnp.pad(u_row, ((0, 0), (0, 0), (0, rank_max)))
    v_win = jnp.take(v_padded, slot_index, axis=1).reshape(2, columns, rank_max, v_row.shape[2])
    u_win = jnp.take(u_padded, slot_index, axis=2).reshape(2, u_row.shape[1], columns, rank_max)
    return (v_win, u_win)


def slot_lookup(starts, counts, rank_max, slot_count):
    position = jnp.arange(slot_count, dtype=jnp.int32)
    started = starts[:, None, :] <= position[None, :, None]
    owner_tile = jnp.sum(started.astype(jnp.int32), axis=2) - 1
    first_slot = jnp.max(jnp.where(started, starts[:, None, :], 0), axis=2)
    within = position[None, :] - first_slot
    live_slot = position[None, :] < (starts[:, -1] + counts[:, -1])[:, None]
    flat_index = jnp.where(live_slot, owner_tile * rank_max + within, 0)
    return (flat_index, live_slot)


def take_slots(values, chosen):
    return jnp.take(values, chosen, axis=1)


def per_device(wavefield, u_factors, v_factors, tile_ranks, tile_offsets):
    rec_dev, src_dev, samples = wavefield.shape
    freq_dev = u_factors.shape[1]
    rows_dev = u_factors.shape[2]
    tile_size = u_factors.shape[3]
    slot_count = u_factors.shape[4]
    freq_group = lax.axis_size("freq")
    row_group = lax.axis_size("rows")
    freqs = freq_dev * freq_group
    receivers = rec_dev * freq_group
    columns = receivers // tile_size
    sources = src_dev * row_group
    forward, inverse = spectral_tables(freqs, samples)
    spectrum = jnp.einsum("kct,rst->kcrs", forward, wavefield, preferred_element_type=jnp.float32)
    spectrum = spectrum.astype(jnp.bfloat16).reshape(freqs, 2, rec_dev * src_dev)
    windows = jax.vmap(
        functools.partial(tile_windows, rank_max=RANK_MAX), in_axes=(1, 1, 0), out_axes=(1, 1)
    )
    rank_slots = jnp.arange(RANK_MAX, dtype=jnp.int32)
    tile_row = 0
    v_win, u_win = windows(
        v_factors[:, :, tile_row], u_factors[:, :, tile_row], tile_offsets[:, tile_row]
    )
    rank_mask = rank_slots[None, None, :] < tile_ranks[:, tile_row, :, None]
    flat_index, live_slot = slot_lookup(
        tile_offsets[:, tile_row], tile_ranks[:, tile_row], RANK_MAX, slot_count
    )
    prepared = [(v_win, u_win, rank_mask, flat_index, live_slot)]
    by_frequency = lax.all_to_all(spectrum, "freq", split_axis=0, concat_axis=2, tiled=True)
    portion = lax.all_gather(by_frequency[None], "rows", axis=0, tiled=True)
    blocks_in = portion.shape[0]
    spectra = portion.reshape(blocks_in, freq_dev, 2, columns, tile_size, src_dev)
    spectra = jnp.transpose(spectra, (1, 2, 3, 4, 0, 5)).reshape(
        freq_dev, 2, columns, tile_size, blocks_in * src_dev
    )
    tile_row = 0
    v_win, u_win, rank_mask, flat_index, live_slot = prepared[tile_row]
    quadrants = jnp.einsum(
        "afjmr,fbjrs->fabjms", v_win, spectra, preferred_element_type=jnp.float32
    )
    coeffs = jnp.stack(
        [quadrants[:, 0, 0] - quadrants[:, 1, 1], quadrants[:, 0, 1] + quadrants[:, 1, 0]], axis=1
    )
    coeffs = jnp.where(rank_mask[:, None, :, :, None], coeffs, 0.0).astype(jnp.bfloat16)
    stacked = coeffs.reshape(freq_dev, 2, columns * RANK_MAX, blocks_in * src_dev)
    packed = jax.vmap(take_slots)(stacked, flat_index)
    packed = jnp.where(live_slot[:, None, :, None], packed, jnp.zeros((), jnp.bfloat16))
    products = jnp.einsum(
        "afrk,fcks->facrs", u_factors[:, :, tile_row], packed, preferred_element_type=jnp.float32
    )
    results = [
        jnp.stack(
            [products[:, 0, 0] - products[:, 1, 1], products[:, 0, 1] + products[:, 1, 0]], axis=1
        )
    ]
    merged = jnp.stack(results, axis=2)
    bands = merged.astype(jnp.bfloat16).reshape(
        freq_dev, 2, rows_dev * tile_size, blocks_in, src_dev
    )
    bands = bands.reshape(freq_dev, 2, rows_dev * tile_size * sources)
    returned = lax.all_to_all(bands, "freq", split_axis=2, concat_axis=0, tiled=True)
    series = jnp.einsum("kcq,kct->qt", returned, inverse, preferred_element_type=jnp.float32)
    return series.astype(jnp.bfloat16).reshape(rows_dev * tile_size // freq_group, sources, samples)


def transform_kernel(traces_ref, table_ref, out_ref, rows_ref, turned_ref):
    rows, kinds = rows_ref.shape[0], out_ref.shape[0] * out_ref.shape[1] // SUBLANES
    rows_ref[...] = jnp.dot(traces_ref[...], table_ref[...], preferred_element_type=jnp.float32)
    for source in range(SUBLANES):
        part = rows_ref[pl.ds(source, rows // SUBLANES, stride=SUBLANES), :]
        turned_ref[pl.ds(source, kinds, stride=SUBLANES), :] = part.T[:kinds]
    out_ref[...] = turned_ref[...].astype(jnp.bfloat16).reshape(out_ref.shape)


def transform(traces, table, groups):
    rows, samples = traces.shape
    receivers = rows // SUBLANES
    kinds = table.shape[1]
    padded = jnp.pad(table, ((0, 0), (0, LANES - kinds)))
    block = LANES
    return pl.pallas_call(
        transform_kernel,
        grid=(receivers // block,),
        in_specs=[
            pl.BlockSpec((block * SUBLANES, samples), lambda i: (i, 0)),
            pl.BlockSpec((samples, LANES), lambda i: (0, 0)),
        ],
        out_specs=pl.BlockSpec((groups, kinds * SUBLANES // groups, block), lambda i: (0, 0, i)),
        out_shape=jax.ShapeDtypeStruct(
            (groups, kinds * SUBLANES // groups, receivers), jnp.bfloat16
        ),
        scratch_shapes=[
            pltpu.VMEM((block * SUBLANES, LANES), jnp.float32),
            pltpu.VMEM((kinds * SUBLANES, block), jnp.float32),
        ],
        cost_estimate=pl.CostEstimate(
            flops=2 * rows * samples * LANES, bytes_accessed=rows * samples * 2, transcendentals=0
        ),
        name="transform",
    )(traces, padded)


def coefficient_kernel(
    place_ref, offsets_ref, totals_ref, own_ref, twin_ref, v_ref, v_far_ref, out_ref, far_ref, lhs_ref
):
    groups, rows, receivers = own_ref.shape
    tile = v_ref.shape[3]
    freqs = v_ref.shape[1]
    slots = v_ref.shape[2]
    per_group = receivers // tile
    columns = groups * per_group
    core = place_ref[0]
    half = 2 * SUBLANES
    for k in range(freqs):
        for ref, at in ((own_ref, core), (twin_ref, 1 - core)):
            for column in range(columns):
                group, inner = divmod(column, per_group)
                start = pl.multiple_of(column * 2 * half + at * half, half)
                lhs_ref[k, pl.ds(start, half), :] = ref[
                    group, k * half : (k + 1) * half, inner * tile : (inner + 1) * tile
                ]
    for side, (v, out) in enumerate(((v_ref, out_ref), (v_far_ref, far_ref))):
        for k in range(freqs):
            for low in range(0, slots, tile):
                slot = lax.broadcasted_iota(jnp.int32, (2 * half, tile), 1) + low
                chosen = []
                for part in range(2):
                    products = lax.dot_general(
                        lhs_ref[k],
                        v[part, k, low : low + tile, :],
                        NT,
                        preferred_element_type=jnp.float32,
                    )
                    value = products[: 2 * half]
                    for column in range(1, columns):
                        value = jnp.where(
                            slot >= offsets_ref[side, k, column],
                            products[column * 2 * half : (column + 1) * 2 * half],
                            value,
                        )
                    chosen.append(jnp.where(slot < totals_ref[side, k], value, 0.0))
                by_real, by_imag = chosen
                n = SUBLANES
                real = [by_real[g : g + n] - by_imag[g + n : g + 2 * n] for g in (0, half)]
                imag = [by_real[g + n : g + 2 * n] + by_imag[g : g + n] for g in (0, half)]
                out[k, 0, :, low : low + tile] = jnp.concatenate(real, 0).astype(jnp.bfloat16)
                out[k, 1, :, low : low + tile] = jnp.concatenate(imag, 0).astype(jnp.bfloat16)


def coefficients(place, offsets, totals, own, twin, v_own, v_far):
    freqs, slots = v_own.shape[1], v_own.shape[2]
    tile = v_own.shape[3]
    columns = own.shape[0] * own.shape[2] // tile
    smem = pl.BlockSpec(memory_space=pltpu.SMEM)
    vmem = pl.BlockSpec(memory_space=pltpu.VMEM)
    shape = jax.ShapeDtypeStruct((freqs, 2, 2 * SUBLANES, slots), jnp.bfloat16)
    return pl.pallas_call(
        coefficient_kernel,
        in_specs=[smem] * 3 + [vmem] * 4,
        out_specs=[vmem] * 2,
        out_shape=[shape, shape],
        scratch_shapes=[pltpu.VMEM((freqs, columns * 4 * SUBLANES, tile), jnp.bfloat16)],
        cost_estimate=pl.CostEstimate(
            flops=2 * 4 * freqs * slots * columns * 4 * SUBLANES * tile,
            bytes_accessed=4 * 2**20,
            transcendentals=0,
        ),
        name="coefficients",
    )(place, offsets, totals, own, twin, v_own, v_far)


def band_kernel(place_ref, near_ref, far_ref, u_ref, out_ref, rhs_ref, turned_ref, bands_ref, mix_ref):
    freqs, _, sources, slots = near_ref.shape
    tile = u_ref.shape[2]
    groups = out_ref.shape[0]
    place = place_ref[1]
    wide = 2 * sources
    rhs_ref[...] = jnp.zeros_like(rhs_ref)
    turned_ref[...] = jnp.zeros_like(turned_ref)
    for k in range(freqs):
        for part in range(2):
            for ref, at in ((near_ref, place), (far_ref, 1 - place)):
                value = ref[k, part]
                start = (2 * k + part) * wide + at * sources
                rhs_ref[k, pl.ds(pl.multiple_of(start, sources), sources), :] = value
                start = (2 * k + 1 - part) * wide + at * sources
                turned_ref[k, pl.ds(pl.multiple_of(start, sources), sources), :] = (
                    value if part == 0 else -value
                )
    total = jnp.zeros((tile, 2 * freqs * wide), jnp.float32)
    for k in range(freqs):
        for part, ref in enumerate((rhs_ref, turned_ref)):
            total += lax.dot_general(u_ref[part, k], ref[k], NT, preferred_element_type=jnp.float32)
    bands_ref[...] = total
    packs = LANES // wide
    kinds = 2 * freqs
    block = lax.broadcasted_iota(jnp.int32, (tile // packs, LANES), 1) // wide
    loaded = [bands_ref[pl.ds(b, tile // packs, stride=packs), :] for b in range(packs)]
    rows = tile // packs // groups
    for kind in range(kinds):
        mixed = jnp.zeros((tile // packs, LANES), jnp.float32)
        for b in range(packs):
            shift = (b - kind) * wide % LANES
            moved = pltpu.roll(loaded[b], shift, 1) if shift else loaded[b]
            mixed = jnp.where(block == b, moved, mixed)
        mix_ref[:, kind * rows : (kind + 1) * rows, :] = mixed.reshape(groups, rows, LANES)
    out_ref[...] = mix_ref[...].astype(jnp.bfloat16)


def bands_of(place, near, far, u_own, groups):
    freqs, _, sources, slots = near.shape
    tile = u_own.shape[2]
    kinds = 2 * freqs
    smem = pl.BlockSpec(memory_space=pltpu.SMEM)
    vmem = pl.BlockSpec(memory_space=pltpu.VMEM)
    rows = kinds * tile * 2 * sources // LANES // groups
    return pl.pallas_call(
        band_kernel,
        in_specs=[smem] + [vmem] * 3,
        out_specs=vmem,
        out_shape=jax.ShapeDtypeStruct((groups, rows, LANES), jnp.bfloat16),
        scratch_shapes=[
            pltpu.VMEM((freqs, LANES, slots), jnp.bfloat16),
            pltpu.VMEM((freqs, LANES, slots), jnp.bfloat16),
            pltpu.VMEM((tile, LANES), jnp.float32),
            pltpu.VMEM((groups, rows, LANES), jnp.float32),
        ],
        cost_estimate=pl.CostEstimate(
            flops=2 * 2 * freqs * tile * LANES * slots, bytes_accessed=2**21, transcendentals=0
        ),
        name="bands",
    )(place, near, far, u_own)


def series_kernel(bands_ref, inverse_ref, out_ref, wide_ref):
    groups, rows, lanes = bands_ref.shape
    kinds = inverse_ref.shape[0]
    step = groups * rows // kinds

    @pl.when(pl.program_id(0) == 0)
    def _():
        wide_ref[...] = bands_ref[...].astype(jnp.float32).reshape(groups * rows, lanes)

    part = wide_ref[pl.ds(pl.program_id(0), kinds, stride=step), :]
    out_ref[...] = jnp.dot(
        part.T.astype(jnp.bfloat16), inverse_ref[...], preferred_element_type=jnp.float32
    ).astype(jnp.bfloat16)


def series_of(bands, inverse):
    groups, rows, lanes = bands.shape
    kinds, samples = inverse.shape
    step = groups * rows // kinds
    return pl.pallas_call(
        series_kernel,
        grid=(step,),
        in_specs=[
            pl.BlockSpec(bands.shape, lambda i: (0, 0, 0)),
            pl.BlockSpec(inverse.shape, lambda i: (0, 0)),
        ],
        out_specs=pl.BlockSpec((lanes, samples), lambda i: (i, 0)),
        out_shape=jax.ShapeDtypeStruct((step * lanes, samples), jnp.bfloat16),
        scratch_shapes=[pltpu.VMEM((groups * rows, lanes), jnp.float32)],
        cost_estimate=pl.CostEstimate(
            flops=2 * step * lanes * kinds * samples,
            bytes_accessed=step * lanes * samples * 2,
            transcendentals=0,
        ),
        name="series",
    )(bands, inverse)


def fits(rec_dev, src_dev, freq_dev, rows_dev, tile, slots, freq_group, row_group):
    kinds = 2 * freq_dev * freq_group
    return (
        src_dev == SUBLANES
        and row_group == 4
        and rows_dev == 1
        and rec_dev % tile == 0
        and tile % (4 * LANES // 2) == 0
        and slots % tile == 0
        and kinds <= LANES
        and 2 * freq_dev * src_dev * row_group == LANES
        and tile % (4 * SUBLANES * freq_group) == 0
    )


def per_device_fast(wavefield, u_factors, v_factors, tile_ranks, tile_offsets):
    rec_dev, src_dev, samples = wavefield.shape
    freq_dev = u_factors.shape[1]
    freq_group = lax.axis_size("freq")
    row_group = lax.axis_size("rows")
    freqs = freq_dev * freq_group
    sources = src_dev * row_group
    tile = u_factors.shape[3]
    row = lax.axis_index("rows")
    place = jnp.stack([row % 2, row // 2]).astype(jnp.int32)
    across = [(i, i ^ 2) for i in range(row_group)]
    beside = [(i, i ^ 1) for i in range(row_group)]
    forward, inverse = spectral_tables(freqs, samples)
    u_own, v_own = u_factors[:, :, 0], v_factors[:, :, 0]
    v_far = lax.ppermute(v_own, "rows", across)
    offsets = tile_offsets[:, 0]
    ends = (offsets[:, -1] + tile_ranks[:, 0, -1])[:, None]
    lookup = jnp.concatenate([offsets, ends], axis=1)
    lookup = jnp.stack([lookup, lax.ppermute(lookup, "rows", across)])
    table = forward.reshape(2 * freqs, samples).T
    spectrum = transform(wavefield.reshape(rec_dev * src_dev, samples), table, freq_group)
    own = lax.all_to_all(spectrum, "freq", split_axis=0, concat_axis=0, tiled=True)
    twin = lax.ppermute(own, "rows", beside)
    near, leaving = coefficients(place, lookup, lookup[:, :, -1], own, twin, v_own, v_far)
    far = lax.ppermute(leaving, "rows", across)
    bands = bands_of(place, near, far, u_own, freq_group)
    returned = lax.all_to_all(bands, "freq", split_axis=0, concat_axis=0, tiled=True)
    series = series_of(returned, inverse.reshape(2 * freqs, samples))
    return series.reshape(tile // freq_group, sources, samples)


def choose(wavefield, u_factors, v_factors, tile_ranks, tile_offsets):
    ok = fits(
        wavefield.shape[0],
        wavefield.shape[1],
        u_factors.shape[1],
        u_factors.shape[2],
        u_factors.shape[3],
        u_factors.shape[4],
        lax.axis_size("freq"),
        lax.axis_size("rows"),
    )
    step = per_device_fast if ok else per_device
    return step(wavefield, u_factors, v_factors, tile_ranks, tile_offsets)


def solution(mesh):
    placed = (
        P("freq", "rows", None),
        P(None, "freq", "rows", None, None),
        P(None, "freq", "rows", None, None),
        P("freq", "rows", None),
        P("freq", "rows", None),
    )
    return jax.shard_map(
        choose,
        mesh=mesh,
        in_specs=placed,
        out_specs=P(("rows", "freq"), None, None),
        check_vma=False,
    )
```

```python
import functools
import math

import jax
import jax.numpy as jnp
from jax import lax
from jax.experimental import pallas as pl
from jax.experimental.pallas import tpu as pltpu
from jax.sharding import PartitionSpec as P

RANK_MAX = 64
LANES = 128
SUBLANES = 8
NT = (((1,), (1,)), ((), ()))
VMEM = pl.BlockSpec(memory_space=pltpu.VMEM)
SMEM = pl.BlockSpec(memory_space=pltpu.SMEM)
EARLY = 5


def spectral_tables(freq_count, sample_count):
    freq_bins = jnp.arange(freq_count, dtype=jnp.int32) + 1
    sample_index = jnp.arange(sample_count, dtype=jnp.int32)
    phase_int = freq_bins[:, None] * sample_index[None, :] % sample_count
    angles = phase_int.astype(jnp.float32) * (2.0 * math.pi / sample_count)
    cosine = jnp.cos(angles)
    minus_sine = -jnp.sin(angles)
    stacked = jnp.stack([cosine, minus_sine], axis=1)
    forward = (stacked / math.sqrt(sample_count)).astype(jnp.bfloat16)
    inverse = (stacked / math.sqrt(freq_count)).astype(jnp.bfloat16)
    return (forward, inverse)


def tile_windows(v_row, u_row, starts, rank_max):
    columns = starts.shape[0]
    slot_index = (starts[:, None] + jnp.arange(rank_max, dtype=jnp.int32)[None, :]).reshape(-1)
    v_padded = jnp.pad(v_row, ((0, 0), (0, rank_max), (0, 0)))
    u_padded = jnp.pad(u_row, ((0, 0), (0, 0), (0, rank_max)))
    v_win = jnp.take(v_padded, slot_index, axis=1).reshape(2, columns, rank_max, v_row.shape[2])
    u_win = jnp.take(u_padded, slot_index, axis=2).reshape(2, u_row.shape[1], columns, rank_max)
    return (v_win, u_win)


def slot_lookup(starts, counts, rank_max, slot_count):
    position = jnp.arange(slot_count, dtype=jnp.int32)
    started = starts[:, None, :] <= position[None, :, None]
    owner_tile = jnp.sum(started.astype(jnp.int32), axis=2) - 1
    first_slot = jnp.max(jnp.where(started, starts[:, None, :], 0), axis=2)
    within = position[None, :] - first_slot
    live_slot = position[None, :] < (starts[:, -1] + counts[:, -1])[:, None]
    flat_index = jnp.where(live_slot, owner_tile * rank_max + within, 0)
    return (flat_index, live_slot)


def take_slots(values, chosen):
    return jnp.take(values, chosen, axis=1)


def per_device(wavefield, u_factors, v_factors, tile_ranks, tile_offsets):
    rec_dev, src_dev, samples = wavefield.shape
    freq_dev = u_factors.shape[1]
    rows_dev = u_factors.shape[2]
    tile_size = u_factors.shape[3]
    slot_count = u_factors.shape[4]
    freq_group = lax.axis_size("freq")
    row_group = lax.axis_size("rows")
    freqs = freq_dev * freq_group
    receivers = rec_dev * freq_group
    columns = receivers // tile_size
    sources = src_dev * row_group
    forward, inverse = spectral_tables(freqs, samples)
    spectrum = jnp.einsum("kct,rst->kcrs", forward, wavefield, preferred_element_type=jnp.float32)
    spectrum = spectrum.astype(jnp.bfloat16).reshape(freqs, 2, rec_dev * src_dev)
    windows = jax.vmap(
        functools.partial(tile_windows, rank_max=RANK_MAX), in_axes=(1, 1, 0), out_axes=(1, 1)
    )
    rank_slots = jnp.arange(RANK_MAX, dtype=jnp.int32)
    tile_row = 0
    v_win, u_win = windows(
        v_factors[:, :, tile_row], u_factors[:, :, tile_row], tile_offsets[:, tile_row]
    )
    rank_mask = rank_slots[None, None, :] < tile_ranks[:, tile_row, :, None]
    flat_index, live_slot = slot_lookup(
        tile_offsets[:, tile_row], tile_ranks[:, tile_row], RANK_MAX, slot_count
    )
    prepared = [(v_win, u_win, rank_mask, flat_index, live_slot)]
    by_frequency = lax.all_to_all(spectrum, "freq", split_axis=0, concat_axis=2, tiled=True)
    portion = lax.all_gather(by_frequency[None], "rows", axis=0, tiled=True)
    blocks_in = portion.shape[0]
    spectra = portion.reshape(blocks_in, freq_dev, 2, columns, tile_size, src_dev)
    spectra = jnp.transpose(spectra, (1, 2, 3, 4, 0, 5)).reshape(
        freq_dev, 2, columns, tile_size, blocks_in * src_dev
    )
    tile_row = 0
    v_win, u_win, rank_mask, flat_index, live_slot = prepared[tile_row]
    quadrants = jnp.einsum(
        "afjmr,fbjrs->fabjms", v_win, spectra, preferred_element_type=jnp.float32
    )
    coeffs = jnp.stack(
        [quadrants[:, 0, 0] - quadrants[:, 1, 1], quadrants[:, 0, 1] + quadrants[:, 1, 0]], axis=1
    )
    coeffs = jnp.where(rank_mask[:, None, :, :, None], coeffs, 0.0).astype(jnp.bfloat16)
    stacked = coeffs.reshape(freq_dev, 2, columns * RANK_MAX, blocks_in * src_dev)
    packed = jax.vmap(take_slots)(stacked, flat_index)
    packed = jnp.where(live_slot[:, None, :, None], packed, jnp.zeros((), jnp.bfloat16))
    products = jnp.einsum(
        "afrk,fcks->facrs", u_factors[:, :, tile_row], packed, preferred_element_type=jnp.float32
    )
    results = [
        jnp.stack(
            [products[:, 0, 0] - products[:, 1, 1], products[:, 0, 1] + products[:, 1, 0]], axis=1
        )
    ]
    merged = jnp.stack(results, axis=2)
    bands = merged.astype(jnp.bfloat16).reshape(
        freq_dev, 2, rows_dev * tile_size, blocks_in, src_dev
    )
    bands = bands.reshape(freq_dev, 2, rows_dev * tile_size * sources)
    returned = lax.all_to_all(bands, "freq", split_axis=2, concat_axis=0, tiled=True)
    series = jnp.einsum("kcq,kct->qt", returned, inverse, preferred_element_type=jnp.float32)
    return series.astype(jnp.bfloat16).reshape(rows_dev * tile_size // freq_group, sources, samples)


def transform_kernel(traces_ref, table_ref, *refs):
    groups = lax.axis_size("freq")
    outs, (traces, sems, first, second, turned) = refs[:groups], refs[groups:]
    me = lax.axis_index("freq")
    kinds = table_ref.shape[0]
    rows = first.shape[0]
    blocks = traces_ref.shape[0] // rows
    each = outs[0].shape[0]

    def copy(i):
        part = pl.ds(pl.multiple_of(i * rows, rows), rows)
        return pltpu.make_async_copy(traces_ref.at[part, :], traces.at[part, :], sems.at[i])

    def multiply(i, into):
        copy(i).wait()
        part = pl.ds(pl.multiple_of(i * rows, rows), rows)
        into[:, :kinds] = lax.dot_general(
            traces[part, :], table_ref[...], NT, preferred_element_type=jnp.float32
        )

    def turn(i, source_rows):
        for source in range(SUBLANES):
            part = source_rows[pl.ds(source, rows // SUBLANES, stride=SUBLANES), :]
            turned[pl.ds(source, kinds, stride=SUBLANES), :] = part.T[:kinds]
        lanes = pl.ds(pl.multiple_of(i * LANES, LANES), LANES)
        for shift, out in enumerate(outs):
            group = lax.rem(me + shift, groups)
            start = pl.multiple_of(group * each, each)
            out[:, lanes] = turned[pl.ds(start, each), :].astype(jnp.bfloat16)

    for i in range(blocks):
        copy(i).start()
    multiply(0, first)

    def pair(p, carry):
        multiply(2 * p + 1, second)
        turn(2 * p, first)
        multiply(2 * p + 2, first)
        turn(2 * p + 1, second)
        return carry

    lax.fori_loop(0, (blocks - 1) // 2, pair, 0)
    if blocks % 2 == 0:
        multiply(blocks - 1, second)
        turn(blocks - 2, first)
        turn(blocks - 1, second)
    else:
        turn(blocks - 1, first)


def transform(traces, table, groups):
    rows, samples = traces.shape
    receivers = rows // SUBLANES
    kinds = table.shape[0]
    shape = jax.ShapeDtypeStruct((kinds * SUBLANES // groups, receivers), jnp.bfloat16)
    return pl.pallas_call(
        transform_kernel,
        in_specs=[pl.BlockSpec(memory_space=pltpu.HBM), VMEM],
        out_specs=[VMEM] * groups,
        out_shape=[shape] * groups,
        scratch_shapes=[
            pltpu.VMEM((rows, samples), jnp.bfloat16),
            pltpu.SemaphoreType.DMA((receivers // LANES,)),
            pltpu.VMEM((LANES * SUBLANES, LANES), jnp.float32),
            pltpu.VMEM((LANES * SUBLANES, LANES), jnp.float32),
            pltpu.VMEM((kinds * SUBLANES, LANES), jnp.float32),
        ],
        compiler_params=pltpu.CompilerParams(vmem_limit_bytes=rows * samples * 2 + 6 * 2**20),
        cost_estimate=pl.CostEstimate(
            flops=2 * rows * samples * 256, bytes_accessed=rows * samples * 2, transcendentals=0
        ),
        name="transform",
    )(traces, table)


def coefficient_kernel(shifts, sides, before, *refs):
    count = len(shifts)
    refs = list(refs)
    offsets = [refs.pop(0) for _ in range(sides)]
    own = [refs.pop(0) for _ in range(count)]
    twin = [refs.pop(0) for _ in range(count)]
    factors = [refs.pop(0) for _ in range(sides)]
    earlier = [refs.pop(0) for _ in range(before)]
    outs = [refs.pop(0) for _ in range(sides)]
    (lhs,) = refs
    groups = lax.axis_size("freq")
    me = lax.axis_index("freq")
    core = lax.rem(lax.axis_index("rows"), 2)
    _, freqs, slots, tile = factors[0].shape
    per_block = own[0].shape[1] // tile
    columns = groups * per_block
    half = 2 * SUBLANES
    deep = 2 * half
    for k in range(freqs):
        for arrays, at in ((own, core), (twin, 1 - core)):
            for b in range(count):
                for inner in range(per_block):
                    start = (b * per_block + inner) * deep + at * half
                    lhs[k, pl.ds(pl.multiple_of(start, half), half), :] = arrays[b][
                        k * half : (k + 1) * half, inner * tile : (inner + 1) * tile
                    ]
    for side in range(sides):
        for k in range(freqs):
            for low in range(0, slots, tile):
                slot = lax.broadcasted_iota(jnp.int32, (deep, tile), 1) + low
                chosen = []
                for part in range(2):
                    products = lax.dot_general(
                        lhs[k],
                        factors[side][part, k, low : low + tile, :],
                        NT,
                        preferred_element_type=jnp.float32,
                    )
                    total = jnp.zeros((deep, tile), jnp.float32)
                    for b, shift in enumerate(shifts):
                        column = lax.rem(me + groups - shift, groups) * per_block
                        value = total
                        for inner in range(per_block):
                            at = (b * per_block + inner) * deep
                            value = jnp.where(
                                slot >= offsets[side][k, 0, column + inner],
                                products[at : at + deep],
                                value,
                            )
                        after = jnp.minimum(column + per_block, columns - 1)
                        end = jnp.where(
                            column + per_block < columns, offsets[side][k, 0, after], slots
                        )
                        total = jnp.where(slot >= end, total, value)
                    chosen.append(total)
                by_real, by_imag = chosen
                n = SUBLANES
                real = [by_real[g : g + n] - by_imag[g + n : g + 2 * n] for g in (0, half)]
                imag = [by_real[g + n : g + 2 * n] + by_imag[g : g + n] for g in (0, half)]
                for c, pieces in enumerate((real, imag)):
                    value = jnp.concatenate(pieces, 0)
                    if side < before:
                        value += earlier[side][k, c, :, low : low + tile].astype(jnp.float32)
                    outs[side][k, c, :, low : low + tile] = value.astype(jnp.bfloat16)


def coefficients(shifts, offsets, own, twin, factors, earlier=()):
    sides, count = len(offsets), len(shifts)
    _, freqs, slots, tile = factors[0].shape
    columns = count * own[0].shape[1] // tile
    shape = jax.ShapeDtypeStruct((freqs, 2, 2 * SUBLANES, slots), jnp.bfloat16)
    return pl.pallas_call(
        functools.partial(coefficient_kernel, tuple(shifts), sides, len(earlier)),
        in_specs=[SMEM] * sides + [VMEM] * (2 * count + sides + len(earlier)),
        out_specs=[VMEM] * sides,
        out_shape=[shape] * sides,
        scratch_shapes=[pltpu.VMEM((freqs, columns * 4 * SUBLANES, tile), jnp.bfloat16)],
        compiler_params=pltpu.CompilerParams(vmem_limit_bytes=16 * 2**20),
        cost_estimate=pl.CostEstimate(
            flops=2 * 2 * sides * freqs * slots * columns * 4 * SUBLANES * tile,
            bytes_accessed=2**20,
            transcendentals=0,
        ),
        name="coefficients",
    )(*offsets, *own, *twin, *factors, *earlier)


def band_kernel(offsets_ref, ranks_ref, near_ref, far_ref, u_ref, out_ref, rhs, crossed, bands, mix):
    freqs, _, sources, slots = near_ref.shape
    tile = u_ref.shape[2]
    groups = out_ref.shape[0]
    place = lax.rem(lax.axis_index("rows") // 2, 2)
    last = offsets_ref.shape[2] - 1
    wide = 2 * sources
    rhs[...] = jnp.zeros_like(rhs)
    crossed[...] = jnp.zeros_like(crossed)
    slot = lax.broadcasted_iota(jnp.int32, (sources, slots), 1)
    for k in range(freqs):
        live = slot < offsets_ref[k, 0, last] + ranks_ref[k, 0, last]
        for part in range(2):
            for ref, at in ((near_ref, place), (far_ref, 1 - place)):
                value = jnp.where(live, ref[k, part].astype(jnp.float32), 0.0)
                start = pl.multiple_of((2 * k + part) * wide + at * sources, sources)
                rhs[k, pl.ds(start, sources), :] = value.astype(jnp.bfloat16)
                start = pl.multiple_of((2 * k + 1 - part) * wide + at * sources, sources)
                value = value if part == 0 else -value
                crossed[k, pl.ds(start, sources), :] = value.astype(jnp.bfloat16)
    total = jnp.zeros((tile, 2 * freqs * wide), jnp.float32)
    for k in range(freqs):
        for part, ref in enumerate((rhs, crossed)):
            total += lax.dot_general(u_ref[part, k], ref[k], NT, preferred_element_type=jnp.float32)
    bands[...] = total
    packs = LANES // wide
    kinds = 2 * freqs
    block = lax.broadcasted_iota(jnp.int32, (tile // packs, LANES), 1) // wide
    loaded = [bands[pl.ds(b, tile // packs, stride=packs), :] for b in range(packs)]
    rows = tile // packs // groups
    for kind in range(kinds):
        mixed = jnp.zeros((tile // packs, LANES), jnp.float32)
        for b in range(packs):
            shift = (b - kind) * wide % LANES
            moved = pltpu.roll(loaded[b], shift, 1) if shift else loaded[b]
            mixed = jnp.where(block == b, moved, mixed)
        mix[:, kind * rows : (kind + 1) * rows, :] = mixed.reshape(groups, rows, LANES)
    out_ref[...] = mix[...].astype(jnp.bfloat16)


def bands_of(offsets, ranks, near, far, u_own, groups):
    freqs, _, sources, slots = near.shape
    tile = u_own.shape[2]
    kinds = 2 * freqs
    rows = kinds * tile * 2 * sources // LANES // groups
    return pl.pallas_call(
        band_kernel,
        in_specs=[SMEM] * 2 + [VMEM] * 3,
        out_specs=VMEM,
        out_shape=jax.ShapeDtypeStruct((groups, rows, LANES), jnp.bfloat16),
        scratch_shapes=[
            pltpu.VMEM((freqs, LANES, slots), jnp.bfloat16),
            pltpu.VMEM((freqs, LANES, slots), jnp.bfloat16),
            pltpu.VMEM((tile, LANES), jnp.float32),
            pltpu.VMEM((groups, rows, LANES), jnp.float32),
        ],
        compiler_params=pltpu.CompilerParams(vmem_limit_bytes=8 * 2**20),
        cost_estimate=pl.CostEstimate(
            flops=2 * 2 * freqs * tile * LANES * slots, bytes_accessed=2**21, transcendentals=0
        ),
        name="bands",
    )(offsets, ranks, near, far, u_own)


def series_kernel(bands_ref, inverse_ref, out_ref, wide, done, sems):
    groups, rows, lanes = bands_ref.shape
    kinds = inverse_ref.shape[0]
    steps = groups * rows // kinds
    wide[...] = bands_ref[...].astype(jnp.float32).reshape(groups * rows, lanes)
    copies = []
    for i in range(steps):
        part = wide[pl.ds(i, kinds, stride=steps), :]
        done[i] = jnp.dot(
            part.T.astype(jnp.bfloat16), inverse_ref[...], preferred_element_type=jnp.float32
        ).astype(jnp.bfloat16)
        copies.append(
            pltpu.make_async_copy(
                done.at[i], out_ref.at[i * lanes : (i + 1) * lanes, :], sems.at[i]
            )
        )
        copies[-1].start()
    for copy in copies:
        copy.wait()


def series_of(bands, inverse):
    groups, rows, lanes = bands.shape
    kinds, samples = inverse.shape
    steps = groups * rows // kinds
    return pl.pallas_call(
        series_kernel,
        in_specs=[VMEM] * 2,
        out_specs=pl.BlockSpec(memory_space=pl.ANY),
        out_shape=jax.ShapeDtypeStruct((steps * lanes, samples), jnp.bfloat16),
        scratch_shapes=[
            pltpu.VMEM((groups * rows, lanes), jnp.float32),
            pltpu.VMEM((steps, lanes, samples), jnp.bfloat16),
            pltpu.SemaphoreType.DMA((steps,)),
        ],
        compiler_params=pltpu.CompilerParams(vmem_limit_bytes=16 * 2**20),
        cost_estimate=pl.CostEstimate(
            flops=2 * steps * lanes * kinds * samples,
            bytes_accessed=steps * lanes * samples * 2,
            transcendentals=0,
        ),
        name="series",
    )(bands, inverse)


def fits(rec_dev, src_dev, freq_dev, rows_dev, tile, slots, freq_group, row_group):
    kinds = 2 * freq_dev * freq_group
    return (
        src_dev == SUBLANES
        and row_group == 4
        and rows_dev == 1
        and freq_group > 1
        and rec_dev % tile == 0
        and tile % (2 * LANES) == 0
        and slots % tile == 0
        and kinds <= LANES
        and 2 * freq_dev * src_dev * row_group == LANES
        and tile % (4 * SUBLANES * freq_group) == 0
    )


def per_device_fast(wavefield, u_factors, v_factors, tile_ranks, tile_offsets):
    rec_dev, src_dev, samples = wavefield.shape
    freq_dev = u_factors.shape[1]
    groups = lax.axis_size("freq")
    row_group = lax.axis_size("rows")
    freqs = freq_dev * groups
    sources = src_dev * row_group
    tile = u_factors.shape[3]
    across = [(i, i ^ 2) for i in range(row_group)]
    beside = [(i, i ^ 1) for i in range(row_group)]
    forward, inverse = spectral_tables(freqs, samples)
    u_own, v_own = u_factors[:, :, 0], v_factors[:, :, 0]
    v_far = lax.ppermute(v_own, "rows", across)
    offsets_far = lax.ppermute(tile_offsets, "rows", across)
    table = forward.reshape(2 * freqs, samples)
    sent = transform(wavefield.reshape(rec_dev * src_dev, samples), table, groups)
    order = sorted(range(1, groups), key=lambda s: abs(2 * s - groups))
    own = [sent[0]]
    for shift in order:
        ring = [(i, (i + shift) % groups) for i in range(groups)]
        own.append(lax.ppermute(sent[shift], "freq", ring))
    twin = [lax.ppermute(block, "rows", beside) for block in own]
    shifts = [0] + order
    cut = EARLY
    a, b = slice(0, cut), slice(cut, groups)
    (near,) = coefficients(shifts[a], [tile_offsets], own[a], twin[a], [v_own])
    (leaving,) = coefficients(shifts[a], [offsets_far], own[a], twin[a], [v_far])
    near, leaving = coefficients(
        shifts[b], [tile_offsets, offsets_far], own[b], twin[b], [v_own, v_far], [near, leaving]
    )
    far = lax.ppermute(leaving, "rows", across)
    bands = bands_of(tile_offsets, tile_ranks, near, far, u_own, groups)
    returned = lax.all_to_all(bands, "freq", split_axis=0, concat_axis=0, tiled=True)
    series = series_of(returned, inverse.reshape(2 * freqs, samples))
    return series.reshape(tile // groups, sources, samples)


def choose(wavefield, u_factors, v_factors, tile_ranks, tile_offsets):
    ok = fits(
        wavefield.shape[0],
        wavefield.shape[1],
        u_factors.shape[1],
        u_factors.shape[2],
        u_factors.shape[3],
        u_factors.shape[4],
        lax.axis_size("freq"),
        lax.axis_size("rows"),
    )
    step = per_device_fast if ok else per_device
    return step(wavefield, u_factors, v_factors, tile_ranks, tile_offsets)


def solution(mesh):
    placed = (
        P("freq", "rows", None),
        P(None, "freq", "rows", None, None),
        P(None, "freq", "rows", None, None),
        P("freq", "rows", None),
        P("freq", "rows", None),
    )
    return jax.shard_map(
        choose,
        mesh=mesh,
        in_specs=placed,
        out_specs=P(("rows", "freq"), None, None),
        check_vma=False,
    )
```

```python
import functools
import math

import jax
import jax.numpy as jnp
from jax import lax
from jax.experimental import pallas as pl
from jax.experimental.pallas import tpu as pltpu
from jax.sharding import PartitionSpec as P

RANK_MAX = 64
LANES = 128
SUBLANES = 8
NT = (((1,), (1,)), ((), ()))
VMEM = pl.BlockSpec(memory_space=pltpu.VMEM)
SMEM = pl.BlockSpec(memory_space=pltpu.SMEM)
EARLY = 5
AHEAD = 3


def spectral_tables(freq_count, sample_count):
    freq_bins = jnp.arange(freq_count, dtype=jnp.int32) + 1
    sample_index = jnp.arange(sample_count, dtype=jnp.int32)
    phase_int = freq_bins[:, None] * sample_index[None, :] % sample_count
    angles = phase_int.astype(jnp.float32) * (2.0 * math.pi / sample_count)
    cosine = jnp.cos(angles)
    minus_sine = -jnp.sin(angles)
    stacked = jnp.stack([cosine, minus_sine], axis=1)
    forward = (stacked / math.sqrt(sample_count)).astype(jnp.bfloat16)
    inverse = (stacked / math.sqrt(freq_count)).astype(jnp.bfloat16)
    return (forward, inverse)


def tile_windows(v_row, u_row, starts, rank_max):
    columns = starts.shape[0]
    slot_index = (starts[:, None] + jnp.arange(rank_max, dtype=jnp.int32)[None, :]).reshape(-1)
    v_padded = jnp.pad(v_row, ((0, 0), (0, rank_max), (0, 0)))
    u_padded = jnp.pad(u_row, ((0, 0), (0, 0), (0, rank_max)))
    v_win = jnp.take(v_padded, slot_index, axis=1).reshape(2, columns, rank_max, v_row.shape[2])
    u_win = jnp.take(u_padded, slot_index, axis=2).reshape(2, u_row.shape[1], columns, rank_max)
    return (v_win, u_win)


def slot_lookup(starts, counts, rank_max, slot_count):
    position = jnp.arange(slot_count, dtype=jnp.int32)
    started = starts[:, None, :] <= position[None, :, None]
    owner_tile = jnp.sum(started.astype(jnp.int32), axis=2) - 1
    first_slot = jnp.max(jnp.where(started, starts[:, None, :], 0), axis=2)
    within = position[None, :] - first_slot
    live_slot = position[None, :] < (starts[:, -1] + counts[:, -1])[:, None]
    flat_index = jnp.where(live_slot, owner_tile * rank_max + within, 0)
    return (flat_index, live_slot)


def take_slots(values, chosen):
    return jnp.take(values, chosen, axis=1)


def per_device(wavefield, u_factors, v_factors, tile_ranks, tile_offsets):
    rec_dev, src_dev, samples = wavefield.shape
    freq_dev = u_factors.shape[1]
    rows_dev = u_factors.shape[2]
    tile_size = u_factors.shape[3]
    slot_count = u_factors.shape[4]
    freq_group = lax.axis_size("freq")
    row_group = lax.axis_size("rows")
    freqs = freq_dev * freq_group
    receivers = rec_dev * freq_group
    columns = receivers // tile_size
    sources = src_dev * row_group
    forward, inverse = spectral_tables(freqs, samples)
    spectrum = jnp.einsum("kct,rst->kcrs", forward, wavefield, preferred_element_type=jnp.float32)
    spectrum = spectrum.astype(jnp.bfloat16).reshape(freqs, 2, rec_dev * src_dev)
    windows = jax.vmap(
        functools.partial(tile_windows, rank_max=RANK_MAX), in_axes=(1, 1, 0), out_axes=(1, 1)
    )
    rank_slots = jnp.arange(RANK_MAX, dtype=jnp.int32)
    tile_row = 0
    v_win, u_win = windows(
        v_factors[:, :, tile_row], u_factors[:, :, tile_row], tile_offsets[:, tile_row]
    )
    rank_mask = rank_slots[None, None, :] < tile_ranks[:, tile_row, :, None]
    flat_index, live_slot = slot_lookup(
        tile_offsets[:, tile_row], tile_ranks[:, tile_row], RANK_MAX, slot_count
    )
    prepared = [(v_win, u_win, rank_mask, flat_index, live_slot)]
    by_frequency = lax.all_to_all(spectrum, "freq", split_axis=0, concat_axis=2, tiled=True)
    portion = lax.all_gather(by_frequency[None], "rows", axis=0, tiled=True)
    blocks_in = portion.shape[0]
    spectra = portion.reshape(blocks_in, freq_dev, 2, columns, tile_size, src_dev)
    spectra = jnp.transpose(spectra, (1, 2, 3, 4, 0, 5)).reshape(
        freq_dev, 2, columns, tile_size, blocks_in * src_dev
    )
    tile_row = 0
    v_win, u_win, rank_mask, flat_index, live_slot = prepared[tile_row]
    quadrants = jnp.einsum(
        "afjmr,fbjrs->fabjms", v_win, spectra, preferred_element_type=jnp.float32
    )
    coeffs = jnp.stack(
        [quadrants[:, 0, 0] - quadrants[:, 1, 1], quadrants[:, 0, 1] + quadrants[:, 1, 0]], axis=1
    )
    coeffs = jnp.where(rank_mask[:, None, :, :, None], coeffs, 0.0).astype(jnp.bfloat16)
    stacked = coeffs.reshape(freq_dev, 2, columns * RANK_MAX, blocks_in * src_dev)
    packed = jax.vmap(take_slots)(stacked, flat_index)
    packed = jnp.where(live_slot[:, None, :, None], packed, jnp.zeros((), jnp.bfloat16))
    products = jnp.einsum(
        "afrk,fcks->facrs", u_factors[:, :, tile_row], packed, preferred_element_type=jnp.float32
    )
    results = [
        jnp.stack(
            [products[:, 0, 0] - products[:, 1, 1], products[:, 0, 1] + products[:, 1, 0]], axis=1
        )
    ]
    merged = jnp.stack(results, axis=2)
    bands = merged.astype(jnp.bfloat16).reshape(
        freq_dev, 2, rows_dev * tile_size, blocks_in, src_dev
    )
    bands = bands.reshape(freq_dev, 2, rows_dev * tile_size * sources)
    returned = lax.all_to_all(bands, "freq", split_axis=2, concat_axis=0, tiled=True)
    series = jnp.einsum("kcq,kct->qt", returned, inverse, preferred_element_type=jnp.float32)
    return series.astype(jnp.bfloat16).reshape(rows_dev * tile_size // freq_group, sources, samples)


def transform_kernel(traces_ref, table_ref, *refs):
    groups = lax.axis_size("freq")
    outs, (traces, sems, products, turned) = refs[:groups], refs[groups:]
    me = lax.axis_index("freq")
    rows = products.shape[1]
    kinds = turned.shape[0] // SUBLANES
    packs = LANES // kinds
    blocks = traces_ref.shape[0] // rows
    each = outs[0].shape[0]

    def copy(i):
        part = pl.ds(pl.multiple_of(i * rows, rows), rows)
        return pltpu.make_async_copy(traces_ref.at[part, :], traces.at[part, :], sems.at[i])

    def turn(i, source_rows):
        place = lax.broadcasted_iota(jnp.int32, (rows // SUBLANES, LANES), 1) // kinds
        for first in range(0, SUBLANES, packs):
            mixed = source_rows[pl.ds(first, rows // SUBLANES, stride=SUBLANES), :]
            for m in range(1, packs):
                part = source_rows[pl.ds(first + m, rows // SUBLANES, stride=SUBLANES), :]
                mixed = jnp.where(place == m, part, mixed)
            mixed = mixed.T
            for m in range(packs):
                turned[pl.ds(first + m, kinds, stride=SUBLANES), :] = mixed[
                    m * kinds : (m + 1) * kinds
                ]
        lanes = pl.ds(pl.multiple_of(i * LANES, LANES), LANES)
        for shift, out in enumerate(outs):
            group = lax.rem(me + shift, groups)
            start = pl.multiple_of(group * each, each)
            out[:, lanes] = turned[pl.ds(start, each), :].astype(jnp.bfloat16)

    for i in range(min(AHEAD, blocks)):
        copy(i).start()

    def step(i, carry):
        now = lax.rem(i, 2)

        @pl.when(i + AHEAD < blocks)
        def _():
            copy(i + AHEAD).start()

        copy(i).wait()
        part = pl.ds(pl.multiple_of(i * rows, rows), rows)
        products[now] = lax.dot_general(
            traces[part, :], table_ref[...], NT, preferred_element_type=jnp.float32
        )
        turn(jnp.maximum(i - 1, 0), products.at[1 - now])
        return carry

    lax.fori_loop(0, blocks, step, 0)
    turn(blocks - 1, products.at[(blocks - 1) % 2])


def transform(traces, table, groups):
    rows, samples = traces.shape
    receivers = rows // SUBLANES
    kinds = table.shape[0]
    repeated = jnp.tile(table, (LANES // kinds, 1))
    shape = jax.ShapeDtypeStruct((kinds * SUBLANES // groups, receivers), jnp.bfloat16)
    return pl.pallas_call(
        transform_kernel,
        in_specs=[pl.BlockSpec(memory_space=pltpu.HBM), VMEM],
        out_specs=[VMEM] * groups,
        out_shape=[shape] * groups,
        scratch_shapes=[
            pltpu.VMEM((rows, samples), jnp.bfloat16),
            pltpu.SemaphoreType.DMA((receivers // LANES,)),
            pltpu.VMEM((2, LANES * SUBLANES, LANES), jnp.float32),
            pltpu.VMEM((kinds * SUBLANES, LANES), jnp.float32),
        ],
        compiler_params=pltpu.CompilerParams(vmem_limit_bytes=48 * 2**20),
        cost_estimate=pl.CostEstimate(
            flops=2 * rows * samples * 256, bytes_accessed=rows * samples * 2, transcendentals=0
        ),
        name="transform",
    )(traces, repeated)


def coefficient_kernel(shifts, sides, before, *refs):
    count = len(shifts)
    refs = list(refs)
    offsets = [refs.pop(0) for _ in range(sides)]
    own = [refs.pop(0) for _ in range(count)]
    twin = [refs.pop(0) for _ in range(count)]
    factors = [refs.pop(0) for _ in range(sides)]
    earlier = [refs.pop(0) for _ in range(before)]
    outs = [refs.pop(0) for _ in range(sides)]
    (lhs,) = refs
    groups = lax.axis_size("freq")
    me = lax.axis_index("freq")
    core = lax.rem(lax.axis_index("rows"), 2)
    _, freqs, slots, tile = factors[0].shape
    per_block = own[0].shape[1] // tile
    columns = groups * per_block
    half = 2 * SUBLANES
    deep = 2 * half
    for k in range(freqs):
        for arrays, at in ((own, core), (twin, 1 - core)):
            for b in range(count):
                for inner in range(per_block):
                    start = (b * per_block + inner) * deep + at * half
                    lhs[k, pl.ds(pl.multiple_of(start, half), half), :] = arrays[b][
                        k * half : (k + 1) * half, inner * tile : (inner + 1) * tile
                    ]
    for side in range(sides):
        for k in range(freqs):
            for low in range(0, slots, tile):
                slot = lax.broadcasted_iota(jnp.int32, (deep, tile), 1) + low
                chosen = []
                for part in range(2):
                    products = lax.dot_general(
                        lhs[k],
                        factors[side][part, k, low : low + tile, :],
                        NT,
                        preferred_element_type=jnp.float32,
                    )
                    total = jnp.zeros((deep, tile), jnp.float32)
                    for b, shift in enumerate(shifts):
                        column = lax.rem(me + groups - shift, groups) * per_block
                        value = total
                        for inner in range(per_block):
                            at = (b * per_block + inner) * deep
                            value = jnp.where(
                                slot >= offsets[side][k, 0, column + inner],
                                products[at : at + deep],
                                value,
                            )
                        after = jnp.minimum(column + per_block, columns - 1)
                        end = jnp.where(
                            column + per_block < columns, offsets[side][k, 0, after], slots
                        )
                        total = jnp.where(slot >= end, total, value)
                    chosen.append(total)
                by_real, by_imag = chosen
                n = SUBLANES
                real = [by_real[g : g + n] - by_imag[g + n : g + 2 * n] for g in (0, half)]
                imag = [by_real[g + n : g + 2 * n] + by_imag[g : g + n] for g in (0, half)]
                for c, pieces in enumerate((real, imag)):
                    value = jnp.concatenate(pieces, 0)
                    if side < before:
                        value += earlier[side][k, c, :, low : low + tile].astype(jnp.float32)
                    outs[side][k, c, :, low : low + tile] = value.astype(jnp.bfloat16)


def coefficients(shifts, offsets, own, twin, factors, earlier=()):
    sides, count = len(offsets), len(shifts)
    _, freqs, slots, tile = factors[0].shape
    columns = count * own[0].shape[1] // tile
    shape = jax.ShapeDtypeStruct((freqs, 2, 2 * SUBLANES, slots), jnp.bfloat16)
    return pl.pallas_call(
        functools.partial(coefficient_kernel, tuple(shifts), sides, len(earlier)),
        in_specs=[SMEM] * sides + [VMEM] * (2 * count + sides + len(earlier)),
        out_specs=[VMEM] * sides,
        out_shape=[shape] * sides,
        scratch_shapes=[pltpu.VMEM((freqs, columns * 4 * SUBLANES, tile), jnp.bfloat16)],
        compiler_params=pltpu.CompilerParams(vmem_limit_bytes=16 * 2**20),
        cost_estimate=pl.CostEstimate(
            flops=2 * 2 * sides * freqs * slots * columns * 4 * SUBLANES * tile,
            bytes_accessed=2**20,
            transcendentals=0,
        ),
        name="coefficients",
    )(*offsets, *own, *twin, *factors, *earlier)


def band_kernel(add, at_near, offsets_ref, ranks_ref, coeffs_ref, u_ref, *refs):
    refs = list(refs)
    other_ref = refs.pop(0) if add else None
    out_ref, rhs, crossed = refs[:3]
    freqs, _, sources, slots = coeffs_ref.shape
    tile = u_ref.shape[2]
    place = lax.rem(lax.axis_index("rows") // 2, 2)
    at = place if at_near else 1 - place
    last = offsets_ref.shape[2] - 1
    wide = 2 * sources
    rhs[...] = jnp.zeros_like(rhs)
    crossed[...] = jnp.zeros_like(crossed)
    slot = lax.broadcasted_iota(jnp.int32, (sources, slots), 1)
    for k in range(freqs):
        live = slot < offsets_ref[k, 0, last] + ranks_ref[k, 0, last]
        for part in range(2):
            value = jnp.where(live, coeffs_ref[k, part].astype(jnp.float32), 0.0)
            start = pl.multiple_of((2 * k + part) * wide + at * sources, sources)
            rhs[k, pl.ds(start, sources), :] = value.astype(jnp.bfloat16)
            start = pl.multiple_of((2 * k + 1 - part) * wide + at * sources, sources)
            value = value if part == 0 else -value
            crossed[k, pl.ds(start, sources), :] = value.astype(jnp.bfloat16)
    total = other_ref[...] if add else jnp.zeros((tile, 2 * freqs * wide), jnp.float32)
    for k in range(freqs):
        for part, ref in enumerate((rhs, crossed)):
            total += lax.dot_general(u_ref[part, k], ref[k], NT, preferred_element_type=jnp.float32)
    if not add:
        out_ref[...] = total
        return
    bands, mix = refs[3:]
    groups = out_ref.shape[0]
    bands[...] = total
    packs = LANES // wide
    kinds = 2 * freqs
    block = lax.broadcasted_iota(jnp.int32, (tile // packs, LANES), 1) // wide
    loaded = [bands[pl.ds(b, tile // packs, stride=packs), :] for b in range(packs)]
    rows = tile // packs // groups
    for kind in range(kinds):
        mixed = jnp.zeros((tile // packs, LANES), jnp.float32)
        for b in range(packs):
            shift = (b - kind) * wide % LANES
            moved = pltpu.roll(loaded[b], shift, 1) if shift else loaded[b]
            mixed = jnp.where(block == b, moved, mixed)
        mix[:, kind * rows : (kind + 1) * rows, :] = mixed.reshape(groups, rows, LANES)
    out_ref[...] = mix[...].astype(jnp.bfloat16)


def bands_of(at_near, offsets, ranks, coeffs, u_own, groups, other=None):
    add = other is not None
    freqs, _, sources, slots = coeffs.shape
    tile = u_own.shape[2]
    rows = 2 * freqs * tile * 2 * sources // LANES // groups
    partial = jax.ShapeDtypeStruct((tile, LANES), jnp.float32)
    whole = jax.ShapeDtypeStruct((groups, rows, LANES), jnp.bfloat16)
    spread = pltpu.VMEM((freqs, LANES, slots), jnp.bfloat16)
    mixing = [pltpu.VMEM((tile, LANES), jnp.float32), pltpu.VMEM(whole.shape, jnp.float32)]
    return pl.pallas_call(
        functools.partial(band_kernel, add, at_near),
        in_specs=[SMEM] * 2 + [VMEM] * (3 if add else 2),
        out_specs=VMEM,
        out_shape=whole if add else partial,
        scratch_shapes=[spread, spread] + (mixing if add else []),
        compiler_params=pltpu.CompilerParams(vmem_limit_bytes=8 * 2**20),
        cost_estimate=pl.CostEstimate(
            flops=2 * 2 * freqs * tile * LANES * slots, bytes_accessed=2**20, transcendentals=0
        ),
        name="bands",
    )(offsets, ranks, coeffs, u_own, *([other] if add else []))


def series_kernel(bands_ref, inverse_ref, out_ref, wide, done, sems):
    groups, rows, lanes = bands_ref.shape
    kinds = inverse_ref.shape[0]
    steps = groups * rows // kinds
    wide[...] = bands_ref[...].astype(jnp.float32).reshape(groups * rows, lanes)
    copies = []
    for i in range(steps):
        part = wide[pl.ds(i, kinds, stride=steps), :]
        done[i] = jnp.dot(
            part.T.astype(jnp.bfloat16), inverse_ref[...], preferred_element_type=jnp.float32
        ).astype(jnp.bfloat16)
        copies.append(
            pltpu.make_async_copy(
                done.at[i], out_ref.at[i * lanes : (i + 1) * lanes, :], sems.at[i]
            )
        )
        copies[-1].start()
    for copy in copies:
        copy.wait()


def series_of(bands, inverse):
    groups, rows, lanes = bands.shape
    kinds, samples = inverse.shape
    steps = groups * rows // kinds
    return pl.pallas_call(
        series_kernel,
        in_specs=[VMEM] * 2,
        out_specs=pl.BlockSpec(memory_space=pl.ANY),
        out_shape=jax.ShapeDtypeStruct((steps * lanes, samples), jnp.bfloat16),
        scratch_shapes=[
            pltpu.VMEM((groups * rows, lanes), jnp.float32),
            pltpu.VMEM((steps, lanes, samples), jnp.bfloat16),
            pltpu.SemaphoreType.DMA((steps,)),
        ],
        compiler_params=pltpu.CompilerParams(vmem_limit_bytes=16 * 2**20),
        cost_estimate=pl.CostEstimate(
            flops=2 * steps * lanes * kinds * samples,
            bytes_accessed=steps * lanes * samples * 2,
            transcendentals=0,
        ),
        name="series",
    )(bands, inverse)


def fits(rec_dev, src_dev, freq_dev, rows_dev, tile, slots, freq_group, row_group):
    kinds = 2 * freq_dev * freq_group
    return (
        src_dev == SUBLANES
        and row_group == 4
        and rows_dev == 1
        and freq_group > 1
        and rec_dev % tile == 0
        and tile % (2 * LANES) == 0
        and slots % tile == 0
        and LANES % kinds == 0
        and SUBLANES % (LANES // kinds) == 0
        and 2 * freq_dev * src_dev * row_group == LANES
        and tile % (4 * SUBLANES * freq_group) == 0
    )


def per_device_fast(wavefield, u_factors, v_factors, tile_ranks, tile_offsets):
    rec_dev, src_dev, samples = wavefield.shape
    freq_dev = u_factors.shape[1]
    groups = lax.axis_size("freq")
    row_group = lax.axis_size("rows")
    freqs = freq_dev * groups
    sources = src_dev * row_group
    tile = u_factors.shape[3]
    across = [(i, i ^ 2) for i in range(row_group)]
    beside = [(i, i ^ 1) for i in range(row_group)]
    forward, inverse = spectral_tables(freqs, samples)
    u_own, v_own = u_factors[:, :, 0], v_factors[:, :, 0]
    v_far = lax.ppermute(v_own, "rows", across)
    offsets_far = lax.ppermute(tile_offsets, "rows", across)
    table = forward.reshape(2 * freqs, samples)
    sent = transform(wavefield.reshape(rec_dev * src_dev, samples), table, groups)
    order = sorted(range(1, groups), key=lambda s: abs(2 * s - groups))
    own = [sent[0]]
    for shift in order:
        ring = [(i, (i + shift) % groups) for i in range(groups)]
        own.append(lax.ppermute(sent[shift], "freq", ring))
    shifts = [0] + order
    early, late = shifts[:EARLY], shifts[EARLY:]
    own_early, own_late = own[:EARLY], own[EARLY:]
    twin_early = [lax.ppermute(block, "rows", beside) for block in own_early]
    (near,) = coefficients(early, [tile_offsets], own_early, twin_early, [v_own])
    (leaving,) = coefficients(early, [offsets_far], own_early, twin_early, [v_far])
    own_late, near, leaving = lax.optimization_barrier((own_late, near, leaving))
    twin_late = [lax.ppermute(block, "rows", beside) for block in own_late]
    (leaving,) = coefficients(late, [offsets_far], own_late, twin_late, [v_far], [leaving])
    far = lax.ppermute(leaving, "rows", across)
    (near,) = coefficients(late, [tile_offsets], own_late, twin_late, [v_own], [near])
    half = bands_of(True, tile_offsets, tile_ranks, near, u_own, groups)
    bands = bands_of(False, tile_offsets, tile_ranks, far, u_own, groups, half)
    returned = lax.all_to_all(bands, "freq", split_axis=0, concat_axis=0, tiled=True)
    series = series_of(returned, inverse.reshape(2 * freqs, samples))
    return series.reshape(tile // groups, sources, samples)


def choose(wavefield, u_factors, v_factors, tile_ranks, tile_offsets):
    ok = fits(
        wavefield.shape[0],
        wavefield.shape[1],
        u_factors.shape[1],
        u_factors.shape[2],
        u_factors.shape[3],
        u_factors.shape[4],
        lax.axis_size("freq"),
        lax.axis_size("rows"),
    )
    step = per_device_fast if ok else per_device
    return step(wavefield, u_factors, v_factors, tile_ranks, tile_offsets)


def solution(mesh):
    placed = (
        P("freq", "rows", None),
        P(None, "freq", "rows", None, None),
        P(None, "freq", "rows", None, None),
        P("freq", "rows", None),
        P("freq", "rows", None),
    )
    return jax.shard_map(
        choose,
        mesh=mesh,
        in_specs=placed,
        out_specs=P(("rows", "freq"), None, None),
        check_vma=False,
    )
```

```python
import functools
import math

import jax
import jax.numpy as jnp
from jax import lax
from jax.experimental import pallas as pl
from jax.experimental.pallas import tpu as pltpu
from jax.sharding import PartitionSpec as P


RANK_MAX = 64
LANES = 128
SUBLANES = 8
NT = (((1,), (1,)), ((), ()))
VMEM = pl.BlockSpec(memory_space=pltpu.VMEM)
SMEM = pl.BlockSpec(memory_space=pltpu.SMEM)
EARLY = 5
AHEAD = 3


def spectral_tables(freq_count, sample_count):
    freq_bins = jnp.arange(freq_count, dtype=jnp.int32) + 1
    sample_index = jnp.arange(sample_count, dtype=jnp.int32)
    phase_int = freq_bins[:, None] * sample_index[None, :] % sample_count
    angles = phase_int.astype(jnp.float32) * (2.0 * math.pi / sample_count)
    cosine = jnp.cos(angles)
    minus_sine = -jnp.sin(angles)
    stacked = jnp.stack([cosine, minus_sine], axis=1)
    forward = (stacked / math.sqrt(sample_count)).astype(jnp.bfloat16)
    inverse = (stacked / math.sqrt(freq_count)).astype(jnp.bfloat16)
    return (forward, inverse)


def tile_windows(v_row, u_row, starts, rank_max):
    columns = starts.shape[0]
    slot_index = (starts[:, None] + jnp.arange(rank_max, dtype=jnp.int32)[None, :]).reshape(-1)
    v_padded = jnp.pad(v_row, ((0, 0), (0, rank_max), (0, 0)))
    u_padded = jnp.pad(u_row, ((0, 0), (0, 0), (0, rank_max)))
    v_win = jnp.take(v_padded, slot_index, axis=1).reshape(2, columns, rank_max, v_row.shape[2])
    u_win = jnp.take(u_padded, slot_index, axis=2).reshape(2, u_row.shape[1], columns, rank_max)
    return (v_win, u_win)


def slot_lookup(starts, counts, rank_max, slot_count):
    position = jnp.arange(slot_count, dtype=jnp.int32)
    started = starts[:, None, :] <= position[None, :, None]
    owner_tile = jnp.sum(started.astype(jnp.int32), axis=2) - 1
    first_slot = jnp.max(jnp.where(started, starts[:, None, :], 0), axis=2)
    within = position[None, :] - first_slot
    live_slot = position[None, :] < (starts[:, -1] + counts[:, -1])[:, None]
    flat_index = jnp.where(live_slot, owner_tile * rank_max + within, 0)
    return (flat_index, live_slot)


def take_slots(values, chosen):
    return jnp.take(values, chosen, axis=1)


def per_device(wavefield, u_factors, v_factors, tile_ranks, tile_offsets):
    rec_dev, src_dev, samples = wavefield.shape
    freq_dev = u_factors.shape[1]
    rows_dev = u_factors.shape[2]
    tile_size = u_factors.shape[3]
    slot_count = u_factors.shape[4]
    freq_group = lax.axis_size("freq")
    row_group = lax.axis_size("rows")
    freqs = freq_dev * freq_group
    receivers = rec_dev * freq_group
    columns = receivers // tile_size
    sources = src_dev * row_group
    forward, inverse = spectral_tables(freqs, samples)
    spectrum = jnp.einsum("kct,rst->kcrs", forward, wavefield, preferred_element_type=jnp.float32)
    spectrum = spectrum.astype(jnp.bfloat16).reshape(freqs, 2, rec_dev * src_dev)
    windows = jax.vmap(
        functools.partial(tile_windows, rank_max=RANK_MAX), in_axes=(1, 1, 0), out_axes=(1, 1)
    )
    rank_slots = jnp.arange(RANK_MAX, dtype=jnp.int32)
    tile_row = 0
    v_win, u_win = windows(
        v_factors[:, :, tile_row], u_factors[:, :, tile_row], tile_offsets[:, tile_row]
    )
    rank_mask = rank_slots[None, None, :] < tile_ranks[:, tile_row, :, None]
    flat_index, live_slot = slot_lookup(
        tile_offsets[:, tile_row], tile_ranks[:, tile_row], RANK_MAX, slot_count
    )
    prepared = [(v_win, u_win, rank_mask, flat_index, live_slot)]
    by_frequency = lax.all_to_all(spectrum, "freq", split_axis=0, concat_axis=2, tiled=True)
    portion = lax.all_gather(by_frequency[None], "rows", axis=0, tiled=True)
    blocks_in = portion.shape[0]
    spectra = portion.reshape(blocks_in, freq_dev, 2, columns, tile_size, src_dev)
    spectra = jnp.transpose(spectra, (1, 2, 3, 4, 0, 5)).reshape(
        freq_dev, 2, columns, tile_size, blocks_in * src_dev
    )
    tile_row = 0
    v_win, u_win, rank_mask, flat_index, live_slot = prepared[tile_row]
    quadrants = jnp.einsum(
        "afjmr,fbjrs->fabjms", v_win, spectra, preferred_element_type=jnp.float32
    )
    coeffs = jnp.stack(
        [quadrants[:, 0, 0] - quadrants[:, 1, 1], quadrants[:, 0, 1] + quadrants[:, 1, 0]], axis=1
    )
    coeffs = jnp.where(rank_mask[:, None, :, :, None], coeffs, 0.0).astype(jnp.bfloat16)
    stacked = coeffs.reshape(freq_dev, 2, columns * RANK_MAX, blocks_in * src_dev)
    packed = jax.vmap(take_slots)(stacked, flat_index)
    packed = jnp.where(live_slot[:, None, :, None], packed, jnp.zeros((), jnp.bfloat16))
    products = jnp.einsum(
        "afrk,fcks->facrs", u_factors[:, :, tile_row], packed, preferred_element_type=jnp.float32
    )
    results = [
        jnp.stack(
            [products[:, 0, 0] - products[:, 1, 1], products[:, 0, 1] + products[:, 1, 0]], axis=1
        )
    ]
    merged = jnp.stack(results, axis=2)
    bands = merged.astype(jnp.bfloat16).reshape(
        freq_dev, 2, rows_dev * tile_size, blocks_in, src_dev
    )
    bands = bands.reshape(freq_dev, 2, rows_dev * tile_size * sources)
    returned = lax.all_to_all(bands, "freq", split_axis=2, concat_axis=0, tiled=True)
    series = jnp.einsum("kcq,kct->qt", returned, inverse, preferred_element_type=jnp.float32)
    return series.astype(jnp.bfloat16).reshape(rows_dev * tile_size // freq_group, sources, samples)


def transform_kernel(traces_ref, table_ref, *refs):
    groups = lax.axis_size("freq")
    outs, (traces, sems, products, turned) = refs[:groups], refs[groups:]
    me = lax.axis_index("freq")
    rows = products.shape[1]
    kinds = turned.shape[0] // SUBLANES
    packs = LANES // kinds
    blocks = traces_ref.shape[0] // rows
    each = outs[0].shape[0]

    def copy(i):
        part = pl.ds(pl.multiple_of(i * rows, rows), rows)
        return pltpu.make_async_copy(traces_ref.at[part, :], traces.at[part, :], sems.at[i])

    def turn(i, source_rows):
        place = lax.broadcasted_iota(jnp.int32, (rows // SUBLANES, LANES), 1) // kinds
        for first in range(0, SUBLANES, packs):
            mixed = source_rows[pl.ds(first, rows // SUBLANES, stride=SUBLANES), :]
            for m in range(1, packs):
                part = source_rows[pl.ds(first + m, rows // SUBLANES, stride=SUBLANES), :]
                mixed = jnp.where(place == m, part, mixed)
            mixed = mixed.T
            for m in range(packs):
                turned[pl.ds(first + m, kinds, stride=SUBLANES), :] = mixed[
                    m * kinds : (m + 1) * kinds
                ]
        lanes = pl.ds(pl.multiple_of(i * LANES, LANES), LANES)
        for shift, out in enumerate(outs):
            group = lax.rem(me + shift, groups)
            start = pl.multiple_of(group * each, each)
            out[:, lanes] = turned[pl.ds(start, each), :].astype(jnp.bfloat16)

    for i in range(min(AHEAD, blocks)):
        copy(i).start()

    def step(i, carry):
        now = lax.rem(i, 2)

        @pl.when(i + AHEAD < blocks)
        def _():
            copy(i + AHEAD).start()

        copy(i).wait()
        part = pl.ds(pl.multiple_of(i * rows, rows), rows)
        products[now] = lax.dot_general(
            traces[part, :], table_ref[...], NT, preferred_element_type=jnp.float32
        )
        turn(jnp.maximum(i - 1, 0), products.at[1 - now])
        return carry

    lax.fori_loop(0, blocks, step, 0)
    turn(blocks - 1, products.at[(blocks - 1) % 2])


def transform(traces, table, groups):
    rows, samples = traces.shape
    receivers = rows // SUBLANES
    kinds = table.shape[0]
    repeated = jnp.tile(table, (LANES // kinds, 1))
    shape = jax.ShapeDtypeStruct((kinds * SUBLANES // groups, receivers), jnp.bfloat16)
    return pl.pallas_call(
        transform_kernel,
        in_specs=[pl.BlockSpec(memory_space=pltpu.HBM), VMEM],
        out_specs=[VMEM] * groups,
        out_shape=[shape] * groups,
        scratch_shapes=[
            pltpu.VMEM((rows, samples), jnp.bfloat16),
            pltpu.SemaphoreType.DMA((receivers // LANES,)),
            pltpu.VMEM((2, LANES * SUBLANES, LANES), jnp.float32),
            pltpu.VMEM((kinds * SUBLANES, LANES), jnp.float32),
        ],
        compiler_params=pltpu.CompilerParams(vmem_limit_bytes=48 * 2**20),
        cost_estimate=pl.CostEstimate(
            flops=2 * rows * samples * 256, bytes_accessed=rows * samples * 2, transcendentals=0
        ),
        name="transform",
    )(traces, repeated)


def coefficient_kernel(shifts, sides, before, *refs):
    count = len(shifts)
    refs = list(refs)
    offsets = [refs.pop(0) for _ in range(sides)]
    own = [refs.pop(0) for _ in range(count)]
    twin = [refs.pop(0) for _ in range(count)]
    factors = [refs.pop(0) for _ in range(sides)]
    earlier = [refs.pop(0) for _ in range(before)]
    outs = [refs.pop(0) for _ in range(sides)]
    (lhs,) = refs
    groups = lax.axis_size("freq")
    me = lax.axis_index("freq")
    core = lax.rem(lax.axis_index("rows"), 2)
    _, freqs, slots, tile = factors[0].shape
    per_block = own[0].shape[1] // tile
    columns = groups * per_block
    half = 2 * SUBLANES
    deep = 2 * half
    for k in range(freqs):
        for arrays, at in ((own, core), (twin, 1 - core)):
            for b in range(count):
                for inner in range(per_block):
                    start = (b * per_block + inner) * deep + at * half
                    lhs[k, pl.ds(pl.multiple_of(start, half), half), :] = arrays[b][
                        k * half : (k + 1) * half, inner * tile : (inner + 1) * tile
                    ]
    for side in range(sides):
        for k in range(freqs):
            for low in range(0, slots, tile):
                slot = lax.broadcasted_iota(jnp.int32, (deep, tile), 1) + low
                chosen = []
                for part in range(2):
                    products = lax.dot_general(
                        lhs[k],
                        factors[side][part, k, low : low + tile, :],
                        NT,
                        preferred_element_type=jnp.float32,
                    )
                    total = jnp.zeros((deep, tile), jnp.float32)
                    for b, shift in enumerate(shifts):
                        column = lax.rem(me + groups - shift, groups) * per_block
                        value = total
                        for inner in range(per_block):
                            at = (b * per_block + inner) * deep
                            value = jnp.where(
                                slot >= offsets[side][k, 0, column + inner],
                                products[at : at + deep],
                                value,
                            )
                        after = jnp.minimum(column + per_block, columns - 1)
                        end = jnp.where(
                            column + per_block < columns, offsets[side][k, 0, after], slots
                        )
                        total = jnp.where(slot >= end, total, value)
                    chosen.append(total)
                by_real, by_imag = chosen
                n = SUBLANES
                real = [by_real[g : g + n] - by_imag[g + n : g + 2 * n] for g in (0, half)]
                imag = [by_real[g + n : g + 2 * n] + by_imag[g : g + n] for g in (0, half)]
                for c, pieces in enumerate((real, imag)):
                    value = jnp.concatenate(pieces, 0)
                    if side < before:
                        value += earlier[side][k, c, :, low : low + tile].astype(jnp.float32)
                    outs[side][k, c, :, low : low + tile] = value.astype(jnp.bfloat16)


def coefficients(shifts, offsets, own, twin, factors, earlier=()):
    sides, count = len(offsets), len(shifts)
    _, freqs, slots, tile = factors[0].shape
    columns = count * own[0].shape[1] // tile
    shape = jax.ShapeDtypeStruct((freqs, 2, 2 * SUBLANES, slots), jnp.bfloat16)
    return pl.pallas_call(
        functools.partial(coefficient_kernel, tuple(shifts), sides, len(earlier)),
        in_specs=[SMEM] * sides + [VMEM] * (2 * count + sides + len(earlier)),
        out_specs=[VMEM] * sides,
        out_shape=[shape] * sides,
        scratch_shapes=[pltpu.VMEM((freqs, columns * 4 * SUBLANES, tile), jnp.bfloat16)],
        compiler_params=pltpu.CompilerParams(vmem_limit_bytes=16 * 2**20),
        cost_estimate=pl.CostEstimate(
            flops=2 * 2 * sides * freqs * slots * columns * 4 * SUBLANES * tile,
            bytes_accessed=2**20,
            transcendentals=0,
        ),
        name="coefficients",
    )(*offsets, *own, *twin, *factors, *earlier)


def band_kernel(add, at_near, offsets_ref, ranks_ref, coeffs_ref, u_ref, *refs):
    refs = list(refs)
    other_ref = refs.pop(0) if add else None
    out_ref, rhs, crossed = refs[:3]
    freqs, _, sources, slots = coeffs_ref.shape
    tile = u_ref.shape[2]
    place = lax.rem(lax.axis_index("rows") // 2, 2)
    at = place if at_near else 1 - place
    last = offsets_ref.shape[2] - 1
    wide = 2 * sources
    rhs[...] = jnp.zeros_like(rhs)
    crossed[...] = jnp.zeros_like(crossed)
    slot = lax.broadcasted_iota(jnp.int32, (sources, slots), 1)
    for k in range(freqs):
        live = slot < offsets_ref[k, 0, last] + ranks_ref[k, 0, last]
        for part in range(2):
            value = jnp.where(live, coeffs_ref[k, part].astype(jnp.float32), 0.0)
            start = pl.multiple_of((2 * k + part) * wide + at * sources, sources)
            rhs[k, pl.ds(start, sources), :] = value.astype(jnp.bfloat16)
            start = pl.multiple_of((2 * k + 1 - part) * wide + at * sources, sources)
            value = value if part == 0 else -value
            crossed[k, pl.ds(start, sources), :] = value.astype(jnp.bfloat16)
    total = other_ref[...] if add else jnp.zeros((tile, 2 * freqs * wide), jnp.float32)
    for k in range(freqs):
        for part, ref in enumerate((rhs, crossed)):
            total += lax.dot_general(u_ref[part, k], ref[k], NT, preferred_element_type=jnp.float32)
    if not add:
        out_ref[...] = total
        return
    bands, mix = refs[3:]
    groups = out_ref.shape[0]
    bands[...] = total
    packs = LANES // wide
    kinds = 2 * freqs
    block = lax.broadcasted_iota(jnp.int32, (tile // packs, LANES), 1) // wide
    loaded = [bands[pl.ds(b, tile // packs, stride=packs), :] for b in range(packs)]
    rows = tile // packs // groups
    for kind in range(kinds):
        mixed = jnp.zeros((tile // packs, LANES), jnp.float32)
        for b in range(packs):
            shift = (b - kind) * wide % LANES
            moved = pltpu.roll(loaded[b], shift, 1) if shift else loaded[b]
            mixed = jnp.where(block == b, moved, mixed)
        mix[:, kind * rows : (kind + 1) * rows, :] = mixed.reshape(groups, rows, LANES)
    out_ref[...] = mix[...].astype(jnp.bfloat16)


def bands_of(at_near, offsets, ranks, coeffs, u_own, groups, other=None):
    add = other is not None
    freqs, _, sources, slots = coeffs.shape
    tile = u_own.shape[2]
    rows = 2 * freqs * tile * 2 * sources // LANES // groups
    partial = jax.ShapeDtypeStruct((tile, LANES), jnp.float32)
    whole = jax.ShapeDtypeStruct((groups, rows, LANES), jnp.bfloat16)
    spread = pltpu.VMEM((freqs, LANES, slots), jnp.bfloat16)
    mixing = [pltpu.VMEM((tile, LANES), jnp.float32), pltpu.VMEM(whole.shape, jnp.float32)]
    return pl.pallas_call(
        functools.partial(band_kernel, add, at_near),
        in_specs=[SMEM] * 2 + [VMEM] * (3 if add else 2),
        out_specs=VMEM,
        out_shape=whole if add else partial,
        scratch_shapes=[spread, spread] + (mixing if add else []),
        compiler_params=pltpu.CompilerParams(vmem_limit_bytes=8 * 2**20),
        cost_estimate=pl.CostEstimate(
            flops=2 * 2 * freqs * tile * LANES * slots, bytes_accessed=2**20, transcendentals=0
        ),
        name="bands",
    )(offsets, ranks, coeffs, u_own, *([other] if add else []))


def series_kernel(bands_ref, inverse_ref, out_ref, wide, done, sems):
    groups, rows, lanes = bands_ref.shape
    kinds = inverse_ref.shape[0]
    steps = groups * rows // kinds
    wide[...] = bands_ref[...].astype(jnp.float32).reshape(groups * rows, lanes)
    copies = []
    for i in range(steps):
        part = wide[pl.ds(i, kinds, stride=steps), :]
        done[i] = jnp.dot(
            part.T.astype(jnp.bfloat16), inverse_ref[...], preferred_element_type=jnp.float32
        ).astype(jnp.bfloat16)
        copies.append(
            pltpu.make_async_copy(
                done.at[i], out_ref.at[i * lanes : (i + 1) * lanes, :], sems.at[i]
            )
        )
        copies[-1].start()
    for copy in copies:
        copy.wait()


def series_of(bands, inverse):
    groups, rows, lanes = bands.shape
    kinds, samples = inverse.shape
    steps = groups * rows // kinds
    return pl.pallas_call(
        series_kernel,
        in_specs=[VMEM] * 2,
        out_specs=pl.BlockSpec(memory_space=pl.ANY),
        out_shape=jax.ShapeDtypeStruct((steps * lanes, samples), jnp.bfloat16),
        scratch_shapes=[
            pltpu.VMEM((groups * rows, lanes), jnp.float32),
            pltpu.VMEM((steps, lanes, samples), jnp.bfloat16),
            pltpu.SemaphoreType.DMA((steps,)),
        ],
        compiler_params=pltpu.CompilerParams(vmem_limit_bytes=16 * 2**20),
        cost_estimate=pl.CostEstimate(
            flops=2 * steps * lanes * kinds * samples,
            bytes_accessed=steps * lanes * samples * 2,
            transcendentals=0,
        ),
        name="series",
    )(bands, inverse)


def fits(rec_dev, src_dev, freq_dev, rows_dev, tile, slots, freq_group, row_group):
    kinds = 2 * freq_dev * freq_group
    return (
        src_dev == SUBLANES
        and row_group == 4
        and rows_dev == 1
        and freq_group > 1
        and rec_dev % tile == 0
        and tile % (2 * LANES) == 0
        and slots % tile == 0
        and LANES % kinds == 0
        and SUBLANES % (LANES // kinds) == 0
        and 2 * freq_dev * src_dev * row_group == LANES
        and tile % (4 * SUBLANES * freq_group) == 0
    )


def shift_order(groups):
    return sorted(range(1, groups), key=lambda s: abs(2 * s - groups))


def per_device_fast(wavefield, u_factors, v_factors, tile_ranks, tile_offsets):
    rec_dev, src_dev, samples = wavefield.shape
    freq_dev = u_factors.shape[1]
    groups = lax.axis_size("freq")
    row_group = lax.axis_size("rows")
    freqs = freq_dev * groups
    sources = src_dev * row_group
    tile = u_factors.shape[3]
    across = [(i, i ^ 2) for i in range(row_group)]
    beside = [(i, i ^ 1) for i in range(row_group)]
    forward, inverse = spectral_tables(freqs, samples)
    u_own, v_own = u_factors[:, :, 0], v_factors[:, :, 0]
    v_far = lax.ppermute(v_own, "rows", across)
    offsets_far = lax.ppermute(tile_offsets, "rows", across)
    table = forward.reshape(2 * freqs, samples)
    sent = transform(wavefield.reshape(rec_dev * src_dev, samples), table, groups)
    order = shift_order(groups)
    own = [sent[0]]
    for shift in order:
        ring = [(i, (i + shift) % groups) for i in range(groups)]
        own.append(lax.ppermute(sent[shift], "freq", ring))
    shifts = [0] + order
    early, late = shifts[:EARLY], shifts[EARLY:]
    own_early, own_late = own[:EARLY], own[EARLY:]
    twin_early = []
    for shift, block in zip(early, own_early):
        twin_early.append(lax.ppermute(block, "rows", beside))
    (near,) = coefficients(early, [tile_offsets], own_early, twin_early, [v_own])
    (leaving,) = coefficients(early, [offsets_far], own_early, twin_early, [v_far])
    own_late, near, leaving = lax.optimization_barrier((own_late, near, leaving))
    twin_late = [lax.ppermute(block, "rows", beside) for block in own_late]
    (leaving,) = coefficients(late, [offsets_far], own_late, twin_late, [v_far], [leaving])
    far = lax.ppermute(leaving, "rows", across)
    (near,) = coefficients(late, [tile_offsets], own_late, twin_late, [v_own], [near])
    half = bands_of(True, tile_offsets, tile_ranks, near, u_own, groups)
    bands = bands_of(False, tile_offsets, tile_ranks, far, u_own, groups, half)
    returned = lax.all_to_all(bands, "freq", split_axis=0, concat_axis=0, tiled=True)
    series = series_of(returned, inverse.reshape(2 * freqs, samples))
    return series.reshape(tile // groups, sources, samples)


def choose(wavefield, u_factors, v_factors, tile_ranks, tile_offsets):
    ok = fits(
        wavefield.shape[0],
        wavefield.shape[1],
        u_factors.shape[1],
        u_factors.shape[2],
        u_factors.shape[3],
        u_factors.shape[4],
        lax.axis_size("freq"),
        lax.axis_size("rows"),
    )
    step = per_device_fast if ok else per_device
    return step(wavefield, u_factors, v_factors, tile_ranks, tile_offsets)


def solution(mesh):
    placed = (
        P("freq", "rows", None),
        P(None, "freq", "rows", None, None),
        P(None, "freq", "rows", None, None),
        P("freq", "rows", None),
        P("freq", "rows", None),
    )
    return jax.shard_map(
        choose,
        mesh=mesh,
        in_specs=placed,
        out_specs=P(("rows", "freq"), None, None),
        check_vma=False,
    )
```

```python
import functools
import math

import jax
import jax.numpy as jnp
from jax import lax
from jax.experimental import pallas as pl
from jax.experimental.pallas import tpu as pltpu
from jax.sharding import PartitionSpec as P


RANK_MAX = 64
LANES = 128
SUBLANES = 8
NT = (((1,), (1,)), ((), ()))
VMEM = pl.BlockSpec(memory_space=pltpu.VMEM)
SMEM = pl.BlockSpec(memory_space=pltpu.SMEM)
LATE = 2
PAIRED = (4, 8, 16)
AHEAD = 3


def spectral_tables(freq_count, sample_count):
    freq_bins = jnp.arange(freq_count, dtype=jnp.int32) + 1
    sample_index = jnp.arange(sample_count, dtype=jnp.int32)
    phase_int = freq_bins[:, None] * sample_index[None, :] % sample_count
    angles = phase_int.astype(jnp.float32) * (2.0 * math.pi / sample_count)
    cosine = jnp.cos(angles)
    minus_sine = -jnp.sin(angles)
    stacked = jnp.stack([cosine, minus_sine], axis=1)
    forward = (stacked / math.sqrt(sample_count)).astype(jnp.bfloat16)
    inverse = (stacked / math.sqrt(freq_count)).astype(jnp.bfloat16)
    return (forward, inverse)


def tile_windows(v_row, u_row, starts, rank_max):
    columns = starts.shape[0]
    slot_index = (starts[:, None] + jnp.arange(rank_max, dtype=jnp.int32)[None, :]).reshape(-1)
    v_padded = jnp.pad(v_row, ((0, 0), (0, rank_max), (0, 0)))
    u_padded = jnp.pad(u_row, ((0, 0), (0, 0), (0, rank_max)))
    v_win = jnp.take(v_padded, slot_index, axis=1).reshape(2, columns, rank_max, v_row.shape[2])
    u_win = jnp.take(u_padded, slot_index, axis=2).reshape(2, u_row.shape[1], columns, rank_max)
    return (v_win, u_win)


def slot_lookup(starts, counts, rank_max, slot_count):
    position = jnp.arange(slot_count, dtype=jnp.int32)
    started = starts[:, None, :] <= position[None, :, None]
    owner_tile = jnp.sum(started.astype(jnp.int32), axis=2) - 1
    first_slot = jnp.max(jnp.where(started, starts[:, None, :], 0), axis=2)
    within = position[None, :] - first_slot
    live_slot = position[None, :] < (starts[:, -1] + counts[:, -1])[:, None]
    flat_index = jnp.where(live_slot, owner_tile * rank_max + within, 0)
    return (flat_index, live_slot)


def take_slots(values, chosen):
    return jnp.take(values, chosen, axis=1)


def per_device(wavefield, u_factors, v_factors, tile_ranks, tile_offsets):
    rec_dev, src_dev, samples = wavefield.shape
    freq_dev = u_factors.shape[1]
    rows_dev = u_factors.shape[2]
    tile_size = u_factors.shape[3]
    slot_count = u_factors.shape[4]
    freq_group = lax.axis_size("freq")
    row_group = lax.axis_size("rows")
    freqs = freq_dev * freq_group
    receivers = rec_dev * freq_group
    columns = receivers // tile_size
    sources = src_dev * row_group
    forward, inverse = spectral_tables(freqs, samples)
    spectrum = jnp.einsum("kct,rst->kcrs", forward, wavefield, preferred_element_type=jnp.float32)
    spectrum = spectrum.astype(jnp.bfloat16).reshape(freqs, 2, rec_dev * src_dev)
    windows = jax.vmap(
        functools.partial(tile_windows, rank_max=RANK_MAX), in_axes=(1, 1, 0), out_axes=(1, 1)
    )
    rank_slots = jnp.arange(RANK_MAX, dtype=jnp.int32)
    tile_row = 0
    v_win, u_win = windows(
        v_factors[:, :, tile_row], u_factors[:, :, tile_row], tile_offsets[:, tile_row]
    )
    rank_mask = rank_slots[None, None, :] < tile_ranks[:, tile_row, :, None]
    flat_index, live_slot = slot_lookup(
        tile_offsets[:, tile_row], tile_ranks[:, tile_row], RANK_MAX, slot_count
    )
    prepared = [(v_win, u_win, rank_mask, flat_index, live_slot)]
    by_frequency = lax.all_to_all(spectrum, "freq", split_axis=0, concat_axis=2, tiled=True)
    portion = lax.all_gather(by_frequency[None], "rows", axis=0, tiled=True)
    blocks_in = portion.shape[0]
    spectra = portion.reshape(blocks_in, freq_dev, 2, columns, tile_size, src_dev)
    spectra = jnp.transpose(spectra, (1, 2, 3, 4, 0, 5)).reshape(
        freq_dev, 2, columns, tile_size, blocks_in * src_dev
    )
    tile_row = 0
    v_win, u_win, rank_mask, flat_index, live_slot = prepared[tile_row]
    quadrants = jnp.einsum(
        "afjmr,fbjrs->fabjms", v_win, spectra, preferred_element_type=jnp.float32
    )
    coeffs = jnp.stack(
        [quadrants[:, 0, 0] - quadrants[:, 1, 1], quadrants[:, 0, 1] + quadrants[:, 1, 0]], axis=1
    )
    coeffs = jnp.where(rank_mask[:, None, :, :, None], coeffs, 0.0).astype(jnp.bfloat16)
    stacked = coeffs.reshape(freq_dev, 2, columns * RANK_MAX, blocks_in * src_dev)
    packed = jax.vmap(take_slots)(stacked, flat_index)
    packed = jnp.where(live_slot[:, None, :, None], packed, jnp.zeros((), jnp.bfloat16))
    products = jnp.einsum(
        "afrk,fcks->facrs", u_factors[:, :, tile_row], packed, preferred_element_type=jnp.float32
    )
    results = [
        jnp.stack(
            [products[:, 0, 0] - products[:, 1, 1], products[:, 0, 1] + products[:, 1, 0]], axis=1
        )
    ]
    merged = jnp.stack(results, axis=2)
    bands = merged.astype(jnp.bfloat16).reshape(
        freq_dev, 2, rows_dev * tile_size, blocks_in, src_dev
    )
    bands = bands.reshape(freq_dev, 2, rows_dev * tile_size * sources)
    returned = lax.all_to_all(bands, "freq", split_axis=2, concat_axis=0, tiled=True)
    series = jnp.einsum("kcq,kct->qt", returned, inverse, preferred_element_type=jnp.float32)
    return series.astype(jnp.bfloat16).reshape(rows_dev * tile_size // freq_group, sources, samples)


def transform_kernel(traces_ref, table_ref, *refs):
    groups = lax.axis_size("freq")
    outs, (traces, sems, products, turned) = refs[:groups], refs[groups:]
    me = lax.axis_index("freq")
    rows = products.shape[1]
    kinds = turned.shape[0] // SUBLANES
    packs = LANES // kinds
    blocks = traces_ref.shape[0] // rows
    each = outs[0].shape[0]

    def copy(i):
        part = pl.ds(pl.multiple_of(i * rows, rows), rows)
        return pltpu.make_async_copy(traces_ref.at[part, :], traces.at[part, :], sems.at[i])

    def turn(i, source_rows):
        place = lax.broadcasted_iota(jnp.int32, (rows // SUBLANES, LANES), 1) // kinds
        for first in range(0, SUBLANES, packs):
            mixed = source_rows[pl.ds(first, rows // SUBLANES, stride=SUBLANES), :]
            for m in range(1, packs):
                part = source_rows[pl.ds(first + m, rows // SUBLANES, stride=SUBLANES), :]
                mixed = jnp.where(place == m, part, mixed)
            mixed = mixed.T
            for m in range(packs):
                turned[pl.ds(first + m, kinds, stride=SUBLANES), :] = mixed[
                    m * kinds : (m + 1) * kinds
                ]
        lanes = pl.ds(pl.multiple_of(i * LANES, LANES), LANES)
        for shift, out in enumerate(outs):
            group = me ^ shift
            start = pl.multiple_of(group * each, each)
            out[:, lanes] = turned[pl.ds(start, each), :].astype(jnp.bfloat16)

    for i in range(min(AHEAD, blocks)):
        copy(i).start()

    def step(i, carry):
        now = lax.rem(i, 2)

        @pl.when(i + AHEAD < blocks)
        def _():
            copy(i + AHEAD).start()

        copy(i).wait()
        part = pl.ds(pl.multiple_of(i * rows, rows), rows)
        turn(jnp.maximum(i - 1, 0), products.at[1 - now])
        products[now] = lax.dot_general(
            traces[part, :], table_ref[...], NT, preferred_element_type=jnp.float32
        )
        return carry

    lax.fori_loop(0, blocks, step, 0)
    turn(blocks - 1, products.at[(blocks - 1) % 2])


def transform(traces, table, groups):
    rows, samples = traces.shape
    receivers = rows // SUBLANES
    kinds = table.shape[0]
    repeated = jnp.tile(table, (LANES // kinds, 1))
    shape = jax.ShapeDtypeStruct((kinds * SUBLANES // groups, receivers), jnp.bfloat16)
    return pl.pallas_call(
        transform_kernel,
        in_specs=[pl.BlockSpec(memory_space=pltpu.HBM), VMEM],
        out_specs=[VMEM] * groups,
        out_shape=[shape] * groups,
        scratch_shapes=[
            pltpu.VMEM((rows, samples), jnp.bfloat16),
            pltpu.SemaphoreType.DMA((receivers // LANES,)),
            pltpu.VMEM((2, LANES * SUBLANES, LANES), jnp.float32),
            pltpu.VMEM((kinds * SUBLANES, LANES), jnp.float32),
        ],
        compiler_params=pltpu.CompilerParams(vmem_limit_bytes=48 * 2**20),
        cost_estimate=pl.CostEstimate(
            flops=2 * rows * samples * 256, bytes_accessed=rows * samples * 2, transcendentals=0
        ),
        name="transform",
    )(traces, repeated)


def coefficient_kernel(shifts, sides, before, *refs):
    count = len(shifts)
    refs = list(refs)
    offsets = [refs.pop(0) for _ in range(sides)]
    own = [refs.pop(0) for _ in range(count)]
    twin = [refs.pop(0) for _ in range(count)]
    factors = [refs.pop(0) for _ in range(sides)]
    earlier = [refs.pop(0) for _ in range(before)]
    outs = [refs.pop(0) for _ in range(sides)]
    (lhs,) = refs
    groups = lax.axis_size("freq")
    me = lax.axis_index("freq")
    core = lax.rem(lax.axis_index("rows"), 2)
    _, freqs, slots, tile = factors[0].shape
    per_block = own[0].shape[1] // tile
    columns = groups * per_block
    half = 2 * SUBLANES
    deep = 2 * half
    for k in range(freqs):
        for arrays, at in ((own, core), (twin, 1 - core)):
            for b in range(count):
                for inner in range(per_block):
                    start = (b * per_block + inner) * deep + at * half
                    lhs[k, pl.ds(pl.multiple_of(start, half), half), :] = arrays[b][
                        k * half : (k + 1) * half, inner * tile : (inner + 1) * tile
                    ]
    for side in range(sides):
        for k in range(freqs):
            for low in range(0, slots, tile):
                slot = lax.broadcasted_iota(jnp.int32, (deep, tile), 1) + low
                chosen = []
                for part in range(2):
                    products = lax.dot_general(
                        lhs[k],
                        factors[side][part, k, low : low + tile, :],
                        NT,
                        preferred_element_type=jnp.float32,
                    )
                    total = jnp.zeros((deep, tile), jnp.float32)
                    for b, shift in enumerate(shifts):
                        column = (me ^ shift) * per_block
                        value = total
                        for inner in range(per_block):
                            at = (b * per_block + inner) * deep
                            value = jnp.where(
                                slot >= offsets[side][k, 0, column + inner],
                                products[at : at + deep],
                                value,
                            )
                        after = jnp.minimum(column + per_block, columns - 1)
                        end = jnp.where(
                            column + per_block < columns, offsets[side][k, 0, after], slots
                        )
                        total = jnp.where(slot >= end, total, value)
                    chosen.append(total)
                by_real, by_imag = chosen
                n = SUBLANES
                real = [by_real[g : g + n] - by_imag[g + n : g + 2 * n] for g in (0, half)]
                imag = [by_real[g + n : g + 2 * n] + by_imag[g : g + n] for g in (0, half)]
                for c, pieces in enumerate((real, imag)):
                    value = jnp.concatenate(pieces, 0)
                    if side < before:
                        value += earlier[side][k, c, :, low : low + tile].astype(jnp.float32)
                    outs[side][k, c, :, low : low + tile] = value.astype(jnp.bfloat16)


def coefficients(shifts, offsets, own, twin, factors, earlier=()):
    sides, count = len(offsets), len(shifts)
    _, freqs, slots, tile = factors[0].shape
    columns = count * own[0].shape[1] // tile
    shape = jax.ShapeDtypeStruct((freqs, 2, 2 * SUBLANES, slots), jnp.bfloat16)
    return pl.pallas_call(
        functools.partial(coefficient_kernel, tuple(shifts), sides, len(earlier)),
        in_specs=[SMEM] * sides + [VMEM] * (2 * count + sides + len(earlier)),
        out_specs=[VMEM] * sides,
        out_shape=[shape] * sides,
        scratch_shapes=[pltpu.VMEM((freqs, columns * 4 * SUBLANES, tile), jnp.bfloat16)],
        compiler_params=pltpu.CompilerParams(vmem_limit_bytes=16 * 2**20),
        cost_estimate=pl.CostEstimate(
            flops=2 * 2 * sides * freqs * slots * columns * 4 * SUBLANES * tile,
            bytes_accessed=2**20,
            transcendentals=0,
        ),
        name="coefficients",
    )(*offsets, *own, *twin, *factors, *earlier)


def band_kernel(add, at_near, offsets_ref, ranks_ref, coeffs_ref, u_ref, *refs):
    refs = list(refs)
    other_ref = refs.pop(0) if add else None
    out_ref, rhs, crossed = refs[:3]
    freqs, _, sources, slots = coeffs_ref.shape
    tile = u_ref.shape[2]
    place = lax.rem(lax.axis_index("rows") // 2, 2)
    at = place if at_near else 1 - place
    last = offsets_ref.shape[2] - 1
    wide = 2 * sources
    rhs[...] = jnp.zeros_like(rhs)
    crossed[...] = jnp.zeros_like(crossed)
    slot = lax.broadcasted_iota(jnp.int32, (sources, slots), 1)
    for k in range(freqs):
        live = slot < offsets_ref[k, 0, last] + ranks_ref[k, 0, last]
        for part in range(2):
            value = jnp.where(live, coeffs_ref[k, part].astype(jnp.float32), 0.0)
            start = pl.multiple_of((2 * k + part) * wide + at * sources, sources)
            rhs[k, pl.ds(start, sources), :] = value.astype(jnp.bfloat16)
            start = pl.multiple_of((2 * k + 1 - part) * wide + at * sources, sources)
            value = value if part == 0 else -value
            crossed[k, pl.ds(start, sources), :] = value.astype(jnp.bfloat16)
    total = other_ref[...] if add else jnp.zeros((tile, 2 * freqs * wide), jnp.float32)
    for k in range(freqs):
        for part, ref in enumerate((rhs, crossed)):
            total += lax.dot_general(u_ref[part, k], ref[k], NT, preferred_element_type=jnp.float32)
    if not add:
        out_ref[...] = total
        return
    bands, mix = refs[3:]
    groups = out_ref.shape[0]
    bands[...] = total
    packs = LANES // wide
    kinds = 2 * freqs
    block = lax.broadcasted_iota(jnp.int32, (tile // packs, LANES), 1) // wide
    loaded = [bands[pl.ds(b, tile // packs, stride=packs), :] for b in range(packs)]
    rows = tile // packs // groups
    for kind in range(kinds):
        mixed = jnp.zeros((tile // packs, LANES), jnp.float32)
        for b in range(packs):
            shift = (b - kind) * wide % LANES
            moved = pltpu.roll(loaded[b], shift, 1) if shift else loaded[b]
            mixed = jnp.where(block == b, moved, mixed)
        mix[:, kind * rows : (kind + 1) * rows, :] = mixed.reshape(groups, rows, LANES)
    out_ref[...] = mix[...].astype(jnp.bfloat16)


def bands_of(at_near, offsets, ranks, coeffs, u_own, groups, other=None):
    add = other is not None
    freqs, _, sources, slots = coeffs.shape
    tile = u_own.shape[2]
    rows = 2 * freqs * tile * 2 * sources // LANES // groups
    partial = jax.ShapeDtypeStruct((tile, LANES), jnp.float32)
    whole = jax.ShapeDtypeStruct((groups, rows, LANES), jnp.bfloat16)
    spread = pltpu.VMEM((freqs, LANES, slots), jnp.bfloat16)
    mixing = [pltpu.VMEM((tile, LANES), jnp.float32), pltpu.VMEM(whole.shape, jnp.float32)]
    return pl.pallas_call(
        functools.partial(band_kernel, add, at_near),
        in_specs=[SMEM] * 2 + [VMEM] * (3 if add else 2),
        out_specs=VMEM,
        out_shape=whole if add else partial,
        scratch_shapes=[spread, spread] + (mixing if add else []),
        compiler_params=pltpu.CompilerParams(vmem_limit_bytes=8 * 2**20),
        cost_estimate=pl.CostEstimate(
            flops=2 * 2 * freqs * tile * LANES * slots, bytes_accessed=2**20, transcendentals=0
        ),
        name="bands",
    )(offsets, ranks, coeffs, u_own, *([other] if add else []))


def series_kernel(scale, bands_ref, table_ref, out_ref, wide, done, sems):
    groups, rows, lanes = bands_ref.shape
    kinds = table_ref.shape[0]
    steps = groups * rows // kinds
    wide[...] = bands_ref[...].astype(jnp.float32).reshape(groups * rows, lanes) * scale
    copies = []
    for i in range(steps):
        part = wide[pl.ds(i, kinds, stride=steps), :]
        done[i] = jnp.dot(
            part.T.astype(jnp.bfloat16), table_ref[...], preferred_element_type=jnp.float32
        ).astype(jnp.bfloat16)
        copies.append(
            pltpu.make_async_copy(
                done.at[i], out_ref.at[i * lanes : (i + 1) * lanes, :], sems.at[i]
            )
        )
        copies[-1].start()
    for copy in copies:
        copy.wait()


def series_of(bands, table, scale):
    groups, rows, lanes = bands.shape
    kinds, samples = table.shape
    steps = groups * rows // kinds
    return pl.pallas_call(
        functools.partial(series_kernel, scale),
        in_specs=[VMEM] * 2,
        out_specs=pl.BlockSpec(memory_space=pl.ANY),
        out_shape=jax.ShapeDtypeStruct((steps * lanes, samples), jnp.bfloat16),
        scratch_shapes=[
            pltpu.VMEM((groups * rows, lanes), jnp.float32),
            pltpu.VMEM((steps, lanes, samples), jnp.bfloat16),
            pltpu.SemaphoreType.DMA((steps,)),
        ],
        compiler_params=pltpu.CompilerParams(vmem_limit_bytes=16 * 2**20),
        cost_estimate=pl.CostEstimate(
            flops=2 * steps * lanes * kinds * samples,
            bytes_accessed=steps * lanes * samples * 2,
            transcendentals=0,
        ),
        name="series",
    )(bands, table)


def fits(rec_dev, src_dev, samples, freq_dev, rows_dev, tile, slots, freq_group, row_group):
    kinds = 2 * freq_dev * freq_group
    ratio = math.sqrt(samples) / math.sqrt(freq_dev * freq_group)
    return (
        math.frexp(ratio)[0] == 0.5
        and math.sqrt(samples).is_integer()
        and src_dev == SUBLANES
        and row_group == 4
        and rows_dev == 1
        and freq_group in PAIRED
        and rec_dev % tile == 0
        and tile % (2 * LANES) == 0
        and slots % tile == 0
        and LANES % kinds == 0
        and SUBLANES % (LANES // kinds) == 0
        and 2 * freq_dev * src_dev * row_group == LANES
        and tile % (4 * SUBLANES * freq_group) == 0
    )


def shift_order(groups):
    return [(groups // 2 - 1 - 2 * i) % (groups - 1) + 1 for i in range(groups - 1)]


def arrivals(groups):
    order = shift_order(groups)
    late = [s for s in order if s >= groups // 2][-LATE:]
    return [0] + [s for s in order if s not in late], late


def per_device_fast(wavefield, u_factors, v_factors, tile_ranks, tile_offsets):
    rec_dev, src_dev, samples = wavefield.shape
    freq_dev = u_factors.shape[1]
    groups = lax.axis_size("freq")
    row_group = lax.axis_size("rows")
    freqs = freq_dev * groups
    sources = src_dev * row_group
    tile = u_factors.shape[3]
    across = [(i, i ^ 2) for i in range(row_group)]
    beside = [(i, i ^ 1) for i in range(row_group)]
    forward, _ = spectral_tables(freqs, samples)
    u_own, v_own = u_factors[:, :, 0], v_factors[:, :, 0]
    v_far = lax.ppermute(v_own, "rows", across)
    offsets_far = lax.ppermute(tile_offsets, "rows", across)
    table = forward.reshape(2 * freqs, samples)
    sent = transform(wavefield.reshape(rec_dev * src_dev, samples), table, groups)
    own = {0: sent[0]}
    for shift in shift_order(groups):
        swap = [(i, i ^ shift) for i in range(groups)]
        own[shift] = lax.ppermute(sent[shift], "freq", swap)
    early, late = arrivals(groups)
    own_early, own_late = [own[s] for s in early], [own[s] for s in late]
    twin_early = []
    for shift, block in zip(early, own_early):
        twin_early.append(lax.ppermute(block, "rows", beside))
    (near,) = coefficients(early, [tile_offsets], own_early, twin_early, [v_own])
    (leaving,) = coefficients(early, [offsets_far], own_early, twin_early, [v_far])
    own_late, near, leaving = lax.optimization_barrier((own_late, near, leaving))
    twin_late = [lax.ppermute(block, "rows", beside) for block in own_late]
    (leaving,) = coefficients(late, [offsets_far], own_late, twin_late, [v_far], [leaving])
    far = lax.ppermute(leaving, "rows", across)
    (near,) = coefficients(late, [tile_offsets], own_late, twin_late, [v_own], [near])
    half = bands_of(True, tile_offsets, tile_ranks, near, u_own, groups)
    bands = bands_of(False, tile_offsets, tile_ranks, far, u_own, groups, half)
    returned = lax.all_to_all(bands, "freq", split_axis=0, concat_axis=0, tiled=True)
    series = series_of(returned, table, math.sqrt(samples) / math.sqrt(freqs))
    return series.reshape(tile // groups, sources, samples)


def choose(wavefield, u_factors, v_factors, tile_ranks, tile_offsets):
    ok = fits(
        wavefield.shape[0],
        wavefield.shape[1],
        wavefield.shape[2],
        u_factors.shape[1],
        u_factors.shape[2],
        u_factors.shape[3],
        u_factors.shape[4],
        lax.axis_size("freq"),
        lax.axis_size("rows"),
    )
    step = per_device_fast if ok else per_device
    return step(wavefield, u_factors, v_factors, tile_ranks, tile_offsets)


def solution(mesh):
    placed = (
        P("freq", "rows", None),
        P(None, "freq", "rows", None, None),
        P(None, "freq", "rows", None, None),
        P("freq", "rows", None),
        P("freq", "rows", None),
    )
    return jax.shard_map(
        choose,
        mesh=mesh,
        in_specs=placed,
        out_specs=P(("rows", "freq"), None, None),
        check_vma=False,
    )
```

```python
import functools
import math

import jax
import jax.numpy as jnp
from jax import lax
from jax.experimental import pallas as pl
from jax.experimental.pallas import tpu as pltpu
from jax.sharding import PartitionSpec as P


RANK_MAX = 64
LANES = 128
SUBLANES = 8
NT = (((1,), (1,)), ((), ()))
VMEM = pl.BlockSpec(memory_space=pltpu.VMEM)
SMEM = pl.BlockSpec(memory_space=pltpu.SMEM)
LATE = 2
PAIRED = (4, 8, 16)
AHEAD = 3


def spectral_tables(freq_count, sample_count):
    freq_bins = jnp.arange(freq_count, dtype=jnp.int32) + 1
    sample_index = jnp.arange(sample_count, dtype=jnp.int32)
    phase_int = freq_bins[:, None] * sample_index[None, :] % sample_count
    angles = phase_int.astype(jnp.float32) * (2.0 * math.pi / sample_count)
    cosine = jnp.cos(angles)
    minus_sine = -jnp.sin(angles)
    stacked = jnp.stack([cosine, minus_sine], axis=1)
    forward = (stacked / math.sqrt(sample_count)).astype(jnp.bfloat16)
    inverse = (stacked / math.sqrt(freq_count)).astype(jnp.bfloat16)
    return (forward, inverse)


def tile_windows(v_row, u_row, starts, rank_max):
    columns = starts.shape[0]
    slot_index = (starts[:, None] + jnp.arange(rank_max, dtype=jnp.int32)[None, :]).reshape(-1)
    v_padded = jnp.pad(v_row, ((0, 0), (0, rank_max), (0, 0)))
    u_padded = jnp.pad(u_row, ((0, 0), (0, 0), (0, rank_max)))
    v_win = jnp.take(v_padded, slot_index, axis=1).reshape(2, columns, rank_max, v_row.shape[2])
    u_win = jnp.take(u_padded, slot_index, axis=2).reshape(2, u_row.shape[1], columns, rank_max)
    return (v_win, u_win)


def slot_lookup(starts, counts, rank_max, slot_count):
    position = jnp.arange(slot_count, dtype=jnp.int32)
    started = starts[:, None, :] <= position[None, :, None]
    owner_tile = jnp.sum(started.astype(jnp.int32), axis=2) - 1
    first_slot = jnp.max(jnp.where(started, starts[:, None, :], 0), axis=2)
    within = position[None, :] - first_slot
    live_slot = position[None, :] < (starts[:, -1] + counts[:, -1])[:, None]
    flat_index = jnp.where(live_slot, owner_tile * rank_max + within, 0)
    return (flat_index, live_slot)


def take_slots(values, chosen):
    return jnp.take(values, chosen, axis=1)


def per_device(wavefield, u_factors, v_factors, tile_ranks, tile_offsets):
    rec_dev, src_dev, samples = wavefield.shape
    freq_dev = u_factors.shape[1]
    rows_dev = u_factors.shape[2]
    tile_size = u_factors.shape[3]
    slot_count = u_factors.shape[4]
    freq_group = lax.axis_size("freq")
    row_group = lax.axis_size("rows")
    freqs = freq_dev * freq_group
    receivers = rec_dev * freq_group
    columns = receivers // tile_size
    sources = src_dev * row_group
    forward, inverse = spectral_tables(freqs, samples)
    spectrum = jnp.einsum("kct,rst->kcrs", forward, wavefield, preferred_element_type=jnp.float32)
    spectrum = spectrum.astype(jnp.bfloat16).reshape(freqs, 2, rec_dev * src_dev)
    windows = jax.vmap(
        functools.partial(tile_windows, rank_max=RANK_MAX), in_axes=(1, 1, 0), out_axes=(1, 1)
    )
    rank_slots = jnp.arange(RANK_MAX, dtype=jnp.int32)
    tile_row = 0
    v_win, u_win = windows(
        v_factors[:, :, tile_row], u_factors[:, :, tile_row], tile_offsets[:, tile_row]
    )
    rank_mask = rank_slots[None, None, :] < tile_ranks[:, tile_row, :, None]
    flat_index, live_slot = slot_lookup(
        tile_offsets[:, tile_row], tile_ranks[:, tile_row], RANK_MAX, slot_count
    )
    prepared = [(v_win, u_win, rank_mask, flat_index, live_slot)]
    by_frequency = lax.all_to_all(spectrum, "freq", split_axis=0, concat_axis=2, tiled=True)
    portion = lax.all_gather(by_frequency[None], "rows", axis=0, tiled=True)
    blocks_in = portion.shape[0]
    spectra = portion.reshape(blocks_in, freq_dev, 2, columns, tile_size, src_dev)
    spectra = jnp.transpose(spectra, (1, 2, 3, 4, 0, 5)).reshape(
        freq_dev, 2, columns, tile_size, blocks_in * src_dev
    )
    tile_row = 0
    v_win, u_win, rank_mask, flat_index, live_slot = prepared[tile_row]
    quadrants = jnp.einsum(
        "afjmr,fbjrs->fabjms", v_win, spectra, preferred_element_type=jnp.float32
    )
    coeffs = jnp.stack(
        [quadrants[:, 0, 0] - quadrants[:, 1, 1], quadrants[:, 0, 1] + quadrants[:, 1, 0]], axis=1
    )
    coeffs = jnp.where(rank_mask[:, None, :, :, None], coeffs, 0.0).astype(jnp.bfloat16)
    stacked = coeffs.reshape(freq_dev, 2, columns * RANK_MAX, blocks_in * src_dev)
    packed = jax.vmap(take_slots)(stacked, flat_index)
    packed = jnp.where(live_slot[:, None, :, None], packed, jnp.zeros((), jnp.bfloat16))
    products = jnp.einsum(
        "afrk,fcks->facrs", u_factors[:, :, tile_row], packed, preferred_element_type=jnp.float32
    )
    results = [
        jnp.stack(
            [products[:, 0, 0] - products[:, 1, 1], products[:, 0, 1] + products[:, 1, 0]], axis=1
        )
    ]
    merged = jnp.stack(results, axis=2)
    bands = merged.astype(jnp.bfloat16).reshape(
        freq_dev, 2, rows_dev * tile_size, blocks_in, src_dev
    )
    bands = bands.reshape(freq_dev, 2, rows_dev * tile_size * sources)
    returned = lax.all_to_all(bands, "freq", split_axis=2, concat_axis=0, tiled=True)
    series = jnp.einsum("kcq,kct->qt", returned, inverse, preferred_element_type=jnp.float32)
    return series.astype(jnp.bfloat16).reshape(rows_dev * tile_size // freq_group, sources, samples)


def transform_kernel(traces_ref, table_ref, *refs):
    groups = lax.axis_size("freq")
    outs, (traces, sems, products, turned) = refs[:groups], refs[groups:]
    me = lax.axis_index("freq")
    rows = products.shape[1]
    kinds = turned.shape[0] // SUBLANES
    packs = LANES // kinds
    blocks = traces_ref.shape[0] // rows
    each = outs[0].shape[0]

    def copy(i):
        part = pl.ds(pl.multiple_of(i * rows, rows), rows)
        return pltpu.make_async_copy(traces_ref.at[part, :], traces.at[part, :], sems.at[i])

    def turn(i, source_rows):
        place = lax.broadcasted_iota(jnp.int32, (rows // SUBLANES, LANES), 1) // kinds
        for first in range(0, SUBLANES, packs):
            mixed = source_rows[pl.ds(first, rows // SUBLANES, stride=SUBLANES), :]
            for m in range(1, packs):
                part = source_rows[pl.ds(first + m, rows // SUBLANES, stride=SUBLANES), :]
                mixed = jnp.where(place == m, part, mixed)
            mixed = mixed.T
            for m in range(packs):
                turned[pl.ds(first + m, kinds, stride=SUBLANES), :] = mixed[
                    m * kinds : (m + 1) * kinds
                ]
        lanes = pl.ds(pl.multiple_of(i * LANES, LANES), LANES)
        for shift, out in enumerate(outs):
            group = me ^ shift
            start = pl.multiple_of(group * each, each)
            out[:, lanes] = turned[pl.ds(start, each), :].astype(jnp.bfloat16)

    for i in range(min(AHEAD, blocks)):
        copy(i).start()

    def step(i, carry):
        now = lax.rem(i, 2)

        @pl.when(i + AHEAD < blocks)
        def _():
            copy(i + AHEAD).start()

        copy(i).wait()
        part = pl.ds(pl.multiple_of(i * rows, rows), rows)
        turn(jnp.maximum(i - 1, 0), products.at[1 - now])
        products[now] = lax.dot_general(
            traces[part, :], table_ref[...], NT, preferred_element_type=jnp.float32
        )
        return carry

    lax.fori_loop(0, blocks, step, 0)
    turn(blocks - 1, products.at[(blocks - 1) % 2])


def transform(traces, table, groups):
    rows, samples = traces.shape
    receivers = rows // SUBLANES
    kinds = table.shape[0]
    repeated = jnp.tile(table, (LANES // kinds, 1))
    shape = jax.ShapeDtypeStruct((kinds * SUBLANES // groups, receivers), jnp.bfloat16)
    return pl.pallas_call(
        transform_kernel,
        in_specs=[pl.BlockSpec(memory_space=pltpu.HBM), VMEM],
        out_specs=[VMEM] * groups,
        out_shape=[shape] * groups,
        scratch_shapes=[
            pltpu.VMEM((rows, samples), jnp.bfloat16),
            pltpu.SemaphoreType.DMA((receivers // LANES,)),
            pltpu.VMEM((2, LANES * SUBLANES, LANES), jnp.float32),
            pltpu.VMEM((kinds * SUBLANES, LANES), jnp.float32),
        ],
        compiler_params=pltpu.CompilerParams(vmem_limit_bytes=45 * 2**20),
        cost_estimate=pl.CostEstimate(
            flops=2 * rows * samples * 256, bytes_accessed=rows * samples * 2, transcendentals=0
        ),
        name="transform",
    )(traces, repeated)


def coefficient_kernel(shifts, sides, before, *refs):
    count = len(shifts)
    refs = list(refs)
    offsets = [refs.pop(0) for _ in range(sides)]
    arrays = [refs.pop(0) for _ in range(count)]
    factors = [refs.pop(0) for _ in range(sides)]
    earlier = [refs.pop(0) for _ in range(before)]
    outs = [refs.pop(0) for _ in range(sides)]
    (lhs,) = refs
    groups = lax.axis_size("freq")
    me = lax.axis_index("freq")
    _, freqs, slots, tile = factors[0].shape
    per_block = arrays[0].shape[1] // tile
    columns = groups * per_block
    n = SUBLANES
    deep = 2 * n
    for k in range(freqs):
        for b in range(count):
            for inner in range(per_block):
                start = (b * per_block + inner) * deep
                lhs[k, start : start + deep, :] = arrays[b][
                    k * deep : (k + 1) * deep, inner * tile : (inner + 1) * tile
                ]
    for side in range(sides):
        for k in range(freqs):
            for low in range(0, slots, tile):
                slot = lax.broadcasted_iota(jnp.int32, (deep, tile), 1) + low
                chosen = []
                for part in range(2):
                    products = lax.dot_general(
                        lhs[k],
                        factors[side][part, k, low : low + tile, :],
                        NT,
                        preferred_element_type=jnp.float32,
                    )
                    total = jnp.zeros((deep, tile), jnp.float32)
                    for b, shift in enumerate(shifts):
                        column = (me ^ shift) * per_block
                        value = total
                        for inner in range(per_block):
                            at = (b * per_block + inner) * deep
                            value = jnp.where(
                                slot >= offsets[side][k, 0, column + inner],
                                products[at : at + deep],
                                value,
                            )
                        after = jnp.minimum(column + per_block, columns - 1)
                        end = jnp.where(
                            column + per_block < columns, offsets[side][k, 0, after], slots
                        )
                        total = jnp.where(slot >= end, total, value)
                    chosen.append(total)
                by_real, by_imag = chosen
                value = jnp.concatenate(
                    [by_real[:n] - by_imag[n:], by_real[n:] + by_imag[:n]], axis=0
                )
                if side < before:
                    value += earlier[side][k, :, low : low + tile].astype(jnp.float32)
                outs[side][k, :, low : low + tile] = value.astype(jnp.bfloat16)


def coefficients(shifts, offsets, arrays, factors, earlier=()):
    sides, count = len(offsets), len(shifts)
    _, freqs, slots, tile = factors[0].shape
    rows = count * arrays[0].shape[1] // tile * 2 * SUBLANES
    shape = jax.ShapeDtypeStruct((freqs, 2 * SUBLANES, slots), jnp.bfloat16)
    return pl.pallas_call(
        functools.partial(coefficient_kernel, tuple(shifts), sides, len(earlier)),
        in_specs=[SMEM] * sides + [VMEM] * (count + sides + len(earlier)),
        out_specs=[VMEM] * sides,
        out_shape=[shape] * sides,
        scratch_shapes=[pltpu.VMEM((freqs, rows, tile), jnp.bfloat16)],
        compiler_params=pltpu.CompilerParams(vmem_limit_bytes=12 * 2**20),
        cost_estimate=pl.CostEstimate(
            flops=2 * 4 * sides * freqs * slots * rows * tile,
            bytes_accessed=2**20,
            transcendentals=0,
        ),
        name="coefficients",
    )(*offsets, *arrays, *factors, *earlier)


def band_kernel(add, at_near, offsets_ref, ranks_ref, same_ref, cross_ref, u_ref, *refs):
    refs = list(refs)
    other_ref = refs.pop(0) if add else None
    out_ref, rhs, crossed = refs[:3]
    freqs, sources, slots = same_ref.shape
    tile = u_ref.shape[2]
    first = lax.rem(lax.axis_index("rows"), 2) == 0
    place = lax.rem(lax.axis_index("rows") // 2, 2)
    n = SUBLANES
    at = place if at_near else 1 - place
    last = offsets_ref.shape[2] - 1
    wide = 2 * sources
    rhs[...] = jnp.zeros_like(rhs)
    crossed[...] = jnp.zeros_like(crossed)
    slot = lax.broadcasted_iota(jnp.int32, (sources, slots), 1)
    for k in range(freqs):
        live = slot < offsets_ref[k, 0, last] + ranks_ref[k, 0, last]
        same, cross = same_ref[k].astype(jnp.float32), cross_ref[k].astype(jnp.float32)
        low, high = jnp.where(first, same, cross), jnp.where(first, cross, same)
        for part in range(2):
            rows = slice(part * n, (part + 1) * n)
            value = jnp.where(live, jnp.concatenate([low[rows], high[rows]], axis=0), 0.0)
            start = pl.multiple_of((2 * k + part) * wide + at * sources, sources)
            rhs[k, pl.ds(start, sources), :] = value.astype(jnp.bfloat16)
            start = pl.multiple_of((2 * k + 1 - part) * wide + at * sources, sources)
            value = value if part == 0 else -value
            crossed[k, pl.ds(start, sources), :] = value.astype(jnp.bfloat16)
    total = other_ref[...] if add else jnp.zeros((tile, 2 * freqs * wide), jnp.float32)
    for k in range(freqs):
        for part, ref in enumerate((rhs, crossed)):
            total += lax.dot_general(u_ref[part, k], ref[k], NT, preferred_element_type=jnp.float32)
    if not add:
        out_ref[...] = total
        return
    bands, mix = refs[3:]
    groups = out_ref.shape[0]
    bands[...] = total
    packs = LANES // wide
    kinds = 2 * freqs
    block = lax.broadcasted_iota(jnp.int32, (tile // packs, LANES), 1) // wide
    loaded = [bands[pl.ds(b, tile // packs, stride=packs), :] for b in range(packs)]
    rows = tile // packs // groups
    for kind in range(kinds):
        mixed = jnp.zeros((tile // packs, LANES), jnp.float32)
        for b in range(packs):
            shift = (b - kind) * wide % LANES
            moved = pltpu.roll(loaded[b], shift, 1) if shift else loaded[b]
            mixed = jnp.where(block == b, moved, mixed)
        mix[:, kind * rows : (kind + 1) * rows, :] = mixed.reshape(groups, rows, LANES)
    out_ref[...] = mix[...].astype(jnp.bfloat16)


def bands_of(at_near, offsets, ranks, same, cross, u_own, groups, other=None):
    add = other is not None
    freqs, sources, slots = same.shape
    tile = u_own.shape[2]
    rows = 2 * freqs * tile * 2 * sources // LANES // groups
    partial = jax.ShapeDtypeStruct((tile, LANES), jnp.float32)
    whole = jax.ShapeDtypeStruct((groups, rows, LANES), jnp.bfloat16)
    spread = pltpu.VMEM((freqs, LANES, slots), jnp.bfloat16)
    mixing = [pltpu.VMEM((tile, LANES), jnp.float32), pltpu.VMEM(whole.shape, jnp.float32)]
    return pl.pallas_call(
        functools.partial(band_kernel, add, at_near),
        in_specs=[SMEM] * 2 + [VMEM] * (4 if add else 3),
        out_specs=VMEM,
        out_shape=whole if add else partial,
        scratch_shapes=[spread, spread] + (mixing if add else []),
        compiler_params=pltpu.CompilerParams(vmem_limit_bytes=8 * 2**20),
        cost_estimate=pl.CostEstimate(
            flops=2 * 2 * freqs * tile * LANES * slots, bytes_accessed=2**20, transcendentals=0
        ),
        name="bands",
    )(offsets, ranks, same, cross, u_own, *([other] if add else []))


def series_kernel(scale, bands_ref, table_ref, out_ref, wide, done, sems):
    groups, rows, lanes = bands_ref.shape
    kinds = table_ref.shape[0]
    steps = groups * rows // kinds
    wide[...] = bands_ref[...].astype(jnp.float32).reshape(groups * rows, lanes) * scale
    copies = []
    for i in range(steps):
        part = wide[pl.ds(i, kinds, stride=steps), :]
        done[i] = jnp.dot(
            part.T.astype(jnp.bfloat16), table_ref[...], preferred_element_type=jnp.float32
        ).astype(jnp.bfloat16)
        copies.append(
            pltpu.make_async_copy(
                done.at[i], out_ref.at[i * lanes : (i + 1) * lanes, :], sems.at[i]
            )
        )
        copies[-1].start()
    for copy in copies:
        copy.wait()


def series_of(bands, table, scale):
    groups, rows, lanes = bands.shape
    kinds, samples = table.shape
    steps = groups * rows // kinds
    return pl.pallas_call(
        functools.partial(series_kernel, scale),
        in_specs=[VMEM] * 2,
        out_specs=pl.BlockSpec(memory_space=pl.ANY),
        out_shape=jax.ShapeDtypeStruct((steps * lanes, samples), jnp.bfloat16),
        scratch_shapes=[
            pltpu.VMEM((groups * rows, lanes), jnp.float32),
            pltpu.VMEM((steps, lanes, samples), jnp.bfloat16),
            pltpu.SemaphoreType.DMA((steps,)),
        ],
        compiler_params=pltpu.CompilerParams(vmem_limit_bytes=16 * 2**20),
        cost_estimate=pl.CostEstimate(
            flops=2 * steps * lanes * kinds * samples,
            bytes_accessed=steps * lanes * samples * 2,
            transcendentals=0,
        ),
        name="series",
    )(bands, table)


def fits(rec_dev, src_dev, samples, freq_dev, rows_dev, tile, slots, freq_group, row_group):
    kinds = 2 * freq_dev * freq_group
    ratio = math.sqrt(samples) / math.sqrt(freq_dev * freq_group)
    return (
        math.frexp(ratio)[0] == 0.5
        and math.sqrt(samples).is_integer()
        and src_dev == SUBLANES
        and row_group == 4
        and rows_dev == 1
        and freq_group in PAIRED
        and rec_dev % tile == 0
        and tile % (2 * LANES) == 0
        and slots % tile == 0
        and LANES % kinds == 0
        and SUBLANES % (LANES // kinds) == 0
        and 2 * freq_dev * src_dev * row_group == LANES
        and tile % (4 * SUBLANES * freq_group) == 0
    )


def shift_order(groups):
    return [(groups // 2 - 1 - 2 * i) % (groups - 1) + 1 for i in range(groups - 1)]


def arrivals(groups):
    order = shift_order(groups)
    late = [s for s in order if s >= groups // 2][-LATE:]
    return [0] + [s for s in order if s not in late], late


def per_device_fast(wavefield, u_factors, v_factors, tile_ranks, tile_offsets):
    rec_dev, src_dev, samples = wavefield.shape
    freq_dev = u_factors.shape[1]
    groups = lax.axis_size("freq")
    row_group = lax.axis_size("rows")
    freqs = freq_dev * groups
    sources = src_dev * row_group
    tile = u_factors.shape[3]

    def swapped(value, bits):
        return lax.ppermute(value, "rows", [(i, i ^ bits) for i in range(row_group)])

    twin, far, both = 1, 2, 3
    forward, _ = spectral_tables(freqs, samples)
    u_own, v_own = u_factors[:, :, 0], v_factors[:, :, 0]
    v_far = swapped(v_own, far)
    v_twin = swapped(v_own, twin)
    table = forward.reshape(2 * freqs, samples)
    offsets = [tile_offsets] + [swapped(tile_offsets, bits) for bits in (twin, far, both)]
    sent = transform(wavefield.reshape(rec_dev * src_dev, samples), table, groups)
    blocks = {0: sent[0]}
    for shift in shift_order(groups):
        swap = [(i, i ^ shift) for i in range(groups)]
        blocks[shift] = lax.ppermute(sent[shift], "freq", swap)
    early, late = arrivals(groups)
    soon, later = [blocks[s] for s in early], [blocks[s] for s in late]
    own, to_twin = coefficients(early, offsets[:2], soon, [v_own, v_twin])
    v_far, own, to_twin = lax.optimization_barrier((v_far, own, to_twin))
    v_both = swapped(v_far, twin)
    (to_far,) = coefficients(early, offsets[2:3], soon, [v_far])
    v_both, to_far = lax.optimization_barrier((v_both, to_far))
    (to_both,) = coefficients(early, offsets[3:], soon, [v_both])
    later, to_both, to_far = lax.optimization_barrier((later, to_both, to_far))
    to_far, to_both = coefficients(late, offsets[2:], later, [v_far, v_both], [to_far, to_both])
    later, to_far, to_both = lax.optimization_barrier((later, to_far, to_both))
    from_far, from_both = swapped(to_far, far), swapped(to_both, both)
    own, to_twin = coefficients(late, offsets[:2], later, [v_own, v_twin], [own, to_twin])
    from_twin = swapped(to_twin, twin)
    half = bands_of(True, tile_offsets, tile_ranks, own, from_twin, u_own, groups)
    bands = bands_of(False, tile_offsets, tile_ranks, from_far, from_both, u_own, groups, half)
    returned = lax.all_to_all(bands, "freq", split_axis=0, concat_axis=0, tiled=True)
    series = series_of(returned, table, math.sqrt(samples) / math.sqrt(freqs))
    return series.reshape(tile // groups, sources, samples)


def choose(wavefield, u_factors, v_factors, tile_ranks, tile_offsets):
    ok = fits(
        wavefield.shape[0],
        wavefield.shape[1],
        wavefield.shape[2],
        u_factors.shape[1],
        u_factors.shape[2],
        u_factors.shape[3],
        u_factors.shape[4],
        lax.axis_size("freq"),
        lax.axis_size("rows"),
    )
    step = per_device_fast if ok else per_device
    return step(wavefield, u_factors, v_factors, tile_ranks, tile_offsets)


def solution(mesh):
    placed = (
        P("freq", "rows", None),
        P(None, "freq", "rows", None, None),
        P(None, "freq", "rows", None, None),
        P("freq", "rows", None),
        P("freq", "rows", None),
    )
    return jax.shard_map(
        choose,
        mesh=mesh,
        in_specs=placed,
        out_specs=P(("rows", "freq"), None, None),
        check_vma=False,
    )
```

```python
import functools
import math

import jax
import jax.numpy as jnp
from jax import lax
from jax.experimental import pallas as pl
from jax.experimental.pallas import tpu as pltpu
from jax.sharding import PartitionSpec as P


RANK_MAX = 64
LANES = 128
SUBLANES = 8
NT = (((1,), (1,)), ((), ()))
VMEM = pl.BlockSpec(memory_space=pltpu.VMEM)
SMEM = pl.BlockSpec(memory_space=pltpu.SMEM)
PAIRED = (4, 8, 16)
AHEAD = 3


def spectral_tables(freq_count, sample_count):
    freq_bins = jnp.arange(freq_count, dtype=jnp.int32) + 1
    sample_index = jnp.arange(sample_count, dtype=jnp.int32)
    phase_int = freq_bins[:, None] * sample_index[None, :] % sample_count
    angles = phase_int.astype(jnp.float32) * (2.0 * math.pi / sample_count)
    cosine = jnp.cos(angles)
    minus_sine = -jnp.sin(angles)
    stacked = jnp.stack([cosine, minus_sine], axis=1)
    forward = (stacked / math.sqrt(sample_count)).astype(jnp.bfloat16)
    inverse = (stacked / math.sqrt(freq_count)).astype(jnp.bfloat16)
    return (forward, inverse)


def tile_windows(v_row, u_row, starts, rank_max):
    columns = starts.shape[0]
    slot_index = (starts[:, None] + jnp.arange(rank_max, dtype=jnp.int32)[None, :]).reshape(-1)
    v_padded = jnp.pad(v_row, ((0, 0), (0, rank_max), (0, 0)))
    u_padded = jnp.pad(u_row, ((0, 0), (0, 0), (0, rank_max)))
    v_win = jnp.take(v_padded, slot_index, axis=1).reshape(2, columns, rank_max, v_row.shape[2])
    u_win = jnp.take(u_padded, slot_index, axis=2).reshape(2, u_row.shape[1], columns, rank_max)
    return (v_win, u_win)


def slot_lookup(starts, counts, rank_max, slot_count):
    position = jnp.arange(slot_count, dtype=jnp.int32)
    started = starts[:, None, :] <= position[None, :, None]
    owner_tile = jnp.sum(started.astype(jnp.int32), axis=2) - 1
    first_slot = jnp.max(jnp.where(started, starts[:, None, :], 0), axis=2)
    within = position[None, :] - first_slot
    live_slot = position[None, :] < (starts[:, -1] + counts[:, -1])[:, None]
    flat_index = jnp.where(live_slot, owner_tile * rank_max + within, 0)
    return (flat_index, live_slot)


def take_slots(values, chosen):
    return jnp.take(values, chosen, axis=1)


def per_device(wavefield, u_factors, v_factors, tile_ranks, tile_offsets):
    rec_dev, src_dev, samples = wavefield.shape
    freq_dev = u_factors.shape[1]
    rows_dev = u_factors.shape[2]
    tile_size = u_factors.shape[3]
    slot_count = u_factors.shape[4]
    freq_group = lax.axis_size("freq")
    row_group = lax.axis_size("rows")
    freqs = freq_dev * freq_group
    receivers = rec_dev * freq_group
    columns = receivers // tile_size
    sources = src_dev * row_group
    forward, inverse = spectral_tables(freqs, samples)
    spectrum = jnp.einsum("kct,rst->kcrs", forward, wavefield, preferred_element_type=jnp.float32)
    spectrum = spectrum.astype(jnp.bfloat16).reshape(freqs, 2, rec_dev * src_dev)
    windows = jax.vmap(
        functools.partial(tile_windows, rank_max=RANK_MAX), in_axes=(1, 1, 0), out_axes=(1, 1)
    )
    rank_slots = jnp.arange(RANK_MAX, dtype=jnp.int32)
    tile_row = 0
    v_win, u_win = windows(
        v_factors[:, :, tile_row], u_factors[:, :, tile_row], tile_offsets[:, tile_row]
    )
    rank_mask = rank_slots[None, None, :] < tile_ranks[:, tile_row, :, None]
    flat_index, live_slot = slot_lookup(
        tile_offsets[:, tile_row], tile_ranks[:, tile_row], RANK_MAX, slot_count
    )
    prepared = [(v_win, u_win, rank_mask, flat_index, live_slot)]
    by_frequency = lax.all_to_all(spectrum, "freq", split_axis=0, concat_axis=2, tiled=True)
    portion = lax.all_gather(by_frequency[None], "rows", axis=0, tiled=True)
    blocks_in = portion.shape[0]
    spectra = portion.reshape(blocks_in, freq_dev, 2, columns, tile_size, src_dev)
    spectra = jnp.transpose(spectra, (1, 2, 3, 4, 0, 5)).reshape(
        freq_dev, 2, columns, tile_size, blocks_in * src_dev
    )
    tile_row = 0
    v_win, u_win, rank_mask, flat_index, live_slot = prepared[tile_row]
    quadrants = jnp.einsum(
        "afjmr,fbjrs->fabjms", v_win, spectra, preferred_element_type=jnp.float32
    )
    coeffs = jnp.stack(
        [quadrants[:, 0, 0] - quadrants[:, 1, 1], quadrants[:, 0, 1] + quadrants[:, 1, 0]], axis=1
    )
    coeffs = jnp.where(rank_mask[:, None, :, :, None], coeffs, 0.0).astype(jnp.bfloat16)
    stacked = coeffs.reshape(freq_dev, 2, columns * RANK_MAX, blocks_in * src_dev)
    packed = jax.vmap(take_slots)(stacked, flat_index)
    packed = jnp.where(live_slot[:, None, :, None], packed, jnp.zeros((), jnp.bfloat16))
    products = jnp.einsum(
        "afrk,fcks->facrs", u_factors[:, :, tile_row], packed, preferred_element_type=jnp.float32
    )
    results = [
        jnp.stack(
            [products[:, 0, 0] - products[:, 1, 1], products[:, 0, 1] + products[:, 1, 0]], axis=1
        )
    ]
    merged = jnp.stack(results, axis=2)
    bands = merged.astype(jnp.bfloat16).reshape(
        freq_dev, 2, rows_dev * tile_size, blocks_in, src_dev
    )
    bands = bands.reshape(freq_dev, 2, rows_dev * tile_size * sources)
    returned = lax.all_to_all(bands, "freq", split_axis=2, concat_axis=0, tiled=True)
    series = jnp.einsum("kcq,kct->qt", returned, inverse, preferred_element_type=jnp.float32)
    return series.astype(jnp.bfloat16).reshape(rows_dev * tile_size // freq_group, sources, samples)


def transform_kernel(traces_ref, table_ref, *refs):
    groups = lax.axis_size("freq")
    outs, (traces, sems, products, turned) = refs[:groups], refs[groups:]
    me = lax.axis_index("freq")
    rows = products.shape[1]
    kinds = turned.shape[0] // SUBLANES
    packs = LANES // kinds
    blocks = traces_ref.shape[0] // rows
    each = outs[0].shape[0]

    def copy(i):
        part = pl.ds(pl.multiple_of(i * rows, rows), rows)
        return pltpu.make_async_copy(traces_ref.at[part, :], traces.at[part, :], sems.at[i])

    def turn(i, source_rows):
        place = lax.broadcasted_iota(jnp.int32, (rows // SUBLANES, LANES), 1) // kinds
        for first in range(0, SUBLANES, packs):
            mixed = source_rows[pl.ds(first, rows // SUBLANES, stride=SUBLANES), :]
            for m in range(1, packs):
                part = source_rows[pl.ds(first + m, rows // SUBLANES, stride=SUBLANES), :]
                mixed = jnp.where(place == m, part, mixed)
            mixed = mixed.T
            for m in range(packs):
                turned[pl.ds(first + m, kinds, stride=SUBLANES), :] = mixed[
                    m * kinds : (m + 1) * kinds
                ]
        lanes = pl.ds(pl.multiple_of(i * LANES, LANES), LANES)
        for shift, out in enumerate(outs):
            group = me ^ shift
            start = pl.multiple_of(group * each, each)
            out[:, lanes] = turned[pl.ds(start, each), :].astype(jnp.bfloat16)

    for i in range(min(AHEAD, blocks)):
        copy(i).start()

    def step(i, carry):
        now = lax.rem(i, 2)

        @pl.when(i + AHEAD < blocks)
        def _():
            copy(i + AHEAD).start()

        copy(i).wait()
        part = pl.ds(pl.multiple_of(i * rows, rows), rows)
        turn(jnp.maximum(i - 1, 0), products.at[1 - now])
        products[now] = lax.dot_general(
            traces[part, :], table_ref[...], NT, preferred_element_type=jnp.float32
        )
        return carry

    lax.fori_loop(0, blocks, step, 0)
    turn(blocks - 1, products.at[(blocks - 1) % 2])


def transform(traces, table, groups):
    rows, samples = traces.shape
    receivers = rows // SUBLANES
    kinds = table.shape[0]
    repeated = jnp.tile(table, (LANES // kinds, 1))
    shape = jax.ShapeDtypeStruct((kinds * SUBLANES // groups, receivers), jnp.bfloat16)
    return pl.pallas_call(
        transform_kernel,
        in_specs=[pl.BlockSpec(memory_space=pltpu.HBM), VMEM],
        out_specs=[VMEM] * groups,
        out_shape=[shape] * groups,
        scratch_shapes=[
            pltpu.VMEM((rows, samples), jnp.bfloat16),
            pltpu.SemaphoreType.DMA((receivers // LANES,)),
            pltpu.VMEM((2, LANES * SUBLANES, LANES), jnp.float32),
            pltpu.VMEM((kinds * SUBLANES, LANES), jnp.float32),
        ],
        compiler_params=pltpu.CompilerParams(vmem_limit_bytes=48 * 2**20),
        cost_estimate=pl.CostEstimate(
            flops=2 * rows * samples * 256, bytes_accessed=rows * samples * 2, transcendentals=0
        ),
        name="transform",
    )(traces, repeated)


def coefficient_kernel(shifts, sides, before, *refs):
    count = len(shifts)
    refs = list(refs)
    offsets = [refs.pop(0) for _ in range(sides)]
    own = [refs.pop(0) for _ in range(count)]
    twin = [refs.pop(0) for _ in range(count)]
    factors = [refs.pop(0) for _ in range(sides)]
    earlier = [refs.pop(0) for _ in range(before)]
    outs = [refs.pop(0) for _ in range(sides)]
    (lhs,) = refs
    groups = lax.axis_size("freq")
    me = lax.axis_index("freq")
    core = lax.rem(lax.axis_index("rows"), 2)
    _, freqs, slots, tile = factors[0].shape
    per_block = own[0].shape[1] // tile
    columns = groups * per_block
    half = 2 * SUBLANES
    deep = 2 * half
    for k in range(freqs):
        for arrays, at in ((own, core), (twin, 1 - core)):
            for b in range(count):
                for inner in range(per_block):
                    start = (b * per_block + inner) * deep + at * half
                    lhs[k, pl.ds(pl.multiple_of(start, half), half), :] = arrays[b][
                        k * half : (k + 1) * half, inner * tile : (inner + 1) * tile
                    ]
    for side in range(sides):
        for k in range(freqs):
            for low in range(0, slots, tile):
                slot = lax.broadcasted_iota(jnp.int32, (deep, tile), 1) + low
                chosen = []
                for part in range(2):
                    products = lax.dot_general(
                        lhs[k],
                        factors[side][part, k, low : low + tile, :],
                        NT,
                        preferred_element_type=jnp.float32,
                    )
                    total = jnp.zeros((deep, tile), jnp.float32)
                    for b, shift in enumerate(shifts):
                        column = (me ^ shift) * per_block
                        value = total
                        for inner in range(per_block):
                            at = (b * per_block + inner) * deep
                            value = jnp.where(
                                slot >= offsets[side][k, 0, column + inner],
                                products[at : at + deep],
                                value,
                            )
                        after = jnp.minimum(column + per_block, columns - 1)
                        end = jnp.where(
                            column + per_block < columns, offsets[side][k, 0, after], slots
                        )
                        total = jnp.where(slot >= end, total, value)
                    chosen.append(total)
                by_real, by_imag = chosen
                n = SUBLANES
                real = [by_real[g : g + n] - by_imag[g + n : g + 2 * n] for g in (0, half)]
                imag = [by_real[g + n : g + 2 * n] + by_imag[g : g + n] for g in (0, half)]
                for c, pieces in enumerate((real, imag)):
                    value = jnp.concatenate(pieces, 0)
                    if side < before:
                        value += earlier[side][k, c, :, low : low + tile].astype(jnp.float32)
                    outs[side][k, c, :, low : low + tile] = value.astype(jnp.bfloat16)


def coefficients(shifts, offsets, own, twin, factors, earlier=()):
    sides, count = len(offsets), len(shifts)
    _, freqs, slots, tile = factors[0].shape
    columns = count * own[0].shape[1] // tile
    shape = jax.ShapeDtypeStruct((freqs, 2, 2 * SUBLANES, slots), jnp.bfloat16)
    return pl.pallas_call(
        functools.partial(coefficient_kernel, tuple(shifts), sides, len(earlier)),
        in_specs=[SMEM] * sides + [VMEM] * (2 * count + sides + len(earlier)),
        out_specs=[VMEM] * sides,
        out_shape=[shape] * sides,
        scratch_shapes=[pltpu.VMEM((freqs, columns * 4 * SUBLANES, tile), jnp.bfloat16)],
        compiler_params=pltpu.CompilerParams(vmem_limit_bytes=16 * 2**20),
        cost_estimate=pl.CostEstimate(
            flops=2 * 2 * sides * freqs * slots * columns * 4 * SUBLANES * tile,
            bytes_accessed=2**20,
            transcendentals=0,
        ),
        name="coefficients",
    )(*offsets, *own, *twin, *factors, *earlier)


def band_kernel(add, at_near, offsets_ref, ranks_ref, coeffs_ref, u_ref, *refs):
    refs = list(refs)
    other_ref = refs.pop(0) if add else None
    out_ref, rhs, crossed = refs[:3]
    freqs, _, sources, slots = coeffs_ref.shape
    tile = u_ref.shape[2]
    place = lax.rem(lax.axis_index("rows") // 2, 2)
    at = place if at_near else 1 - place
    last = offsets_ref.shape[2] - 1
    wide = 2 * sources
    rhs[...] = jnp.zeros_like(rhs)
    crossed[...] = jnp.zeros_like(crossed)
    slot = lax.broadcasted_iota(jnp.int32, (sources, slots), 1)
    for k in range(freqs):
        live = slot < offsets_ref[k, 0, last] + ranks_ref[k, 0, last]
        for part in range(2):
            value = jnp.where(live, coeffs_ref[k, part].astype(jnp.float32), 0.0)
            start = pl.multiple_of((2 * k + part) * wide + at * sources, sources)
            rhs[k, pl.ds(start, sources), :] = value.astype(jnp.bfloat16)
            start = pl.multiple_of((2 * k + 1 - part) * wide + at * sources, sources)
            value = value if part == 0 else -value
            crossed[k, pl.ds(start, sources), :] = value.astype(jnp.bfloat16)
    total = other_ref[...] if add else jnp.zeros((tile, 2 * freqs * wide), jnp.float32)
    for k in range(freqs):
        for part, ref in enumerate((rhs, crossed)):
            total += lax.dot_general(u_ref[part, k], ref[k], NT, preferred_element_type=jnp.float32)
    if not add:
        out_ref[...] = total
        return
    bands, mix = refs[3:]
    groups = out_ref.shape[0]
    bands[...] = total
    packs = LANES // wide
    kinds = 2 * freqs
    block = lax.broadcasted_iota(jnp.int32, (tile // packs, LANES), 1) // wide
    loaded = [bands[pl.ds(b, tile // packs, stride=packs), :] for b in range(packs)]
    rows = tile // packs // groups
    for kind in range(kinds):
        mixed = jnp.zeros((tile // packs, LANES), jnp.float32)
        for b in range(packs):
            shift = (b - kind) * wide % LANES
            moved = pltpu.roll(loaded[b], shift, 1) if shift else loaded[b]
            mixed = jnp.where(block == b, moved, mixed)
        mix[:, kind * rows : (kind + 1) * rows, :] = mixed.reshape(groups, rows, LANES)
    out_ref[...] = mix[...].astype(jnp.bfloat16)


def bands_of(at_near, offsets, ranks, coeffs, u_own, groups, other=None):
    add = other is not None
    freqs, _, sources, slots = coeffs.shape
    tile = u_own.shape[2]
    rows = 2 * freqs * tile * 2 * sources // LANES // groups
    partial = jax.ShapeDtypeStruct((tile, LANES), jnp.float32)
    whole = jax.ShapeDtypeStruct((groups, rows, LANES), jnp.bfloat16)
    spread = pltpu.VMEM((freqs, LANES, slots), jnp.bfloat16)
    mixing = [pltpu.VMEM((tile, LANES), jnp.float32), pltpu.VMEM(whole.shape, jnp.float32)]
    return pl.pallas_call(
        functools.partial(band_kernel, add, at_near),
        in_specs=[SMEM] * 2 + [VMEM] * (3 if add else 2),
        out_specs=VMEM,
        out_shape=whole if add else partial,
        scratch_shapes=[spread, spread] + (mixing if add else []),
        compiler_params=pltpu.CompilerParams(vmem_limit_bytes=8 * 2**20),
        cost_estimate=pl.CostEstimate(
            flops=2 * 2 * freqs * tile * LANES * slots, bytes_accessed=2**20, transcendentals=0
        ),
        name="bands",
    )(offsets, ranks, coeffs, u_own, *([other] if add else []))


def series_kernel(scale, bands_ref, table_ref, out_ref, wide, done, sems):
    groups, rows, lanes = bands_ref.shape
    kinds = table_ref.shape[0]
    steps = groups * rows // kinds
    wide[...] = bands_ref[...].astype(jnp.float32).reshape(groups * rows, lanes) * scale
    copies = []
    for i in range(steps):
        part = wide[pl.ds(i, kinds, stride=steps), :]
        done[i] = jnp.dot(
            part.T.astype(jnp.bfloat16), table_ref[...], preferred_element_type=jnp.float32
        ).astype(jnp.bfloat16)
        copies.append(
            pltpu.make_async_copy(
                done.at[i], out_ref.at[i * lanes : (i + 1) * lanes, :], sems.at[i]
            )
        )
        copies[-1].start()
    for copy in copies:
        copy.wait()


def series_of(bands, table, scale):
    groups, rows, lanes = bands.shape
    kinds, samples = table.shape
    steps = groups * rows // kinds
    return pl.pallas_call(
        functools.partial(series_kernel, scale),
        in_specs=[VMEM] * 2,
        out_specs=pl.BlockSpec(memory_space=pl.ANY),
        out_shape=jax.ShapeDtypeStruct((steps * lanes, samples), jnp.bfloat16),
        scratch_shapes=[
            pltpu.VMEM((groups * rows, lanes), jnp.float32),
            pltpu.VMEM((steps, lanes, samples), jnp.bfloat16),
            pltpu.SemaphoreType.DMA((steps,)),
        ],
        compiler_params=pltpu.CompilerParams(vmem_limit_bytes=16 * 2**20),
        cost_estimate=pl.CostEstimate(
            flops=2 * steps * lanes * kinds * samples,
            bytes_accessed=steps * lanes * samples * 2,
            transcendentals=0,
        ),
        name="series",
    )(bands, table)


def fits(rec_dev, src_dev, samples, freq_dev, rows_dev, tile, slots, freq_group, row_group):
    kinds = 2 * freq_dev * freq_group
    ratio = math.sqrt(samples) / math.sqrt(freq_dev * freq_group)
    return (
        math.frexp(ratio)[0] == 0.5
        and math.sqrt(samples).is_integer()
        and src_dev == SUBLANES
        and row_group == 4
        and rows_dev == 1
        and freq_group in PAIRED
        and rec_dev % tile == 0
        and tile % (2 * LANES) == 0
        and slots % tile == 0
        and LANES % kinds == 0
        and SUBLANES % (LANES // kinds) == 0
        and 2 * freq_dev * src_dev * row_group == LANES
        and tile % (4 * SUBLANES * freq_group) == 0
    )


def shift_order(groups):
    return [(groups // 2 - 1 - 2 * i) % (groups - 1) + 1 for i in range(groups - 1)]


def arrivals(groups):
    order = shift_order(groups)
    crossing = [s for s in order if s >= groups // 2]
    middle = [s for s in order[:-1] if s == 1 or s in crossing[2:]]
    early = [s for s in order[:-1] if s not in middle]
    return [0] + early, middle, order[-1:]


def per_device_fast(wavefield, u_factors, v_factors, tile_ranks, tile_offsets):
    rec_dev, src_dev, samples = wavefield.shape
    freq_dev = u_factors.shape[1]
    groups = lax.axis_size("freq")
    row_group = lax.axis_size("rows")
    freqs = freq_dev * groups
    sources = src_dev * row_group
    tile = u_factors.shape[3]
    across = [(i, i ^ 2) for i in range(row_group)]
    beside = [(i, i ^ 1) for i in range(row_group)]
    forward, _ = spectral_tables(freqs, samples)
    u_own, v_own = u_factors[:, :, 0], v_factors[:, :, 0]
    v_far = lax.ppermute(v_own, "rows", across)
    offsets_far = lax.ppermute(tile_offsets, "rows", across)
    table = forward.reshape(2 * freqs, samples)
    sent = transform(wavefield.reshape(rec_dev * src_dev, samples), table, groups)
    own = {0: sent[0]}
    for shift in shift_order(groups):
        swap = [(i, i ^ shift) for i in range(groups)]
        own[shift] = lax.ppermute(sent[shift], "freq", swap)
    early, middle, last = arrivals(groups)

    def twins(shifts):
        pairs = {}
        for shift in shifts:
            pairs[shift] = lax.ppermute(own[shift], "rows", beside)
        return pairs

    def blocks(shifts):
        return [own[s] for s in shifts], [twin[s] for s in shifts]

    twin = twins(early)
    (near,) = coefficients(early, [tile_offsets], *blocks(early), [v_own])
    waiting, near = lax.optimization_barrier(([own[s] for s in middle], near))
    own.update(zip(middle, waiting))
    twin.update(twins(middle))
    (leaving,) = coefficients(early, [offsets_far], *blocks(early), [v_far])
    waiting, near, leaving = lax.optimization_barrier(([own[s] for s in last], near, leaving))
    own.update(zip(last, waiting))
    twin.update(twins(last))
    late = middle + last
    (leaving,) = coefficients(late, [offsets_far], *blocks(late), [v_far], [leaving])
    far = lax.ppermute(leaving, "rows", across)
    (near,) = coefficients(late, [tile_offsets], *blocks(late), [v_own], [near])
    half = bands_of(True, tile_offsets, tile_ranks, near, u_own, groups)
    bands = bands_of(False, tile_offsets, tile_ranks, far, u_own, groups, half)
    returned = lax.all_to_all(bands, "freq", split_axis=0, concat_axis=0, tiled=True)
    series = series_of(returned, table, math.sqrt(samples) / math.sqrt(freqs))
    return series.reshape(tile // groups, sources, samples)


def choose(wavefield, u_factors, v_factors, tile_ranks, tile_offsets):
    ok = fits(
        wavefield.shape[0],
        wavefield.shape[1],
        wavefield.shape[2],
        u_factors.shape[1],
        u_factors.shape[2],
        u_factors.shape[3],
        u_factors.shape[4],
        lax.axis_size("freq"),
        lax.axis_size("rows"),
    )
    step = per_device_fast if ok else per_device
    return step(wavefield, u_factors, v_factors, tile_ranks, tile_offsets)


def solution(mesh):
    placed = (
        P("freq", "rows", None),
        P(None, "freq", "rows", None, None),
        P(None, "freq", "rows", None, None),
        P("freq", "rows", None),
        P("freq", "rows", None),
    )
    return jax.shard_map(
        choose,
        mesh=mesh,
        in_specs=placed,
        out_specs=P(("rows", "freq"), None, None),
        check_vma=False,
    )
```

```python
import functools
import math

import jax
import jax.numpy as jnp
from jax import lax
from jax.experimental import pallas as pl
from jax.experimental.pallas import tpu as pltpu
from jax.sharding import PartitionSpec as P


RANK_MAX = 64
LANES = 128
SUBLANES = 8
NT = (((1,), (1,)), ((), ()))
VMEM = pl.BlockSpec(memory_space=pltpu.VMEM)
SMEM = pl.BlockSpec(memory_space=pltpu.SMEM)
PAIRED = (4, 8, 16)
AHEAD = 3


def spectral_tables(freq_count, sample_count):
    freq_bins = jnp.arange(freq_count, dtype=jnp.int32) + 1
    sample_index = jnp.arange(sample_count, dtype=jnp.int32)
    phase_int = freq_bins[:, None] * sample_index[None, :] % sample_count
    angles = phase_int.astype(jnp.float32) * (2.0 * math.pi / sample_count)
    cosine = jnp.cos(angles)
    minus_sine = -jnp.sin(angles)
    stacked = jnp.stack([cosine, minus_sine], axis=1)
    forward = (stacked / math.sqrt(sample_count)).astype(jnp.bfloat16)
    inverse = (stacked / math.sqrt(freq_count)).astype(jnp.bfloat16)
    return (forward, inverse)


def tile_windows(v_row, u_row, starts, rank_max):
    columns = starts.shape[0]
    slot_index = (starts[:, None] + jnp.arange(rank_max, dtype=jnp.int32)[None, :]).reshape(-1)
    v_padded = jnp.pad(v_row, ((0, 0), (0, rank_max), (0, 0)))
    u_padded = jnp.pad(u_row, ((0, 0), (0, 0), (0, rank_max)))
    v_win = jnp.take(v_padded, slot_index, axis=1).reshape(2, columns, rank_max, v_row.shape[2])
    u_win = jnp.take(u_padded, slot_index, axis=2).reshape(2, u_row.shape[1], columns, rank_max)
    return (v_win, u_win)


def slot_lookup(starts, counts, rank_max, slot_count):
    position = jnp.arange(slot_count, dtype=jnp.int32)
    started = starts[:, None, :] <= position[None, :, None]
    owner_tile = jnp.sum(started.astype(jnp.int32), axis=2) - 1
    first_slot = jnp.max(jnp.where(started, starts[:, None, :], 0), axis=2)
    within = position[None, :] - first_slot
    live_slot = position[None, :] < (starts[:, -1] + counts[:, -1])[:, None]
    flat_index = jnp.where(live_slot, owner_tile * rank_max + within, 0)
    return (flat_index, live_slot)


def take_slots(values, chosen):
    return jnp.take(values, chosen, axis=1)


def per_device(wavefield, u_factors, v_factors, tile_ranks, tile_offsets):
    rec_dev, src_dev, samples = wavefield.shape
    freq_dev = u_factors.shape[1]
    rows_dev = u_factors.shape[2]
    tile_size = u_factors.shape[3]
    slot_count = u_factors.shape[4]
    freq_group = lax.axis_size("freq")
    row_group = lax.axis_size("rows")
    freqs = freq_dev * freq_group
    receivers = rec_dev * freq_group
    columns = receivers // tile_size
    sources = src_dev * row_group
    forward, inverse = spectral_tables(freqs, samples)
    spectrum = jnp.einsum("kct,rst->kcrs", forward, wavefield, preferred_element_type=jnp.float32)
    spectrum = spectrum.astype(jnp.bfloat16).reshape(freqs, 2, rec_dev * src_dev)
    windows = jax.vmap(
        functools.partial(tile_windows, rank_max=RANK_MAX), in_axes=(1, 1, 0), out_axes=(1, 1)
    )
    rank_slots = jnp.arange(RANK_MAX, dtype=jnp.int32)
    tile_row = 0
    v_win, u_win = windows(
        v_factors[:, :, tile_row], u_factors[:, :, tile_row], tile_offsets[:, tile_row]
    )
    rank_mask = rank_slots[None, None, :] < tile_ranks[:, tile_row, :, None]
    flat_index, live_slot = slot_lookup(
        tile_offsets[:, tile_row], tile_ranks[:, tile_row], RANK_MAX, slot_count
    )
    prepared = [(v_win, u_win, rank_mask, flat_index, live_slot)]
    by_frequency = lax.all_to_all(spectrum, "freq", split_axis=0, concat_axis=2, tiled=True)
    portion = lax.all_gather(by_frequency[None], "rows", axis=0, tiled=True)
    blocks_in = portion.shape[0]
    spectra = portion.reshape(blocks_in, freq_dev, 2, columns, tile_size, src_dev)
    spectra = jnp.transpose(spectra, (1, 2, 3, 4, 0, 5)).reshape(
        freq_dev, 2, columns, tile_size, blocks_in * src_dev
    )
    tile_row = 0
    v_win, u_win, rank_mask, flat_index, live_slot = prepared[tile_row]
    quadrants = jnp.einsum(
        "afjmr,fbjrs->fabjms", v_win, spectra, preferred_element_type=jnp.float32
    )
    coeffs = jnp.stack(
        [quadrants[:, 0, 0] - quadrants[:, 1, 1], quadrants[:, 0, 1] + quadrants[:, 1, 0]], axis=1
    )
    coeffs = jnp.where(rank_mask[:, None, :, :, None], coeffs, 0.0).astype(jnp.bfloat16)
    stacked = coeffs.reshape(freq_dev, 2, columns * RANK_MAX, blocks_in * src_dev)
    packed = jax.vmap(take_slots)(stacked, flat_index)
    packed = jnp.where(live_slot[:, None, :, None], packed, jnp.zeros((), jnp.bfloat16))
    products = jnp.einsum(
        "afrk,fcks->facrs", u_factors[:, :, tile_row], packed, preferred_element_type=jnp.float32
    )
    results = [
        jnp.stack(
            [products[:, 0, 0] - products[:, 1, 1], products[:, 0, 1] + products[:, 1, 0]], axis=1
        )
    ]
    merged = jnp.stack(results, axis=2)
    bands = merged.astype(jnp.bfloat16).reshape(
        freq_dev, 2, rows_dev * tile_size, blocks_in, src_dev
    )
    bands = bands.reshape(freq_dev, 2, rows_dev * tile_size * sources)
    returned = lax.all_to_all(bands, "freq", split_axis=2, concat_axis=0, tiled=True)
    series = jnp.einsum("kcq,kct->qt", returned, inverse, preferred_element_type=jnp.float32)
    return series.astype(jnp.bfloat16).reshape(rows_dev * tile_size // freq_group, sources, samples)


def transform_kernel(traces_ref, table_ref, *refs):
    groups = lax.axis_size("freq")
    outs, (traces, sems, products, turned) = refs[:groups], refs[groups:]
    me = lax.axis_index("freq")
    rows = products.shape[1]
    kinds = turned.shape[0] // SUBLANES
    packs = LANES // kinds
    blocks = traces_ref.shape[0] // rows
    each = outs[0].shape[0]

    def copy(i):
        part = pl.ds(pl.multiple_of(i * rows, rows), rows)
        return pltpu.make_async_copy(traces_ref.at[part, :], traces.at[part, :], sems.at[i])

    def turn(i, source_rows):
        place = lax.broadcasted_iota(jnp.int32, (rows // SUBLANES, LANES), 1) // kinds
        for first in range(0, SUBLANES, packs):
            mixed = source_rows[pl.ds(first, rows // SUBLANES, stride=SUBLANES), :]
            for m in range(1, packs):
                part = source_rows[pl.ds(first + m, rows // SUBLANES, stride=SUBLANES), :]
                mixed = jnp.where(place == m, part, mixed)
            mixed = mixed.T
            for m in range(packs):
                turned[pl.ds(first + m, kinds, stride=SUBLANES), :] = mixed[
                    m * kinds : (m + 1) * kinds
                ]
        lanes = pl.ds(pl.multiple_of(i * LANES, LANES), LANES)
        for shift, out in enumerate(outs):
            group = me ^ shift
            start = pl.multiple_of(group * each, each)
            out[:, lanes] = turned[pl.ds(start, each), :].astype(jnp.bfloat16)

    for i in range(min(AHEAD, blocks)):
        copy(i).start()

    def step(i, carry):
        now = lax.rem(i, 2)

        @pl.when(i + AHEAD < blocks)
        def _():
            copy(i + AHEAD).start()

        copy(i).wait()
        part = pl.ds(pl.multiple_of(i * rows, rows), rows)
        turn(jnp.maximum(i - 1, 0), products.at[1 - now])
        products[now] = lax.dot_general(
            traces[part, :], table_ref[...], NT, preferred_element_type=jnp.float32
        )
        return carry

    lax.fori_loop(0, blocks, step, 0)
    turn(blocks - 1, products.at[(blocks - 1) % 2])


def transform(traces, table, groups):
    rows, samples = traces.shape
    receivers = rows // SUBLANES
    kinds = table.shape[0]
    repeated = jnp.tile(table, (LANES // kinds, 1))
    shape = jax.ShapeDtypeStruct((kinds * SUBLANES // groups, receivers), jnp.bfloat16)
    return pl.pallas_call(
        transform_kernel,
        in_specs=[pl.BlockSpec(memory_space=pltpu.HBM), VMEM],
        out_specs=[VMEM] * groups,
        out_shape=[shape] * groups,
        scratch_shapes=[
            pltpu.VMEM((rows, samples), jnp.bfloat16),
            pltpu.SemaphoreType.DMA((receivers // LANES,)),
            pltpu.VMEM((2, LANES * SUBLANES, LANES), jnp.float32),
            pltpu.VMEM((kinds * SUBLANES, LANES), jnp.float32),
        ],
        compiler_params=pltpu.CompilerParams(vmem_limit_bytes=48 * 2**20),
        cost_estimate=pl.CostEstimate(
            flops=2 * rows * samples * 256, bytes_accessed=rows * samples * 2, transcendentals=0
        ),
        name="transform",
    )(traces, repeated)


def coefficient_kernel(shifts, sides, before, *refs):
    count = len(shifts)
    refs = list(refs)
    offsets = [refs.pop(0) for _ in range(sides)]
    own = [refs.pop(0) for _ in range(count)]
    twin = [refs.pop(0) for _ in range(count)]
    factors = [refs.pop(0) for _ in range(sides)]
    earlier = [refs.pop(0) for _ in range(before)]
    outs = [refs.pop(0) for _ in range(sides)]
    (lhs,) = refs
    groups = lax.axis_size("freq")
    me = lax.axis_index("freq")
    core = lax.rem(lax.axis_index("rows"), 2)
    _, freqs, slots, tile = factors[0].shape
    per_block = own[0].shape[1] // tile
    columns = groups * per_block
    half = 2 * SUBLANES
    deep = 2 * half
    for k in range(freqs):
        for arrays, at in ((own, core), (twin, 1 - core)):
            for b in range(count):
                for inner in range(per_block):
                    start = (b * per_block + inner) * deep + at * half
                    lhs[k, pl.ds(pl.multiple_of(start, half), half), :] = arrays[b][
                        k * half : (k + 1) * half, inner * tile : (inner + 1) * tile
                    ]
    for side in range(sides):
        for k in range(freqs):
            for low in range(0, slots, tile):
                slot = lax.broadcasted_iota(jnp.int32, (deep, tile), 1) + low
                chosen = []
                for part in range(2):
                    products = lax.dot_general(
                        lhs[k],
                        factors[side][part, k, low : low + tile, :],
                        NT,
                        preferred_element_type=jnp.float32,
                    )
                    total = jnp.zeros((deep, tile), jnp.float32)
                    for b, shift in enumerate(shifts):
                        column = (me ^ shift) * per_block
                        value = total
                        for inner in range(per_block):
                            at = (b * per_block + inner) * deep
                            value = jnp.where(
                                slot >= offsets[side][k, 0, column + inner],
                                products[at : at + deep],
                                value,
                            )
                        after = jnp.minimum(column + per_block, columns - 1)
                        end = jnp.where(
                            column + per_block < columns, offsets[side][k, 0, after], slots
                        )
                        total = jnp.where(slot >= end, total, value)
                    chosen.append(total)
                by_real, by_imag = chosen
                n = SUBLANES
                real = [by_real[g : g + n] - by_imag[g + n : g + 2 * n] for g in (0, half)]
                imag = [by_real[g + n : g + 2 * n] + by_imag[g : g + n] for g in (0, half)]
                for c, pieces in enumerate((real, imag)):
                    value = jnp.concatenate(pieces, 0)
                    if side < before:
                        value += earlier[side][k, c, :, low : low + tile].astype(jnp.float32)
                    outs[side][k, c, :, low : low + tile] = value.astype(jnp.bfloat16)


def coefficients(shifts, offsets, own, twin, factors, earlier=()):
    sides, count = len(offsets), len(shifts)
    _, freqs, slots, tile = factors[0].shape
    columns = count * own[0].shape[1] // tile
    shape = jax.ShapeDtypeStruct((freqs, 2, 2 * SUBLANES, slots), jnp.bfloat16)
    return pl.pallas_call(
        functools.partial(coefficient_kernel, tuple(shifts), sides, len(earlier)),
        in_specs=[SMEM] * sides + [VMEM] * (2 * count + sides + len(earlier)),
        out_specs=[VMEM] * sides,
        out_shape=[shape] * sides,
        scratch_shapes=[pltpu.VMEM((freqs, columns * 4 * SUBLANES, tile), jnp.bfloat16)],
        compiler_params=pltpu.CompilerParams(vmem_limit_bytes=16 * 2**20),
        cost_estimate=pl.CostEstimate(
            flops=2 * 2 * sides * freqs * slots * columns * 4 * SUBLANES * tile,
            bytes_accessed=2**20,
            transcendentals=0,
        ),
        name="coefficients",
    )(*offsets, *own, *twin, *factors, *earlier)


def band_kernel(add, at_near, offsets_ref, ranks_ref, coeffs_ref, u_ref, *refs):
    refs = list(refs)
    other_ref = refs.pop(0) if add else None
    out_ref, rhs, crossed = refs[:3]
    freqs, _, sources, slots = coeffs_ref.shape
    tile = u_ref.shape[2]
    place = lax.rem(lax.axis_index("rows") // 2, 2)
    at = place if at_near else 1 - place
    last = offsets_ref.shape[2] - 1
    wide = 2 * sources
    rhs[...] = jnp.zeros_like(rhs)
    crossed[...] = jnp.zeros_like(crossed)
    slot = lax.broadcasted_iota(jnp.int32, (sources, slots), 1)
    for k in range(freqs):
        live = slot < offsets_ref[k, 0, last] + ranks_ref[k, 0, last]
        for part in range(2):
            value = jnp.where(live, coeffs_ref[k, part].astype(jnp.float32), 0.0)
            start = pl.multiple_of((2 * k + part) * wide + at * sources, sources)
            rhs[k, pl.ds(start, sources), :] = value.astype(jnp.bfloat16)
            start = pl.multiple_of((2 * k + 1 - part) * wide + at * sources, sources)
            value = value if part == 0 else -value
            crossed[k, pl.ds(start, sources), :] = value.astype(jnp.bfloat16)
    total = other_ref[...] if add else jnp.zeros((tile, 2 * freqs * wide), jnp.float32)
    for k in range(freqs):
        for part, ref in enumerate((rhs, crossed)):
            total += lax.dot_general(u_ref[part, k], ref[k], NT, preferred_element_type=jnp.float32)
    if not add:
        out_ref[...] = total
        return
    bands, mix = refs[3:]
    groups = out_ref.shape[0]
    bands[...] = total
    packs = LANES // wide
    kinds = 2 * freqs
    block = lax.broadcasted_iota(jnp.int32, (tile // packs, LANES), 1) // wide
    loaded = [bands[pl.ds(b, tile // packs, stride=packs), :] for b in range(packs)]
    rows = tile // packs // groups
    for kind in range(kinds):
        mixed = jnp.zeros((tile // packs, LANES), jnp.float32)
        for b in range(packs):
            shift = (b - kind) * wide % LANES
            moved = pltpu.roll(loaded[b], shift, 1) if shift else loaded[b]
            mixed = jnp.where(block == b, moved, mixed)
        mix[:, kind * rows : (kind + 1) * rows, :] = mixed.reshape(groups, rows, LANES)
    out_ref[...] = mix[...].astype(jnp.bfloat16)


def bands_of(at_near, offsets, ranks, coeffs, u_own, groups, other=None):
    add = other is not None
    freqs, _, sources, slots = coeffs.shape
    tile = u_own.shape[2]
    rows = 2 * freqs * tile * 2 * sources // LANES // groups
    partial = jax.ShapeDtypeStruct((tile, LANES), jnp.float32)
    whole = jax.ShapeDtypeStruct((groups, rows, LANES), jnp.bfloat16)
    spread = pltpu.VMEM((freqs, LANES, slots), jnp.bfloat16)
    mixing = [pltpu.VMEM((tile, LANES), jnp.float32), pltpu.VMEM(whole.shape, jnp.float32)]
    return pl.pallas_call(
        functools.partial(band_kernel, add, at_near),
        in_specs=[SMEM] * 2 + [VMEM] * (3 if add else 2),
        out_specs=VMEM,
        out_shape=whole if add else partial,
        scratch_shapes=[spread, spread] + (mixing if add else []),
        compiler_params=pltpu.CompilerParams(vmem_limit_bytes=8 * 2**20),
        cost_estimate=pl.CostEstimate(
            flops=2 * 2 * freqs * tile * LANES * slots, bytes_accessed=2**20, transcendentals=0
        ),
        name="bands",
    )(offsets, ranks, coeffs, u_own, *([other] if add else []))


def series_kernel(scale, bands_ref, table_ref, out_ref, wide, done, sems):
    groups, rows, lanes = bands_ref.shape
    kinds = table_ref.shape[0]
    steps = groups * rows // kinds
    wide[...] = bands_ref[...].astype(jnp.float32).reshape(groups * rows, lanes) * scale
    copies = []
    for i in range(steps):
        part = wide[pl.ds(i, kinds, stride=steps), :]
        done[i] = jnp.dot(
            part.T.astype(jnp.bfloat16), table_ref[...], preferred_element_type=jnp.float32
        ).astype(jnp.bfloat16)
        copies.append(
            pltpu.make_async_copy(
                done.at[i], out_ref.at[i * lanes : (i + 1) * lanes, :], sems.at[i]
            )
        )
        copies[-1].start()
    for copy in copies:
        copy.wait()


def series_of(bands, table, scale):
    groups, rows, lanes = bands.shape
    kinds, samples = table.shape
    steps = groups * rows // kinds
    return pl.pallas_call(
        functools.partial(series_kernel, scale),
        in_specs=[VMEM] * 2,
        out_specs=pl.BlockSpec(memory_space=pl.ANY),
        out_shape=jax.ShapeDtypeStruct((steps * lanes, samples), jnp.bfloat16),
        scratch_shapes=[
            pltpu.VMEM((groups * rows, lanes), jnp.float32),
            pltpu.VMEM((steps, lanes, samples), jnp.bfloat16),
            pltpu.SemaphoreType.DMA((steps,)),
        ],
        compiler_params=pltpu.CompilerParams(vmem_limit_bytes=16 * 2**20),
        cost_estimate=pl.CostEstimate(
            flops=2 * steps * lanes * kinds * samples,
            bytes_accessed=steps * lanes * samples * 2,
            transcendentals=0,
        ),
        name="series",
    )(bands, table)


def fits(rec_dev, src_dev, samples, freq_dev, rows_dev, tile, slots, freq_group, row_group):
    kinds = 2 * freq_dev * freq_group
    ratio = math.sqrt(samples) / math.sqrt(freq_dev * freq_group)
    return (
        math.frexp(ratio)[0] == 0.5
        and math.sqrt(samples).is_integer()
        and src_dev == SUBLANES
        and row_group == 4
        and rows_dev == 1
        and freq_group in PAIRED
        and rec_dev % tile == 0
        and tile % (2 * LANES) == 0
        and slots % tile == 0
        and LANES % kinds == 0
        and SUBLANES % (LANES // kinds) == 0
        and 2 * freq_dev * src_dev * row_group == LANES
        and tile % (4 * SUBLANES * freq_group) == 0
    )


def shift_order(groups):
    return [(groups // 2 - 1 - 2 * i) % (groups - 1) + 1 for i in range(groups - 1)]


def arrivals(groups):
    order = shift_order(groups)
    crossing = [s for s in order[1:] if s >= groups // 2]
    early = [s for s in order if s not in crossing and s != 1]
    return [0] + early, [1] + crossing[:-1], crossing[-1:]


def per_device_fast(wavefield, u_factors, v_factors, tile_ranks, tile_offsets):
    rec_dev, src_dev, samples = wavefield.shape
    freq_dev = u_factors.shape[1]
    groups = lax.axis_size("freq")
    row_group = lax.axis_size("rows")
    freqs = freq_dev * groups
    sources = src_dev * row_group
    tile = u_factors.shape[3]
    across = [(i, i ^ 2) for i in range(row_group)]
    beside = [(i, i ^ 1) for i in range(row_group)]
    forward, _ = spectral_tables(freqs, samples)
    u_own, v_own = u_factors[:, :, 0], v_factors[:, :, 0]
    v_far = lax.ppermute(v_own, "rows", across)
    offsets_far = lax.ppermute(tile_offsets, "rows", across)
    table = forward.reshape(2 * freqs, samples)
    sent = transform(wavefield.reshape(rec_dev * src_dev, samples), table, groups)
    own = {0: sent[0]}
    for shift in shift_order(groups):
        swap = [(i, i ^ shift) for i in range(groups)]
        own[shift] = lax.ppermute(sent[shift], "freq", swap)
    early, middle, last = arrivals(groups)

    def twins(shifts):
        pairs = {}
        for shift in shifts:
            pairs[shift] = lax.ppermute(own[shift], "rows", beside)
        return pairs

    def blocks(shifts):
        return [own[s] for s in shifts], [twin[s] for s in shifts]

    twin = twins(early)
    (near,) = coefficients(early, [tile_offsets], *blocks(early), [v_own])
    waiting, near = lax.optimization_barrier(([own[s] for s in middle], near))
    own.update(zip(middle, waiting))
    twin.update(twins(middle))
    (leaving,) = coefficients(early, [offsets_far], *blocks(early), [v_far])
    waiting, near, leaving = lax.optimization_barrier(([own[s] for s in last], near, leaving))
    own.update(zip(last, waiting))
    twin.update(twins(last))
    late = middle + last
    (leaving,) = coefficients(late, [offsets_far], *blocks(late), [v_far], [leaving])
    far = lax.ppermute(leaving, "rows", across)
    (near,) = coefficients(late, [tile_offsets], *blocks(late), [v_own], [near])
    half = bands_of(True, tile_offsets, tile_ranks, near, u_own, groups)
    bands = bands_of(False, tile_offsets, tile_ranks, far, u_own, groups, half)
    returned = lax.all_to_all(bands, "freq", split_axis=0, concat_axis=0, tiled=True)
    series = series_of(returned, table, math.sqrt(samples) / math.sqrt(freqs))
    return series.reshape(tile // groups, sources, samples)


def choose(wavefield, u_factors, v_factors, tile_ranks, tile_offsets):
    ok = fits(
        wavefield.shape[0],
        wavefield.shape[1],
        wavefield.shape[2],
        u_factors.shape[1],
        u_factors.shape[2],
        u_factors.shape[3],
        u_factors.shape[4],
        lax.axis_size("freq"),
        lax.axis_size("rows"),
    )
    step = per_device_fast if ok else per_device
    return step(wavefield, u_factors, v_factors, tile_ranks, tile_offsets)


def solution(mesh):
    placed = (
        P("freq", "rows", None),
        P(None, "freq", "rows", None, None),
        P(None, "freq", "rows", None, None),
        P("freq", "rows", None),
        P("freq", "rows", None),
    )
    return jax.shard_map(
        choose,
        mesh=mesh,
        in_specs=placed,
        out_specs=P(("rows", "freq"), None, None),
        check_vma=False,
    )
```

```python
import functools
import math

import jax
import jax.numpy as jnp
from jax import lax
from jax.experimental import pallas as pl
from jax.experimental.pallas import tpu as pltpu
from jax.sharding import PartitionSpec as P


RANK_MAX = 64
LANES = 128
SUBLANES = 8
NT = (((1,), (1,)), ((), ()))
VMEM = pl.BlockSpec(memory_space=pltpu.VMEM)
SMEM = pl.BlockSpec(memory_space=pltpu.SMEM)
PAIRED = (4, 8, 16)
AHEAD = 3


def spectral_tables(freq_count, sample_count):
    freq_bins = jnp.arange(freq_count, dtype=jnp.int32) + 1
    sample_index = jnp.arange(sample_count, dtype=jnp.int32)
    phase_int = freq_bins[:, None] * sample_index[None, :] % sample_count
    angles = phase_int.astype(jnp.float32) * (2.0 * math.pi / sample_count)
    cosine = jnp.cos(angles)
    minus_sine = -jnp.sin(angles)
    stacked = jnp.stack([cosine, minus_sine], axis=1)
    forward = (stacked / math.sqrt(sample_count)).astype(jnp.bfloat16)
    inverse = (stacked / math.sqrt(freq_count)).astype(jnp.bfloat16)
    return (forward, inverse)


def tile_windows(v_row, u_row, starts, rank_max):
    columns = starts.shape[0]
    slot_index = (starts[:, None] + jnp.arange(rank_max, dtype=jnp.int32)[None, :]).reshape(-1)
    v_padded = jnp.pad(v_row, ((0, 0), (0, rank_max), (0, 0)))
    u_padded = jnp.pad(u_row, ((0, 0), (0, 0), (0, rank_max)))
    v_win = jnp.take(v_padded, slot_index, axis=1).reshape(2, columns, rank_max, v_row.shape[2])
    u_win = jnp.take(u_padded, slot_index, axis=2).reshape(2, u_row.shape[1], columns, rank_max)
    return (v_win, u_win)


def slot_lookup(starts, counts, rank_max, slot_count):
    position = jnp.arange(slot_count, dtype=jnp.int32)
    started = starts[:, None, :] <= position[None, :, None]
    owner_tile = jnp.sum(started.astype(jnp.int32), axis=2) - 1
    first_slot = jnp.max(jnp.where(started, starts[:, None, :], 0), axis=2)
    within = position[None, :] - first_slot
    live_slot = position[None, :] < (starts[:, -1] + counts[:, -1])[:, None]
    flat_index = jnp.where(live_slot, owner_tile * rank_max + within, 0)
    return (flat_index, live_slot)


def take_slots(values, chosen):
    return jnp.take(values, chosen, axis=1)


def per_device(wavefield, u_factors, v_factors, tile_ranks, tile_offsets):
    rec_dev, src_dev, samples = wavefield.shape
    freq_dev = u_factors.shape[1]
    rows_dev = u_factors.shape[2]
    tile_size = u_factors.shape[3]
    slot_count = u_factors.shape[4]
    freq_group = lax.axis_size("freq")
    row_group = lax.axis_size("rows")
    freqs = freq_dev * freq_group
    receivers = rec_dev * freq_group
    columns = receivers // tile_size
    sources = src_dev * row_group
    forward, inverse = spectral_tables(freqs, samples)
    spectrum = jnp.einsum("kct,rst->kcrs", forward, wavefield, preferred_element_type=jnp.float32)
    spectrum = spectrum.astype(jnp.bfloat16).reshape(freqs, 2, rec_dev * src_dev)
    windows = jax.vmap(
        functools.partial(tile_windows, rank_max=RANK_MAX), in_axes=(1, 1, 0), out_axes=(1, 1)
    )
    rank_slots = jnp.arange(RANK_MAX, dtype=jnp.int32)
    tile_row = 0
    v_win, u_win = windows(
        v_factors[:, :, tile_row], u_factors[:, :, tile_row], tile_offsets[:, tile_row]
    )
    rank_mask = rank_slots[None, None, :] < tile_ranks[:, tile_row, :, None]
    flat_index, live_slot = slot_lookup(
        tile_offsets[:, tile_row], tile_ranks[:, tile_row], RANK_MAX, slot_count
    )
    prepared = [(v_win, u_win, rank_mask, flat_index, live_slot)]
    by_frequency = lax.all_to_all(spectrum, "freq", split_axis=0, concat_axis=2, tiled=True)
    portion = lax.all_gather(by_frequency[None], "rows", axis=0, tiled=True)
    blocks_in = portion.shape[0]
    spectra = portion.reshape(blocks_in, freq_dev, 2, columns, tile_size, src_dev)
    spectra = jnp.transpose(spectra, (1, 2, 3, 4, 0, 5)).reshape(
        freq_dev, 2, columns, tile_size, blocks_in * src_dev
    )
    tile_row = 0
    v_win, u_win, rank_mask, flat_index, live_slot = prepared[tile_row]
    quadrants = jnp.einsum(
        "afjmr,fbjrs->fabjms", v_win, spectra, preferred_element_type=jnp.float32
    )
    coeffs = jnp.stack(
        [quadrants[:, 0, 0] - quadrants[:, 1, 1], quadrants[:, 0, 1] + quadrants[:, 1, 0]], axis=1
    )
    coeffs = jnp.where(rank_mask[:, None, :, :, None], coeffs, 0.0).astype(jnp.bfloat16)
    stacked = coeffs.reshape(freq_dev, 2, columns * RANK_MAX, blocks_in * src_dev)
    packed = jax.vmap(take_slots)(stacked, flat_index)
    packed = jnp.where(live_slot[:, None, :, None], packed, jnp.zeros((), jnp.bfloat16))
    products = jnp.einsum(
        "afrk,fcks->facrs", u_factors[:, :, tile_row], packed, preferred_element_type=jnp.float32
    )
    results = [
        jnp.stack(
            [products[:, 0, 0] - products[:, 1, 1], products[:, 0, 1] + products[:, 1, 0]], axis=1
        )
    ]
    merged = jnp.stack(results, axis=2)
    bands = merged.astype(jnp.bfloat16).reshape(
        freq_dev, 2, rows_dev * tile_size, blocks_in, src_dev
    )
    bands = bands.reshape(freq_dev, 2, rows_dev * tile_size * sources)
    returned = lax.all_to_all(bands, "freq", split_axis=2, concat_axis=0, tiled=True)
    series = jnp.einsum("kcq,kct->qt", returned, inverse, preferred_element_type=jnp.float32)
    return series.astype(jnp.bfloat16).reshape(rows_dev * tile_size // freq_group, sources, samples)


def cosines(kinds, samples):
    row = lax.broadcasted_iota(jnp.int32, (kinds, samples), 0)
    index = lax.broadcasted_iota(jnp.int32, (kinds, samples), 1)
    phase = (((row >> 1) + 1) * index + (row & 1) * (samples // 4)) & (samples - 1)
    angles = phase.astype(jnp.float32) * (2.0 * math.pi / samples)
    return (jnp.cos(angles) * (1.0 / math.sqrt(samples))).astype(jnp.bfloat16)


def transform_kernel(traces_ref, *refs):
    groups = lax.axis_size("freq")
    outs, (table_ref, traces, sems, repeated, products, turned) = refs[:groups], refs[groups:]
    me = lax.axis_index("freq")
    rows = products.shape[1]
    kinds = turned.shape[0] // SUBLANES
    packs = LANES // kinds
    blocks = traces_ref.shape[0] // rows
    each = outs[0].shape[0]

    def copy(i):
        part = pl.ds(pl.multiple_of(i * rows, rows), rows)
        return pltpu.make_async_copy(traces_ref.at[part, :], traces.at[part, :], sems.at[i])

    def turn(i, source_rows):
        place = lax.broadcasted_iota(jnp.int32, (rows // SUBLANES, LANES), 1) // kinds
        for first in range(0, SUBLANES, packs):
            mixed = source_rows[pl.ds(first, rows // SUBLANES, stride=SUBLANES), :]
            for m in range(1, packs):
                part = source_rows[pl.ds(first + m, rows // SUBLANES, stride=SUBLANES), :]
                mixed = jnp.where(place == m, part, mixed)
            mixed = mixed.T
            for m in range(packs):
                turned[pl.ds(first + m, kinds, stride=SUBLANES), :] = mixed[
                    m * kinds : (m + 1) * kinds
                ]
        lanes = pl.ds(pl.multiple_of(i * LANES, LANES), LANES)
        for shift, out in enumerate(outs):
            group = me ^ shift
            start = pl.multiple_of(group * each, each)
            out[:, lanes] = turned[pl.ds(start, each), :].astype(jnp.bfloat16)

    for i in range(min(AHEAD, blocks)):
        copy(i).start()
    table_ref[...] = cosines(kinds, traces.shape[1])
    for m in range(packs):
        repeated[m * kinds : (m + 1) * kinds, :] = table_ref[...]

    def step(i, carry):
        now = lax.rem(i, 2)

        @pl.when(i + AHEAD < blocks)
        def _():
            copy(i + AHEAD).start()

        copy(i).wait()
        part = pl.ds(pl.multiple_of(i * rows, rows), rows)
        turn(jnp.maximum(i - 1, 0), products.at[1 - now])
        products[now] = lax.dot_general(
            traces[part, :], repeated[...], NT, preferred_element_type=jnp.float32
        )
        return carry

    lax.fori_loop(0, blocks, step, 0)
    turn(blocks - 1, products.at[(blocks - 1) % 2])


def transform(traces, kinds, groups):
    rows, samples = traces.shape
    receivers = rows // SUBLANES
    shape = jax.ShapeDtypeStruct((kinds * SUBLANES // groups, receivers), jnp.bfloat16)
    return pl.pallas_call(
        transform_kernel,
        in_specs=[pl.BlockSpec(memory_space=pltpu.HBM)],
        out_specs=[VMEM] * (groups + 1),
        out_shape=[shape] * groups + [jax.ShapeDtypeStruct((kinds, samples), jnp.bfloat16)],
        scratch_shapes=[
            pltpu.VMEM((rows, samples), jnp.bfloat16),
            pltpu.SemaphoreType.DMA((receivers // LANES,)),
            pltpu.VMEM((LANES, samples), jnp.bfloat16),
            pltpu.VMEM((2, LANES * SUBLANES, LANES), jnp.float32),
            pltpu.VMEM((kinds * SUBLANES, LANES), jnp.float32),
        ],
        compiler_params=pltpu.CompilerParams(vmem_limit_bytes=48 * 2**20),
        cost_estimate=pl.CostEstimate(
            flops=2 * rows * samples * 256, bytes_accessed=rows * samples * 2, transcendentals=0
        ),
        name="transform",
    )(traces)


def coefficient_kernel(shifts, sides, before, *refs):
    count = len(shifts)
    refs = list(refs)
    offsets = [refs.pop(0) for _ in range(sides)]
    own = [refs.pop(0) for _ in range(count)]
    twin = [refs.pop(0) for _ in range(count)]
    factors = [refs.pop(0) for _ in range(sides)]
    earlier = [refs.pop(0) for _ in range(before)]
    outs = [refs.pop(0) for _ in range(sides)]
    (lhs,) = refs
    groups = lax.axis_size("freq")
    me = lax.axis_index("freq")
    core = lax.rem(lax.axis_index("rows"), 2)
    _, freqs, slots, tile = factors[0].shape
    per_block = own[0].shape[1] // tile
    columns = groups * per_block
    half = 2 * SUBLANES
    deep = 2 * half
    for k in range(freqs):
        for arrays, at in ((own, core), (twin, 1 - core)):
            for b in range(count):
                for inner in range(per_block):
                    start = (b * per_block + inner) * deep + at * half
                    lhs[k, pl.ds(pl.multiple_of(start, half), half), :] = arrays[b][
                        k * half : (k + 1) * half, inner * tile : (inner + 1) * tile
                    ]
    for side in range(sides):
        for k in range(freqs):
            for low in range(0, slots, tile):
                slot = lax.broadcasted_iota(jnp.int32, (deep, tile), 1) + low
                chosen = []
                for part in range(2):
                    products = lax.dot_general(
                        lhs[k],
                        factors[side][part, k, low : low + tile, :],
                        NT,
                        preferred_element_type=jnp.float32,
                    )
                    total = jnp.zeros((deep, tile), jnp.float32)
                    for b, shift in enumerate(shifts):
                        column = (me ^ shift) * per_block
                        value = total
                        for inner in range(per_block):
                            at = (b * per_block + inner) * deep
                            value = jnp.where(
                                slot >= offsets[side][k, 0, column + inner],
                                products[at : at + deep],
                                value,
                            )
                        after = jnp.minimum(column + per_block, columns - 1)
                        end = jnp.where(
                            column + per_block < columns, offsets[side][k, 0, after], slots
                        )
                        total = jnp.where(slot >= end, total, value)
                    chosen.append(total)
                by_real, by_imag = chosen
                n = SUBLANES
                real = [by_real[g : g + n] - by_imag[g + n : g + 2 * n] for g in (0, half)]
                imag = [by_real[g + n : g + 2 * n] + by_imag[g : g + n] for g in (0, half)]
                for c, pieces in enumerate((real, imag)):
                    value = jnp.concatenate(pieces, 0)
                    if side < before:
                        value += earlier[side][k, c, :, low : low + tile].astype(jnp.float32)
                    outs[side][k, c, :, low : low + tile] = value.astype(jnp.bfloat16)


def coefficients(shifts, offsets, own, twin, factors, earlier=()):
    sides, count = len(offsets), len(shifts)
    _, freqs, slots, tile = factors[0].shape
    columns = count * own[0].shape[1] // tile
    shape = jax.ShapeDtypeStruct((freqs, 2, 2 * SUBLANES, slots), jnp.bfloat16)
    return pl.pallas_call(
        functools.partial(coefficient_kernel, tuple(shifts), sides, len(earlier)),
        in_specs=[SMEM] * sides + [VMEM] * (2 * count + sides + len(earlier)),
        out_specs=[VMEM] * sides,
        out_shape=[shape] * sides,
        scratch_shapes=[pltpu.VMEM((freqs, columns * 4 * SUBLANES, tile), jnp.bfloat16)],
        compiler_params=pltpu.CompilerParams(vmem_limit_bytes=16 * 2**20),
        cost_estimate=pl.CostEstimate(
            flops=2 * 2 * sides * freqs * slots * columns * 4 * SUBLANES * tile,
            bytes_accessed=2**20,
            transcendentals=0,
        ),
        name="coefficients",
    )(*offsets, *own, *twin, *factors, *earlier)


def band_kernel(add, at_near, offsets_ref, ranks_ref, coeffs_ref, u_ref, *refs):
    refs = list(refs)
    other_ref = refs.pop(0) if add else None
    out_ref, rhs, crossed = refs[:3]
    freqs, _, sources, slots = coeffs_ref.shape
    tile = u_ref.shape[2]
    place = lax.rem(lax.axis_index("rows") // 2, 2)
    at = place if at_near else 1 - place
    last = offsets_ref.shape[2] - 1
    wide = 2 * sources
    rhs[...] = jnp.zeros_like(rhs)
    crossed[...] = jnp.zeros_like(crossed)
    slot = lax.broadcasted_iota(jnp.int32, (sources, slots), 1)
    for k in range(freqs):
        live = slot < offsets_ref[k, 0, last] + ranks_ref[k, 0, last]
        for part in range(2):
            value = jnp.where(live, coeffs_ref[k, part].astype(jnp.float32), 0.0)
            start = pl.multiple_of((2 * k + part) * wide + at * sources, sources)
            rhs[k, pl.ds(start, sources), :] = value.astype(jnp.bfloat16)
            start = pl.multiple_of((2 * k + 1 - part) * wide + at * sources, sources)
            value = value if part == 0 else -value
            crossed[k, pl.ds(start, sources), :] = value.astype(jnp.bfloat16)
    total = other_ref[...] if add else jnp.zeros((tile, 2 * freqs * wide), jnp.float32)
    for k in range(freqs):
        for part, ref in enumerate((rhs, crossed)):
            total += lax.dot_general(u_ref[part, k], ref[k], NT, preferred_element_type=jnp.float32)
    if not add:
        out_ref[...] = total
        return
    bands, mix = refs[3:]
    groups = out_ref.shape[0]
    bands[...] = total
    packs = LANES // wide
    kinds = 2 * freqs
    block = lax.broadcasted_iota(jnp.int32, (tile // packs, LANES), 1) // wide
    loaded = [bands[pl.ds(b, tile // packs, stride=packs), :] for b in range(packs)]
    rows = tile // packs // groups
    for kind in range(kinds):
        mixed = jnp.zeros((tile // packs, LANES), jnp.float32)
        for b in range(packs):
            shift = (b - kind) * wide % LANES
            moved = pltpu.roll(loaded[b], shift, 1) if shift else loaded[b]
            mixed = jnp.where(block == b, moved, mixed)
        mix[:, kind * rows : (kind + 1) * rows, :] = mixed.reshape(groups, rows, LANES)
    out_ref[...] = mix[...].astype(jnp.bfloat16)


def bands_of(at_near, offsets, ranks, coeffs, u_own, groups, other=None):
    add = other is not None
    freqs, _, sources, slots = coeffs.shape
    tile = u_own.shape[2]
    rows = 2 * freqs * tile * 2 * sources // LANES // groups
    partial = jax.ShapeDtypeStruct((tile, LANES), jnp.float32)
    whole = jax.ShapeDtypeStruct((groups, rows, LANES), jnp.bfloat16)
    spread = pltpu.VMEM((freqs, LANES, slots), jnp.bfloat16)
    mixing = [pltpu.VMEM((tile, LANES), jnp.float32), pltpu.VMEM(whole.shape, jnp.float32)]
    return pl.pallas_call(
        functools.partial(band_kernel, add, at_near),
        in_specs=[SMEM] * 2 + [VMEM] * (3 if add else 2),
        out_specs=VMEM,
        out_shape=whole if add else partial,
        scratch_shapes=[spread, spread] + (mixing if add else []),
        compiler_params=pltpu.CompilerParams(vmem_limit_bytes=8 * 2**20),
        cost_estimate=pl.CostEstimate(
            flops=2 * 2 * freqs * tile * LANES * slots, bytes_accessed=2**20, transcendentals=0
        ),
        name="bands",
    )(offsets, ranks, coeffs, u_own, *([other] if add else []))


def series_kernel(scale, bands_ref, table_ref, out_ref, wide, done, sems):
    groups, rows, lanes = bands_ref.shape
    kinds = table_ref.shape[0]
    steps = groups * rows // kinds
    wide[...] = bands_ref[...].astype(jnp.float32).reshape(groups * rows, lanes) * scale
    copies = []
    for i in range(steps):
        part = wide[pl.ds(i, kinds, stride=steps), :]
        done[i] = jnp.dot(
            part.T.astype(jnp.bfloat16), table_ref[...], preferred_element_type=jnp.float32
        ).astype(jnp.bfloat16)
        copies.append(
            pltpu.make_async_copy(
                done.at[i], out_ref.at[i * lanes : (i + 1) * lanes, :], sems.at[i]
            )
        )
        copies[-1].start()
    for copy in copies:
        copy.wait()


def series_of(bands, table, scale):
    groups, rows, lanes = bands.shape
    kinds, samples = table.shape
    steps = groups * rows // kinds
    return pl.pallas_call(
        functools.partial(series_kernel, scale),
        in_specs=[VMEM] * 2,
        out_specs=pl.BlockSpec(memory_space=pl.ANY),
        out_shape=jax.ShapeDtypeStruct((steps * lanes, samples), jnp.bfloat16),
        scratch_shapes=[
            pltpu.VMEM((groups * rows, lanes), jnp.float32),
            pltpu.VMEM((steps, lanes, samples), jnp.bfloat16),
            pltpu.SemaphoreType.DMA((steps,)),
        ],
        compiler_params=pltpu.CompilerParams(vmem_limit_bytes=16 * 2**20),
        cost_estimate=pl.CostEstimate(
            flops=2 * steps * lanes * kinds * samples,
            bytes_accessed=steps * lanes * samples * 2,
            transcendentals=0,
        ),
        name="series",
    )(bands, table)


def fits(rec_dev, src_dev, samples, freq_dev, rows_dev, tile, slots, freq_group, row_group):
    kinds = 2 * freq_dev * freq_group
    ratio = math.sqrt(samples) / math.sqrt(freq_dev * freq_group)
    return (
        math.frexp(ratio)[0] == 0.5
        and math.sqrt(samples).is_integer()
        and samples & (samples - 1) == 0
        and src_dev == SUBLANES
        and row_group == 4
        and rows_dev == 1
        and freq_group in PAIRED
        and rec_dev % tile == 0
        and tile % (2 * LANES) == 0
        and slots % tile == 0
        and LANES % kinds == 0
        and SUBLANES % (LANES // kinds) == 0
        and 2 * freq_dev * src_dev * row_group == LANES
        and tile % (4 * SUBLANES * freq_group) == 0
    )


def shift_order(groups):
    return [(groups // 2 - 1 - 2 * i) % (groups - 1) + 1 for i in range(groups - 1)]


def arrivals(groups):
    order = shift_order(groups)
    crossing = [s for s in order[1:] if s >= groups // 2]
    early = [s for s in order if s not in crossing and s != 1]
    return [0] + early, [1] + crossing[:-2], crossing[-2:]


def per_device_fast(wavefield, u_factors, v_factors, tile_ranks, tile_offsets):
    rec_dev, src_dev, samples = wavefield.shape
    freq_dev = u_factors.shape[1]
    groups = lax.axis_size("freq")
    row_group = lax.axis_size("rows")
    freqs = freq_dev * groups
    sources = src_dev * row_group
    tile = u_factors.shape[3]
    across = [(i, i ^ 2) for i in range(row_group)]
    beside = [(i, i ^ 1) for i in range(row_group)]
    u_own, v_own = u_factors[:, :, 0], v_factors[:, :, 0]
    v_far = lax.ppermute(v_own, "rows", across)
    offsets_far = lax.ppermute(tile_offsets, "rows", across)
    *sent, table = transform(wavefield.reshape(rec_dev * src_dev, samples), 2 * freqs, groups)
    own = {0: sent[0]}
    for shift in shift_order(groups):
        swap = [(i, i ^ shift) for i in range(groups)]
        own[shift] = lax.ppermute(sent[shift], "freq", swap)
    early, middle, last = arrivals(groups)

    def twins(shifts):
        pairs = {}
        for shift in shifts:
            pairs[shift] = lax.ppermute(own[shift], "rows", beside)
        return pairs

    def blocks(shifts):
        return [own[s] for s in shifts], [twin[s] for s in shifts]

    twin = twins(early)
    (near,) = coefficients(early, [tile_offsets], *blocks(early), [v_own])
    waiting, near = lax.optimization_barrier(([own[s] for s in middle], near))
    own.update(zip(middle, waiting))
    twin.update(twins(middle))
    (leaving,) = coefficients(early, [offsets_far], *blocks(early), [v_far])
    waiting, near, leaving = lax.optimization_barrier(([own[s] for s in last], near, leaving))
    own.update(zip(last, waiting))
    twin.update(twins(last))
    (leaving,) = coefficients(middle, [offsets_far], *blocks(middle), [v_far], [leaving])
    (leaving,) = coefficients(last, [offsets_far], *blocks(last), [v_far], [leaving])
    late = middle + last
    far = lax.ppermute(leaving, "rows", across)
    (near,) = coefficients(late, [tile_offsets], *blocks(late), [v_own], [near])
    half = bands_of(True, tile_offsets, tile_ranks, near, u_own, groups)
    bands = bands_of(False, tile_offsets, tile_ranks, far, u_own, groups, half)
    returned = lax.all_to_all(bands, "freq", split_axis=0, concat_axis=0, tiled=True)
    series = series_of(returned, table, math.sqrt(samples) / math.sqrt(freqs))
    return series.reshape(tile // groups, sources, samples)


def choose(wavefield, u_factors, v_factors, tile_ranks, tile_offsets):
    ok = fits(
        wavefield.shape[0],
        wavefield.shape[1],
        wavefield.shape[2],
        u_factors.shape[1],
        u_factors.shape[2],
        u_factors.shape[3],
        u_factors.shape[4],
        lax.axis_size("freq"),
        lax.axis_size("rows"),
    )
    step = per_device_fast if ok else per_device
    return step(wavefield, u_factors, v_factors, tile_ranks, tile_offsets)


def solution(mesh):
    placed = (
        P("freq", "rows", None),
        P(None, "freq", "rows", None, None),
        P(None, "freq", "rows", None, None),
        P("freq", "rows", None),
        P("freq", "rows", None),
    )
    return jax.shard_map(
        choose,
        mesh=mesh,
        in_specs=placed,
        out_specs=P(("rows", "freq"), None, None),
        check_vma=False,
    )
```

```python
import functools
import math

import jax
import jax.numpy as jnp
from jax import lax
from jax.experimental import pallas as pl
from jax.experimental.pallas import tpu as pltpu
from jax.sharding import PartitionSpec as P


RANK_MAX = 64
LANES = 128
SUBLANES = 8
NT = (((1,), (1,)), ((), ()))
VMEM = pl.BlockSpec(memory_space=pltpu.VMEM)
SMEM = pl.BlockSpec(memory_space=pltpu.SMEM)
PAIRED = (4, 8, 16)
AHEAD = 3


def spectral_tables(freq_count, sample_count):
    freq_bins = jnp.arange(freq_count, dtype=jnp.int32) + 1
    sample_index = jnp.arange(sample_count, dtype=jnp.int32)
    phase_int = freq_bins[:, None] * sample_index[None, :] % sample_count
    angles = phase_int.astype(jnp.float32) * (2.0 * math.pi / sample_count)
    cosine = jnp.cos(angles)
    minus_sine = -jnp.sin(angles)
    stacked = jnp.stack([cosine, minus_sine], axis=1)
    forward = (stacked / math.sqrt(sample_count)).astype(jnp.bfloat16)
    inverse = (stacked / math.sqrt(freq_count)).astype(jnp.bfloat16)
    return (forward, inverse)


def tile_windows(v_row, u_row, starts, rank_max):
    columns = starts.shape[0]
    slot_index = (starts[:, None] + jnp.arange(rank_max, dtype=jnp.int32)[None, :]).reshape(-1)
    v_padded = jnp.pad(v_row, ((0, 0), (0, rank_max), (0, 0)))
    u_padded = jnp.pad(u_row, ((0, 0), (0, 0), (0, rank_max)))
    v_win = jnp.take(v_padded, slot_index, axis=1).reshape(2, columns, rank_max, v_row.shape[2])
    u_win = jnp.take(u_padded, slot_index, axis=2).reshape(2, u_row.shape[1], columns, rank_max)
    return (v_win, u_win)


def slot_lookup(starts, counts, rank_max, slot_count):
    position = jnp.arange(slot_count, dtype=jnp.int32)
    started = starts[:, None, :] <= position[None, :, None]
    owner_tile = jnp.sum(started.astype(jnp.int32), axis=2) - 1
    first_slot = jnp.max(jnp.where(started, starts[:, None, :], 0), axis=2)
    within = position[None, :] - first_slot
    live_slot = position[None, :] < (starts[:, -1] + counts[:, -1])[:, None]
    flat_index = jnp.where(live_slot, owner_tile * rank_max + within, 0)
    return (flat_index, live_slot)


def take_slots(values, chosen):
    return jnp.take(values, chosen, axis=1)


def per_device(wavefield, u_factors, v_factors, tile_ranks, tile_offsets):
    rec_dev, src_dev, samples = wavefield.shape
    freq_dev = u_factors.shape[1]
    rows_dev = u_factors.shape[2]
    tile_size = u_factors.shape[3]
    slot_count = u_factors.shape[4]
    freq_group = lax.axis_size("freq")
    row_group = lax.axis_size("rows")
    freqs = freq_dev * freq_group
    receivers = rec_dev * freq_group
    columns = receivers // tile_size
    sources = src_dev * row_group
    forward, inverse = spectral_tables(freqs, samples)
    spectrum = jnp.einsum("kct,rst->kcrs", forward, wavefield, preferred_element_type=jnp.float32)
    spectrum = spectrum.astype(jnp.bfloat16).reshape(freqs, 2, rec_dev * src_dev)
    windows = jax.vmap(
        functools.partial(tile_windows, rank_max=RANK_MAX), in_axes=(1, 1, 0), out_axes=(1, 1)
    )
    rank_slots = jnp.arange(RANK_MAX, dtype=jnp.int32)
    tile_row = 0
    v_win, u_win = windows(
        v_factors[:, :, tile_row], u_factors[:, :, tile_row], tile_offsets[:, tile_row]
    )
    rank_mask = rank_slots[None, None, :] < tile_ranks[:, tile_row, :, None]
    flat_index, live_slot = slot_lookup(
        tile_offsets[:, tile_row], tile_ranks[:, tile_row], RANK_MAX, slot_count
    )
    prepared = [(v_win, u_win, rank_mask, flat_index, live_slot)]
    by_frequency = lax.all_to_all(spectrum, "freq", split_axis=0, concat_axis=2, tiled=True)
    portion = lax.all_gather(by_frequency[None], "rows", axis=0, tiled=True)
    blocks_in = portion.shape[0]
    spectra = portion.reshape(blocks_in, freq_dev, 2, columns, tile_size, src_dev)
    spectra = jnp.transpose(spectra, (1, 2, 3, 4, 0, 5)).reshape(
        freq_dev, 2, columns, tile_size, blocks_in * src_dev
    )
    tile_row = 0
    v_win, u_win, rank_mask, flat_index, live_slot = prepared[tile_row]
    quadrants = jnp.einsum(
        "afjmr,fbjrs->fabjms", v_win, spectra, preferred_element_type=jnp.float32
    )
    coeffs = jnp.stack(
        [quadrants[:, 0, 0] - quadrants[:, 1, 1], quadrants[:, 0, 1] + quadrants[:, 1, 0]], axis=1
    )
    coeffs = jnp.where(rank_mask[:, None, :, :, None], coeffs, 0.0).astype(jnp.bfloat16)
    stacked = coeffs.reshape(freq_dev, 2, columns * RANK_MAX, blocks_in * src_dev)
    packed = jax.vmap(take_slots)(stacked, flat_index)
    packed = jnp.where(live_slot[:, None, :, None], packed, jnp.zeros((), jnp.bfloat16))
    products = jnp.einsum(
        "afrk,fcks->facrs", u_factors[:, :, tile_row], packed, preferred_element_type=jnp.float32
    )
    results = [
        jnp.stack(
            [products[:, 0, 0] - products[:, 1, 1], products[:, 0, 1] + products[:, 1, 0]], axis=1
        )
    ]
    merged = jnp.stack(results, axis=2)
    bands = merged.astype(jnp.bfloat16).reshape(
        freq_dev, 2, rows_dev * tile_size, blocks_in, src_dev
    )
    bands = bands.reshape(freq_dev, 2, rows_dev * tile_size * sources)
    returned = lax.all_to_all(bands, "freq", split_axis=2, concat_axis=0, tiled=True)
    series = jnp.einsum("kcq,kct->qt", returned, inverse, preferred_element_type=jnp.float32)
    return series.astype(jnp.bfloat16).reshape(rows_dev * tile_size // freq_group, sources, samples)


def cosines(kinds, samples):
    row = lax.broadcasted_iota(jnp.int32, (kinds, samples), 0)
    index = lax.broadcasted_iota(jnp.int32, (kinds, samples), 1)
    phase = (((row >> 1) + 1) * index + (row & 1) * (samples // 4)) & (samples - 1)
    angles = phase.astype(jnp.float32) * (2.0 * math.pi / samples)
    return (jnp.cos(angles) * (1.0 / math.sqrt(samples))).astype(jnp.bfloat16)


def transform_kernel(traces_ref, *refs):
    groups = lax.axis_size("freq")
    outs, (table_ref, traces, sems, repeated, products, turned) = refs[:groups], refs[groups:]
    me = lax.axis_index("freq")
    rows = products.shape[1]
    kinds = turned.shape[0] // SUBLANES
    packs = LANES // kinds
    blocks = traces_ref.shape[0] // rows
    each = outs[0].shape[0]

    def copy(i):
        part = pl.ds(pl.multiple_of(i * rows, rows), rows)
        return pltpu.make_async_copy(traces_ref.at[part, :], traces.at[part, :], sems.at[i])

    def turn(i, source_rows):
        place = lax.broadcasted_iota(jnp.int32, (rows // SUBLANES, LANES), 1) // kinds
        for first in range(0, SUBLANES, packs):
            mixed = source_rows[pl.ds(first, rows // SUBLANES, stride=SUBLANES), :]
            for m in range(1, packs):
                part = source_rows[pl.ds(first + m, rows // SUBLANES, stride=SUBLANES), :]
                mixed = jnp.where(place == m, part, mixed)
            mixed = mixed.T
            for m in range(packs):
                turned[pl.ds(first + m, kinds, stride=SUBLANES), :] = mixed[
                    m * kinds : (m + 1) * kinds
                ]
        lanes = pl.ds(pl.multiple_of(i * LANES, LANES), LANES)
        for shift, out in enumerate(outs):
            group = me ^ shift
            start = pl.multiple_of(group * each, each)
            out[:, lanes] = turned[pl.ds(start, each), :].astype(jnp.bfloat16)

    for i in range(min(AHEAD, blocks)):
        copy(i).start()
    table_ref[...] = cosines(kinds, traces.shape[1])
    for m in range(packs):
        repeated[m * kinds : (m + 1) * kinds, :] = table_ref[...]

    def step(i, carry):
        now = lax.rem(i, 2)

        @pl.when(i + AHEAD < blocks)
        def _():
            copy(i + AHEAD).start()

        copy(i).wait()
        part = pl.ds(pl.multiple_of(i * rows, rows), rows)
        turn(jnp.maximum(i - 1, 0), products.at[1 - now])
        products[now] = lax.dot_general(
            traces[part, :], repeated[...], NT, preferred_element_type=jnp.float32
        )
        return carry

    lax.fori_loop(0, blocks, step, 0)
    turn(blocks - 1, products.at[(blocks - 1) % 2])


def transform(traces, kinds, groups):
    rows, samples = traces.shape
    receivers = rows // SUBLANES
    shape = jax.ShapeDtypeStruct((kinds * SUBLANES // groups, receivers), jnp.bfloat16)
    return pl.pallas_call(
        transform_kernel,
        in_specs=[pl.BlockSpec(memory_space=pltpu.HBM)],
        out_specs=[VMEM] * (groups + 1),
        out_shape=[shape] * groups + [jax.ShapeDtypeStruct((kinds, samples), jnp.bfloat16)],
        scratch_shapes=[
            pltpu.VMEM((rows, samples), jnp.bfloat16),
            pltpu.SemaphoreType.DMA((receivers // LANES,)),
            pltpu.VMEM((LANES, samples), jnp.bfloat16),
            pltpu.VMEM((2, LANES * SUBLANES, LANES), jnp.float32),
            pltpu.VMEM((kinds * SUBLANES, LANES), jnp.float32),
        ],
        compiler_params=pltpu.CompilerParams(vmem_limit_bytes=48 * 2**20),
        cost_estimate=pl.CostEstimate(
            flops=2 * rows * samples * 256, bytes_accessed=rows * samples * 2, transcendentals=0
        ),
        name="transform",
    )(traces)


def coefficient_kernel(shifts, sides, before, *refs):
    count = len(shifts)
    refs = list(refs)
    offsets = [refs.pop(0) for _ in range(sides)]
    own = [refs.pop(0) for _ in range(count)]
    twin = [refs.pop(0) for _ in range(count)]
    factors = [refs.pop(0) for _ in range(sides)]
    earlier = [refs.pop(0) for _ in range(before)]
    outs = [refs.pop(0) for _ in range(sides)]
    (lhs,) = refs
    groups = lax.axis_size("freq")
    me = lax.axis_index("freq")
    core = lax.rem(lax.axis_index("rows"), 2)
    _, freqs, slots, tile = factors[0].shape
    per_block = own[0].shape[1] // tile
    columns = groups * per_block
    half = 2 * SUBLANES
    deep = 2 * half
    for k in range(freqs):
        for arrays, at in ((own, core), (twin, 1 - core)):
            for b in range(count):
                for inner in range(per_block):
                    start = (b * per_block + inner) * deep + at * half
                    lhs[k, pl.ds(pl.multiple_of(start, half), half), :] = arrays[b][
                        k * half : (k + 1) * half, inner * tile : (inner + 1) * tile
                    ]
    for side in range(sides):
        for k in range(freqs):
            for low in range(0, slots, tile):
                slot = lax.broadcasted_iota(jnp.int32, (deep, tile), 1) + low
                chosen = []
                for part in range(2):
                    products = lax.dot_general(
                        lhs[k],
                        factors[side][part, k, low : low + tile, :],
                        NT,
                        preferred_element_type=jnp.float32,
                    )
                    total = jnp.zeros((deep, tile), jnp.float32)
                    for b, shift in enumerate(shifts):
                        column = (me ^ shift) * per_block
                        value = total
                        for inner in range(per_block):
                            at = (b * per_block + inner) * deep
                            value = jnp.where(
                                slot >= offsets[side][k, 0, column + inner],
                                products[at : at + deep],
                                value,
                            )
                        after = jnp.minimum(column + per_block, columns - 1)
                        end = jnp.where(
                            column + per_block < columns, offsets[side][k, 0, after], slots
                        )
                        total = jnp.where(slot >= end, total, value)
                    chosen.append(total)
                by_real, by_imag = chosen
                n = SUBLANES
                real = [by_real[g : g + n] - by_imag[g + n : g + 2 * n] for g in (0, half)]
                imag = [by_real[g + n : g + 2 * n] + by_imag[g : g + n] for g in (0, half)]
                for c, pieces in enumerate((real, imag)):
                    value = jnp.concatenate(pieces, 0)
                    if side < before:
                        value += earlier[side][k, c, :, low : low + tile].astype(jnp.float32)
                    outs[side][k, c, :, low : low + tile] = value.astype(jnp.bfloat16)


def coefficients(shifts, offsets, own, twin, factors, earlier=()):
    sides, count = len(offsets), len(shifts)
    _, freqs, slots, tile = factors[0].shape
    columns = count * own[0].shape[1] // tile
    shape = jax.ShapeDtypeStruct((freqs, 2, 2 * SUBLANES, slots), jnp.bfloat16)
    return pl.pallas_call(
        functools.partial(coefficient_kernel, tuple(shifts), sides, len(earlier)),
        in_specs=[SMEM] * sides + [VMEM] * (2 * count + sides + len(earlier)),
        out_specs=[VMEM] * sides,
        out_shape=[shape] * sides,
        scratch_shapes=[pltpu.VMEM((freqs, columns * 4 * SUBLANES, tile), jnp.bfloat16)],
        compiler_params=pltpu.CompilerParams(vmem_limit_bytes=16 * 2**20),
        cost_estimate=pl.CostEstimate(
            flops=2 * 2 * sides * freqs * slots * columns * 4 * SUBLANES * tile,
            bytes_accessed=2**20,
            transcendentals=0,
        ),
        name="coefficients",
    )(*offsets, *own, *twin, *factors, *earlier)


def band_kernel(add, at_near, offsets_ref, ranks_ref, coeffs_ref, u_ref, *refs):
    refs = list(refs)
    other_ref = refs.pop(0) if add else None
    out_ref, rhs, crossed = refs[:3]
    freqs, _, sources, slots = coeffs_ref.shape
    tile = u_ref.shape[2]
    place = lax.rem(lax.axis_index("rows") // 2, 2)
    at = place if at_near else 1 - place
    last = offsets_ref.shape[2] - 1
    wide = 2 * sources
    rhs[...] = jnp.zeros_like(rhs)
    crossed[...] = jnp.zeros_like(crossed)
    slot = lax.broadcasted_iota(jnp.int32, (sources, slots), 1)
    for k in range(freqs):
        live = slot < offsets_ref[k, 0, last] + ranks_ref[k, 0, last]
        for part in range(2):
            value = jnp.where(live, coeffs_ref[k, part].astype(jnp.float32), 0.0)
            start = pl.multiple_of((2 * k + part) * wide + at * sources, sources)
            rhs[k, pl.ds(start, sources), :] = value.astype(jnp.bfloat16)
            start = pl.multiple_of((2 * k + 1 - part) * wide + at * sources, sources)
            value = value if part == 0 else -value
            crossed[k, pl.ds(start, sources), :] = value.astype(jnp.bfloat16)
    total = other_ref[...] if add else jnp.zeros((tile, 2 * freqs * wide), jnp.float32)
    for k in range(freqs):
        for part, ref in enumerate((rhs, crossed)):
            total += lax.dot_general(u_ref[part, k], ref[k], NT, preferred_element_type=jnp.float32)
    if not add:
        out_ref[...] = total
        return
    bands, mix = refs[3:]
    groups = out_ref.shape[0]
    bands[...] = total
    packs = LANES // wide
    kinds = 2 * freqs
    block = lax.broadcasted_iota(jnp.int32, (tile // packs, LANES), 1) // wide
    loaded = [bands[pl.ds(b, tile // packs, stride=packs), :] for b in range(packs)]
    rows = tile // packs // groups
    for kind in range(kinds):
        mixed = jnp.zeros((tile // packs, LANES), jnp.float32)
        for b in range(packs):
            shift = (b - kind) * wide % LANES
            moved = pltpu.roll(loaded[b], shift, 1) if shift else loaded[b]
            mixed = jnp.where(block == b, moved, mixed)
        mix[:, kind * rows : (kind + 1) * rows, :] = mixed.reshape(groups, rows, LANES)
    out_ref[...] = mix[...].astype(jnp.bfloat16)


def bands_of(at_near, offsets, ranks, coeffs, u_own, groups, other=None):
    add = other is not None
    freqs, _, sources, slots = coeffs.shape
    tile = u_own.shape[2]
    rows = 2 * freqs * tile * 2 * sources // LANES // groups
    partial = jax.ShapeDtypeStruct((tile, LANES), jnp.float32)
    whole = jax.ShapeDtypeStruct((groups, rows, LANES), jnp.bfloat16)
    spread = pltpu.VMEM((freqs, LANES, slots), jnp.bfloat16)
    mixing = [pltpu.VMEM((tile, LANES), jnp.float32), pltpu.VMEM(whole.shape, jnp.float32)]
    return pl.pallas_call(
        functools.partial(band_kernel, add, at_near),
        in_specs=[SMEM] * 2 + [VMEM] * (3 if add else 2),
        out_specs=VMEM,
        out_shape=whole if add else partial,
        scratch_shapes=[spread, spread] + (mixing if add else []),
        compiler_params=pltpu.CompilerParams(vmem_limit_bytes=8 * 2**20),
        cost_estimate=pl.CostEstimate(
            flops=2 * 2 * freqs * tile * LANES * slots, bytes_accessed=2**20, transcendentals=0
        ),
        name="bands",
    )(offsets, ranks, coeffs, u_own, *([other] if add else []))


def series_kernel(scale, bands_ref, table_ref, out_ref, wide, done, sems):
    groups, rows, lanes = bands_ref.shape
    kinds = table_ref.shape[0]
    steps = groups * rows // kinds
    wide[...] = bands_ref[...].astype(jnp.float32).reshape(groups * rows, lanes) * scale
    copies = []
    for i in range(steps):
        part = wide[pl.ds(i, kinds, stride=steps), :]
        done[i] = jnp.dot(
            part.T.astype(jnp.bfloat16), table_ref[...], preferred_element_type=jnp.float32
        ).astype(jnp.bfloat16)
        copies.append(
            pltpu.make_async_copy(
                done.at[i], out_ref.at[i * lanes : (i + 1) * lanes, :], sems.at[i]
            )
        )
        copies[-1].start()
    for copy in copies:
        copy.wait()


def series_of(bands, table, scale):
    groups, rows, lanes = bands.shape
    kinds, samples = table.shape
    steps = groups * rows // kinds
    return pl.pallas_call(
        functools.partial(series_kernel, scale),
        in_specs=[VMEM] * 2,
        out_specs=pl.BlockSpec(memory_space=pl.ANY),
        out_shape=jax.ShapeDtypeStruct((steps * lanes, samples), jnp.bfloat16),
        scratch_shapes=[
            pltpu.VMEM((groups * rows, lanes), jnp.float32),
            pltpu.VMEM((steps, lanes, samples), jnp.bfloat16),
            pltpu.SemaphoreType.DMA((steps,)),
        ],
        compiler_params=pltpu.CompilerParams(vmem_limit_bytes=16 * 2**20),
        cost_estimate=pl.CostEstimate(
            flops=2 * steps * lanes * kinds * samples,
            bytes_accessed=steps * lanes * samples * 2,
            transcendentals=0,
        ),
        name="series",
    )(bands, table)


def fits(rec_dev, src_dev, samples, freq_dev, rows_dev, tile, slots, freq_group, row_group):
    kinds = 2 * freq_dev * freq_group
    ratio = math.sqrt(samples) / math.sqrt(freq_dev * freq_group)
    return (
        math.frexp(ratio)[0] == 0.5
        and math.sqrt(samples).is_integer()
        and samples & (samples - 1) == 0
        and src_dev == SUBLANES
        and row_group == 4
        and rows_dev == 1
        and freq_group in PAIRED
        and rec_dev % tile == 0
        and tile % (2 * LANES) == 0
        and slots % tile == 0
        and LANES % kinds == 0
        and SUBLANES % (LANES // kinds) == 0
        and 2 * freq_dev * src_dev * row_group == LANES
        and tile % (4 * SUBLANES * freq_group) == 0
    )


def shift_order(groups):
    return [(groups // 2 - 1 - 2 * i) % (groups - 1) + 1 for i in range(groups - 1)]


def arrivals(groups):
    order = shift_order(groups)
    last = [s for s in order[1:] if s >= groups // 2][-2:]
    early = [s for s in order[:2] if s not in last]
    middle = sorted((s for s in order if s not in early + last), key=lambda s: s >= groups // 2)
    return [0] + early, middle, last


def per_device_fast(wavefield, u_factors, v_factors, tile_ranks, tile_offsets):
    rec_dev, src_dev, samples = wavefield.shape
    freq_dev = u_factors.shape[1]
    groups = lax.axis_size("freq")
    row_group = lax.axis_size("rows")
    freqs = freq_dev * groups
    sources = src_dev * row_group
    tile = u_factors.shape[3]
    across = [(i, i ^ 2) for i in range(row_group)]
    beside = [(i, i ^ 1) for i in range(row_group)]
    u_own, v_own = u_factors[:, :, 0], v_factors[:, :, 0]
    v_far = lax.ppermute(v_own, "rows", across)
    offsets_far = lax.ppermute(tile_offsets, "rows", across)
    *sent, table = transform(wavefield.reshape(rec_dev * src_dev, samples), 2 * freqs, groups)
    own = {0: sent[0]}
    for shift in shift_order(groups):
        swap = [(i, i ^ shift) for i in range(groups)]
        own[shift] = lax.ppermute(sent[shift], "freq", swap)
    early, middle, last = arrivals(groups)

    def twins(shifts):
        pairs = {}
        for shift in shifts:
            pairs[shift] = lax.ppermute(own[shift], "rows", beside)
        return pairs

    def blocks(shifts):
        return [own[s] for s in shifts], [twin[s] for s in shifts]

    twin = twins(early)
    (near,) = coefficients(early, [tile_offsets], *blocks(early), [v_own])
    waiting, near = lax.optimization_barrier(([own[s] for s in middle], near))
    own.update(zip(middle, waiting))
    twin.update(twins(middle))
    (leaving,) = coefficients(early, [offsets_far], *blocks(early), [v_far])
    waiting, near, leaving = lax.optimization_barrier(([own[s] for s in last], near, leaving))
    own.update(zip(last, waiting))
    twin.update(twins(last))
    (leaving,) = coefficients(middle, [offsets_far], *blocks(middle), [v_far], [leaving])
    (leaving,) = coefficients(last, [offsets_far], *blocks(last), [v_far], [leaving])
    late = middle + last
    far = lax.ppermute(leaving, "rows", across)
    (near,) = coefficients(late, [tile_offsets], *blocks(late), [v_own], [near])
    half = bands_of(True, tile_offsets, tile_ranks, near, u_own, groups)
    bands = bands_of(False, tile_offsets, tile_ranks, far, u_own, groups, half)
    returned = lax.all_to_all(bands, "freq", split_axis=0, concat_axis=0, tiled=True)
    series = series_of(returned, table, math.sqrt(samples) / math.sqrt(freqs))
    return series.reshape(tile // groups, sources, samples)


def choose(wavefield, u_factors, v_factors, tile_ranks, tile_offsets):
    ok = fits(
        wavefield.shape[0],
        wavefield.shape[1],
        wavefield.shape[2],
        u_factors.shape[1],
        u_factors.shape[2],
        u_factors.shape[3],
        u_factors.shape[4],
        lax.axis_size("freq"),
        lax.axis_size("rows"),
    )
    step = per_device_fast if ok else per_device
    return step(wavefield, u_factors, v_factors, tile_ranks, tile_offsets)


def solution(mesh):
    placed = (
        P("freq", "rows", None),
        P(None, "freq", "rows", None, None),
        P(None, "freq", "rows", None, None),
        P("freq", "rows", None),
        P("freq", "rows", None),
    )
    return jax.shard_map(
        choose,
        mesh=mesh,
        in_specs=placed,
        out_specs=P(("rows", "freq"), None, None),
        check_vma=False,
    )
```
